128 devices in a mesh: prob: 1, samp: 16 (over z, y), feat: 8 (over x, core).
Axes of the slice: x: 4, y: 4, z: 4, core: 2. Of those that a mesh axis runs over, the one named last changes fastest.
Arguments:
- x_mat: bfloat16 [8192, 16384], P(('prob', 'samp'), 'feat')
- w_init: float32 [16384, 256], P(('prob', 'feat'))
- targets: float32 [8192, 256], P(('prob', 'samp'))
- step_size: float32 [16384], P(('prob', 'feat'))
Outputs:
- output 1: float32 [16384, 256], P(('prob', 'feat'))
- output 2: float32 [8192, 256], P(('prob', 'samp'))
All inputs are finite; a program needn't handle non-finite values.
Results may differ from the reference program's by a relative error of at most 0.0040641.
Values are sent between devices in bfloat16 or wider.
A program may use at most 1 GiB of HBM per device.

```python
import math
import jax
import jax.numpy as jnp
from jax import lax

SAMPLES = 8192
FEATURES = 16384
TARGETS = 256
FEAT_BLOCKS = 8
SWEEPS = 4
COMBINE_WEIGHT = 0.8
RIDGE_SCALE = 0.1


def feature_steps(x_mat, spread, start_key):
    col_sq = jnp.sum(jnp.square(x_mat.astype(jnp.float32)), axis=0) / SAMPLES
    precond = spread / col_sq
    root_pre = jnp.sqrt(precond)
    start_dir = jax.random.normal(start_key, (FEATURES,), jnp.float32)
    start_dir = start_dir / jnp.sqrt(jnp.sum(start_dir * start_dir))

    def power_step(direction, unused):
        row_vals = jnp.dot(x_mat, (root_pre * direction).astype(jnp.bfloat16), preferred_element_type=jnp.float32)
        col_vals = root_pre * jnp.dot(row_vals.astype(jnp.bfloat16), x_mat, preferred_element_type=jnp.float32) / SAMPLES
        dir_norm = jnp.sqrt(jnp.sum(col_vals * col_vals))
        return col_vals / dir_norm, dir_norm

    final_dir, dir_norms = lax.scan(power_step, start_dir, None, length=30)
    return precond / dir_norms[-1]


def setup_inputs(seed: int = 0, part: int = 0) -> dict:
    part_key = jax.random.fold_in(jax.random.key(seed), part)
    key_list = jax.random.split(part_key, 8)
    factor_rank = 8
    shared_frac = 2.0 * factor_rank / SAMPLES
    factors = jax.random.normal(key_list[0], (SAMPLES, factor_rank), jnp.float32)
    loadings = jax.random.normal(key_list[1], (FEATURES, factor_rank), jnp.float32)
    noise_part = jax.random.normal(key_list[2], (SAMPLES, FEATURES), jnp.float32)
    shared = jnp.dot(factors, loadings.T)
    x_mat = (math.sqrt(shared_frac / factor_rank) * shared + math.sqrt(1.0 - shared_frac) * noise_part).astype(jnp.bfloat16)
    spread = jnp.exp2(jax.random.uniform(key_list[3], (FEATURES,), jnp.float32, -2.0, 2.0))
    step_size = feature_steps(x_mat, spread, key_list[4])
    z_mat = jax.random.normal(key_list[5], (SAMPLES, TARGETS), jnp.float32).astype(jnp.bfloat16)
    w_raw = lax.dot_general(x_mat, z_mat, (((0,), (0,)), ((), ())), preferred_element_type=jnp.float32)
    w_fit = jnp.dot(x_mat, w_raw.astype(jnp.bfloat16), preferred_element_type=jnp.float32)
    w_init = w_raw * (0.7 / jnp.sqrt(jnp.mean(w_fit * w_fit)))
    w_true = jax.random.normal(key_list[6], (FEATURES, TARGETS), jnp.float32).astype(jnp.bfloat16)
    y_signal = jnp.dot(x_mat, w_true, preferred_element_type=jnp.float32)
    y_noise = jax.random.normal(key_list[7], (SAMPLES, TARGETS), jnp.float32)
    targets = 0.8 * y_signal / jnp.sqrt(jnp.mean(y_signal * y_signal)) + 0.6 * y_noise
    return {"x_mat": x_mat, "w_init": w_init, "targets": targets, "step_size": step_size}


def block_sum(x_mat, weights):
    feat_len = FEATURES // FEAT_BLOCKS
    weights_low = weights.astype(jnp.bfloat16)

    def one_block(total, block):
        x_block = lax.dynamic_slice_in_dim(x_mat, block * feat_len, feat_len, axis=1)
        w_block = lax.dynamic_slice_in_dim(weights_low, block * feat_len, feat_len, axis=0)
        block_prod = jnp.dot(x_block, w_block, preferred_element_type=jnp.float32)
        return total + block_prod.astype(jnp.bfloat16).astype(jnp.float32), None

    total, unused = lax.scan(one_block, jnp.zeros((SAMPLES, TARGETS), jnp.float32), jnp.arange(FEAT_BLOCKS))
    return total


def reference(x_mat, w_init, targets, step_size):
    ridge = RIDGE_SCALE * FEATURES / SAMPLES
    start_resid = targets - block_sum(x_mat, w_init)

    def sweep(state, unused):
        weights, residual = state
        gradient = lax.dot_general(x_mat, residual.astype(jnp.bfloat16), (((0,), (0,)), ((), ())), preferred_element_type=jnp.float32) / SAMPLES
        delta = step_size[:, None] * (gradient - ridge * weights)
        weights = weights + COMBINE_WEIGHT * delta
        residual = residual - COMBINE_WEIGHT * block_sum(x_mat, delta)
        return (weights, residual), None

    (weights, residual), unused = lax.scan(sweep, (w_init, start_resid), None, length=SWEEPS)
    return weights, residual
```

```python
import functools
import math

import jax
import jax.numpy as jnp
from jax import lax
from jax.experimental import pallas as pl
from jax.experimental.pallas import tpu as pltpu
from jax.sharding import PartitionSpec as P

SWEEPS = 4
COMBINE_WEIGHT = 0.8
RIDGE_SCALE = 0.1
PARTS = 2
LANES = 128
MESH = pl.DeviceIdType.MESH
F32 = jnp.float32
BF16 = jnp.bfloat16


def ridge_kernel(ring, chips, samples, ridge, x_hbm, w_hbm, y_hbm, eta_hbm, wo_hbm, ro_hbm,
                 x, xt, w_in, w, r, eta_in, eta_t, eta, g, rs1, s1, rs2, dw, u, ur, rb, wo, ro,
                 load_sem, store_sem,
                 rs1_s, rs1_r, rs2_s, rs2_r, ag1_s, ag1_r, ag2_s, ag2_r,
                 u_s, u_r, rg_s, rg_r, wg1_s, wg1_r, wg2_s, wg2_r, rf_s, rf_r):
    samp = lax.axis_index("samp")
    feat = lax.axis_index("feat")
    rows, width = x.shape
    half = width // 2
    group = half // ring
    chunk = group // ring
    piece = rows // (2 * chips)
    cy, cz = lax.rem(samp, ring), lax.div(samp, ring)
    cx, core = lax.div(feat, 2), lax.rem(feat, 2)
    ys = [cy] + [lax.rem(cy + d, ring) for d in range(1, ring)]
    zs = [cz] + [lax.rem(cz + d, ring) for d in range(1, ring)]
    firsts = (ys, zs)
    seconds = (zs, ys)
    neighbour = [[cz * ring + c for c in ys], [c * ring + cy for c in zs]]
    far_first = sorted(range(1, ring), key=lambda d: -min(d, ring - d))
    peers = [(dx, dc) for dx in far_first + [0] for dc in (0, 1) if dx or dc]

    xs = [cx] + [lax.rem(cx + d, chips) for d in range(1, chips)]
    cores = [core, 1 - core]
    feats = [xs[dx] * 2 + cores[dc] for dx, dc in peers]
    group_rows = [[h * half + c * group for c in firsts[h]] for h in (0, 1)]
    chunk_rows = [[c * chunk for c in seconds[h]] for h in (0, 1)]
    own_chunks = [[group_rows[h][0] + c for c in chunk_rows[h]] for h in (0, 1)]
    piece_rows = [f * piece for f in feats]
    mine = pl.ds(feat * piece, piece)

    def along(axis, d):
        return {"samp": neighbour[axis][d]}

    def remote(src, dst, send, recv, device):
        return pltpu.make_async_remote_copy(
            src_ref=src, dst_ref=dst, send_sem=send, recv_sem=recv, device_id=device, device_id_type=MESH)

    def group_at(h, d):
        return pl.ds(group_rows[h][d], group)

    def part_at(h, e):
        return pl.ds(chunk_rows[h][e], chunk)

    def chunk_at(h, e):
        return pl.ds(own_chunks[h][e], chunk)

    def rs1_copy(p, h, d):
        return remote(g.at[p, group_at(h, d)], rs1.at[p, h, d - 1],
                      rs1_s.at[p, h, d - 1], rs1_r.at[p, h, d - 1], along(h, d))

    def rs2_copy(p, h, d):
        return remote(s1.at[p, h, part_at(h, d)], rs2.at[p, h, d - 1],
                      rs2_s.at[p, h, d - 1], rs2_r.at[p, h, d - 1], along(1 - h, d))

    def gather1(buf, ss, rr, p, h, d):
        at = chunk_at(h, 0)
        return remote(buf.at[p, at], buf.at[p, at], ss.at[p, h, d - 1], rr.at[p, h, d - 1], along(1 - h, d))

    def gather2(buf, ss, rr, p, h, e, d):
        at = chunk_at(h, (ring - e) % ring)
        return remote(buf.at[p, at], buf.at[p, at], ss.at[p, h, e, d - 1], rr.at[p, h, e, d - 1], along(h, d))

    def u_copy(p, i):
        return remote(u.at[p, pl.ds(piece_rows[i], piece)], ur.at[p, i], u_s.at[p, i], u_r.at[p, i], {"feat": feats[i]})

    def r_copy(buf, ss, rr, p, i):
        return remote(buf.at[p, mine], buf.at[p, mine], ss.at[p, i], rr.at[p, i], {"feat": feats[i]})

    def start_u(p):
        step = max(rows // 2, piece)
        for k in range(rows // step):
            at = pl.ds(k * step, step)
            u[p, at] = jnp.dot(x[at], dw[p], preferred_element_type=F32).astype(BF16)
        for i in range(len(peers)):
            u_copy(p, i).start()

    def sum_u(p):
        total = u[p, mine].astype(F32)
        for i in range(len(peers)):
            u_copy(p, i).wait_recv()
        for i in range(len(peers)):
            total = total + ur[p, i].astype(F32)
        for i in range(len(peers)):
            u_copy(p, i).wait_send()
        return total

    def send_r(p):
        rb[p, mine] = r[p].astype(BF16)
        for i in range(len(peers)):
            r_copy(rb, rg_s, rg_r, p, i).start()

    def start_g(p):
        for i in range(len(peers)):
            r_copy(rb, rg_s, rg_r, p, i).wait_recv()
        for d in far_first + [0]:
            for h in (0, 1):
                at = group_at(h, d)
                g[p, at] = jnp.dot(xt[at], rb[p], preferred_element_type=F32)
                if d:
                    rs1_copy(p, h, d).start()
        for i in range(len(peers)):
            r_copy(rb, rg_s, rg_r, p, i).wait_send()

    def mid_g(p):
        for h in (0, 1):
            for d in range(1, ring):
                rs1_copy(p, h, d).wait_recv()
            for e in far_first + [0]:
                total = g[p, chunk_at(h, e)]
                for d in range(1, ring):
                    total = total + rs1[p, h, d - 1, part_at(h, e)]
                s1[p, h, part_at(h, e)] = total
                if e:
                    rs2_copy(p, h, e).start()

    def end_g(p, last):
        for h in (0, 1):
            for d in range(1, ring):
                rs2_copy(p, h, d).wait_recv()
            total = s1[p, h, part_at(h, 0)]
            for d in range(1, ring):
                total = total + rs2[p, h, d - 1]
            delta = eta[h] * (total / samples - ridge * w[p, h])
            at = chunk_at(h, 0)
            dw[p, at] = delta.astype(BF16)
            for d in far_first:
                gather1(dw, ag1_s, ag1_r, p, h, d).start()
            for d in far_first:
                gather2(dw, ag2_s, ag2_r, p, h, 0, d).start()
            new = w[p, h] + COMBINE_WEIGHT * delta
            w[p, h] = new
            if last:
                wo[p, at] = new

    def relay(buf, s1_, r1_, s2_, r2_, p):
        for e in range(1, ring):
            for h in (0, 1):
                gather1(buf, s1_, r1_, p, h, e).wait_recv()
                for d in far_first:
                    gather2(buf, s2_, r2_, p, h, e, d).start()

    def gathered(buf, s1_, r1_, s2_, r2_, p):
        for h in (0, 1):
            for e in range(ring):
                for d in range(1, ring):
                    gather2(buf, s2_, r2_, p, h, e, d).wait_recv()
        for h in (0, 1):
            for d in range(1, ring):
                gather1(buf, s1_, r1_, p, h, d).wait_send()
                for e in range(ring):
                    gather2(buf, s2_, r2_, p, h, e, d).wait_send()

    def sent_g(p):
        for h in (0, 1):
            for d in range(1, ring):
                rs1_copy(p, h, d).wait_send()
                rs2_copy(p, h, d).wait_send()

    ag = (dw, ag1_s, ag1_r, ag2_s, ag2_r)
    wg = (wo, wg1_s, wg1_r, wg2_s, wg2_r)

    loads = [pltpu.make_async_copy(w_hbm, w_in, load_sem.at[0]),
             pltpu.make_async_copy(x_hbm, x, load_sem.at[1]),
             pltpu.make_async_copy(eta_hbm, eta_in, load_sem.at[2])]
    loads += [pltpu.make_async_copy(y_hbm.at[mine, pl.ds(p * LANES, LANES)], r.at[p], load_sem.at[3 + p])
              for p in range(PARTS)]
    for load in loads:
        load.start()
    barrier = pltpu.get_barrier_semaphore()
    for d in range(1, ring):
        for axis in (0, 1):
            pl.semaphore_signal(barrier, inc=1, device_id=along(axis, d), device_id_type=MESH)
    for i in range(len(peers)):
        pl.semaphore_signal(barrier, inc=1, device_id={"feat": feats[i]}, device_id_type=MESH)
    loads[0].wait()
    for p in range(PARTS):
        dw[p] = w_in[:, p * LANES:(p + 1) * LANES].astype(BF16)
        for h in (0, 1):
            w[p, h] = w_in[chunk_at(h, 0), p * LANES:(p + 1) * LANES]
    loads[1].wait()
    pl.semaphore_wait(barrier, 2 * (ring - 1) + len(peers))

    for p in range(PARTS):
        start_u(p)
    tile = min(width, 256)
    for k in range(width // tile):
        at = pl.ds(k * tile, tile)
        xt[at] = x[:, k * tile:(k + 1) * tile].T
    loads[2].wait()
    for h in (0, 1):
        pos = own_chunks[h][0]
        line = eta_in[pl.ds(lax.div(pos, LANES), 1), :]
        wide = jnp.broadcast_to(line, (LANES, LANES)).T
        eta_t[...] = wide
        eta[h] = eta_t[pl.ds(lax.rem(pos, LANES), chunk), :]
    for p in range(PARTS):
        loads[3 + p].wait()
        r[p] = r[p] - sum_u(p)
        send_r(p)

    def sweep(last):
        for p in range(PARTS):
            start_g(p)
        for p in range(PARTS):
            mid_g(p)
        for p in range(PARTS):
            end_g(p, last)
        for p in range(PARTS):
            relay(*ag, p)
        if last:
            for p in range(PARTS):
                for h in (0, 1):
                    for d in far_first:
                        gather1(*wg[:3], p, h, d).start()
                    for d in far_first:
                        gather2(wo, wg2_s, wg2_r, p, h, 0, d).start()
        for p in range(PARTS):
            sent_g(p)
            gathered(*ag, p)
            start_u(p)
        if last:
            for p in range(PARTS):
                relay(*wg, p)
        for p in range(PARTS):
            r[p] = r[p] - COMBINE_WEIGHT * sum_u(p)
            if last:
                ro[p, mine] = r[p]
                for i in range(len(peers)):
                    r_copy(ro, rf_s, rf_r, p, i).start()
            else:
                send_r(p)

    def body(i, carry):
        sweep(False)
        return carry

    lax.fori_loop(0, SWEEPS - 1, body, 0)
    sweep(True)

    stores = []
    for p in range(PARTS):
        for i in range(len(peers)):
            r_copy(ro, rf_s, rf_r, p, i).wait_recv()
        stores.append(pltpu.make_async_copy(ro.at[p], ro_hbm.at[:, pl.ds(p * LANES, LANES)], store_sem.at[p]))
        stores[-1].start()
    for p in range(PARTS):
        gathered(*wg, p)
        stores.append(pltpu.make_async_copy(wo.at[p], wo_hbm.at[:, pl.ds(p * LANES, LANES)], store_sem.at[PARTS + p]))
        stores[-1].start()
    for p in range(PARTS):
        for i in range(len(peers)):
            r_copy(ro, rf_s, rf_r, p, i).wait_send()
    for store in stores:
        store.wait()


def solution(mesh):
    samp_count = mesh.shape["samp"]
    feat_count = mesh.shape["feat"]
    ring = math.isqrt(samp_count)
    chips = feat_count // 2

    def local_solve(x_loc, w_loc, y_loc, eta_loc):
        rows, width = x_loc.shape
        samples = rows * samp_count
        ridge = RIDGE_SCALE * (width * feat_count) / samples
        group = width // 2 // ring
        chunk = group // ring
        piece = rows // feat_count
        npeer = feat_count - 1
        dma = pltpu.SemaphoreType.DMA
        v = pltpu.VMEM
        scratch = [
            v((rows, width), BF16),
            v((width, rows), BF16),
            v((width, PARTS * LANES), F32),
            v((PARTS, 2, chunk, LANES), F32),
            v((PARTS, piece, LANES), F32),
            v((width // LANES, LANES), F32),
            v((LANES, LANES), F32),
            v((2, chunk, LANES), F32),
            v((PARTS, width, LANES), F32),
            v((PARTS, 2, ring - 1, group, LANES), F32),
            v((PARTS, 2, group, LANES), F32),
            v((PARTS, 2, ring - 1, chunk, LANES), F32),
            v((PARTS, width, LANES), BF16),
            v((PARTS, rows, LANES), BF16),
            v((PARTS, npeer, piece, LANES), BF16),
            v((PARTS, rows, LANES), BF16),
            v((PARTS, width, LANES), F32),
            v((PARTS, rows, LANES), F32),
            dma((3 + PARTS,)), dma((2 * PARTS,)),
        ]
        step1 = (PARTS, 2, ring - 1)
        step2 = (PARTS, 2, ring, ring - 1)
        scratch += [dma(step1)] * 6 + [dma(step2)] * 2 + [dma((PARTS, npeer))] * 4
        scratch += [dma(step1)] * 2 + [dma(step2)] * 2 + [dma((PARTS, npeer))] * 2
        return pl.pallas_call(
            functools.partial(ridge_kernel, ring, chips, samples, ridge),
            out_shape=[jax.ShapeDtypeStruct(w_loc.shape, F32), jax.ShapeDtypeStruct(y_loc.shape, F32)],
            in_specs=[pl.BlockSpec(memory_space=pl.ANY)] * 4,
            out_specs=[pl.BlockSpec(memory_space=pl.ANY)] * 2,
            scratch_shapes=scratch,
            compiler_params=pltpu.CompilerParams(
                collective_id=0, has_side_effects=True, vmem_limit_bytes=60 * 1024 * 1024),
        )(x_loc, w_loc, y_loc, eta_loc.reshape(width // LANES, LANES))

    return jax.shard_map(
        local_solve,
        mesh=mesh,
        in_specs=(P(("prob", "samp"), "feat"), P(("prob", "feat"), None), P(("prob", "samp"), None), P(("prob", "feat"))),
        out_specs=(P(("prob", "feat"), None), P(("prob", "samp"), None)),
        check_vma=False,
    )
```

```python
import functools
import math

import jax
import jax.numpy as jnp
from jax import lax
from jax.experimental import pallas as pl
from jax.experimental.pallas import tpu as pltpu
from jax.sharding import PartitionSpec as P

SWEEPS = 4
COMBINE_WEIGHT = 0.8
RIDGE_SCALE = 0.1
PARTS = 2
LANES = 128
MESH = pl.DeviceIdType.MESH
F32 = jnp.float32
BF16 = jnp.bfloat16


def ridge_kernel(ring, chips, samples, ridge, x_hbm, w_hbm, y_hbm, eta_hbm, wo_hbm, ro_hbm,
                 x, xt, w_in, w, r, eta_in, eta_t, eta, g, rs1, near, far, s1, rs2, dw, u, ur, rb, wo, ro,
                 load_sem, store_sem,
                 rs1_s, rs1_r, rs2_s, rs2_r, ag1_s, ag1_r, ag2_s, ag2_r,
                 u_s, u_r, rg_s, rg_r, wg1_s, wg1_r, wg2_s, wg2_r, rf_s, rf_r):
    samp = lax.axis_index("samp")
    feat = lax.axis_index("feat")
    rows, width = x.shape
    half = width // 2
    group = half // ring
    chunk = group // ring
    piece = rows // (2 * chips)
    cy, cz = lax.rem(samp, ring), lax.div(samp, ring)
    cx, core = lax.div(feat, 2), lax.rem(feat, 2)
    ys = [cy] + [lax.rem(cy + d, ring) for d in range(1, ring)]
    zs = [cz] + [lax.rem(cz + d, ring) for d in range(1, ring)]
    firsts = (ys, zs)
    seconds = (zs, ys)
    neighbour = [[cz * ring + c for c in ys], [c * ring + cy for c in zs]]
    far_first = sorted(range(1, ring), key=lambda d: -min(d, ring - d))
    near_first = far_first[::-1]
    sides = (1, ring - 1)
    hg = group // 2
    across = sorted(range(1, chips), key=lambda d: -min(d, chips - d))
    peers = [(dx, dc) for dx in across + [0] for dc in (0, 1) if dx or dc]

    xs = [cx] + [lax.rem(cx + d, chips) for d in range(1, chips)]
    cores = [core, 1 - core]
    feats = [xs[dx] * 2 + cores[dc] for dx, dc in peers]
    group_rows = [[h * half + c * group for c in firsts[h]] for h in (0, 1)]
    chunk_rows = [[c * chunk for c in seconds[h]] for h in (0, 1)]
    own_chunks = [[group_rows[h][0] + c for c in chunk_rows[h]] for h in (0, 1)]
    piece_rows = [f * piece for f in feats]
    mine = pl.ds(feat * piece, piece)

    def along(axis, d):
        return {"samp": neighbour[axis][d]}

    def remote(src, dst, send, recv, device):
        return pltpu.make_async_remote_copy(
            src_ref=src, dst_ref=dst, send_sem=send, recv_sem=recv, device_id=device, device_id_type=MESH)

    def group_at(h, d):
        return pl.ds(group_rows[h][d], group)

    def part_at(h, e):
        return pl.ds(chunk_rows[h][e], chunk)

    def chunk_at(h, e):
        return pl.ds(own_chunks[h][e], chunk)

    def rs1_copy(p, h, kind, k):
        if kind == 0:
            row, dst = group_rows[h][2] + k * hg, rs1.at[p, h, k]
        elif kind == 1:
            row, dst = group_rows[h][sides[k]] + (1 - k) * hg, near.at[p, h, pl.ds((1 - k) * hg, hg)]
        else:
            row, dst = group_rows[h][sides[k]] + k * hg, far.at[p, h, pl.ds(k * hg, hg)]
        return remote(g.at[p, pl.ds(row, hg)], dst, rs1_s.at[p, h, kind, k], rs1_r.at[p, h, kind, k], along(h, sides[k]))

    def rs2_copy(p, h, d):
        return remote(s1.at[p, h, part_at(h, d)], rs2.at[p, h, d - 1],
                      rs2_s.at[p, h, d - 1], rs2_r.at[p, h, d - 1], along(1 - h, d))

    def gather1(buf, ss, rr, p, h, d):
        at = chunk_at(h, 0)
        return remote(buf.at[p, at], buf.at[p, at], ss.at[p, h, d - 1], rr.at[p, h, d - 1], along(1 - h, d))

    def gather2(buf, ss, rr, p, h, e, k):
        at = chunk_at(h, (ring - e) % ring)
        return remote(buf.at[p, at], buf.at[p, at], ss.at[p, h, 0, e, k], rr.at[p, h, 0, e, k], along(h, sides[k]))

    def gather3(buf, ss, rr, p, h, e, k):
        row = group_rows[h][ring - sides[k]] + chunk_rows[h][(ring - e) % ring] + k * (chunk // 2)
        at = pl.ds(row, chunk // 2)
        return remote(buf.at[p, at], buf.at[p, at], ss.at[p, h, 1, e, k], rr.at[p, h, 1, e, k], along(h, sides[k]))

    def u_copy(p, i):
        return remote(u.at[p, pl.ds(piece_rows[i], piece)], ur.at[p, i], u_s.at[p, i], u_r.at[p, i], {"feat": feats[i]})

    def r_copy(buf, ss, rr, p, i):
        return remote(buf.at[p, mine], buf.at[p, mine], ss.at[p, i], rr.at[p, i], {"feat": feats[i]})

    def start_u(p):
        step = max(rows // 2, piece)
        for k in range(rows // step):
            at = pl.ds(k * step, step)
            u[p, at] = jnp.dot(x[at], dw[p], preferred_element_type=F32).astype(BF16)
        for i in range(len(peers)):
            u_copy(p, i).start()

    def sum_u(p):
        total = u[p, mine].astype(F32)
        for i in range(len(peers)):
            u_copy(p, i).wait_recv()
        for i in range(len(peers)):
            total = total + ur[p, i].astype(F32)
        for i in range(len(peers)):
            u_copy(p, i).wait_send()
        return total

    def send_r(p):
        rb[p, mine] = r[p].astype(BF16)
        for i in range(len(peers)):
            r_copy(rb, rg_s, rg_r, p, i).start()

    def start_g(p):
        for i in range(len(peers)):
            r_copy(rb, rg_s, rg_r, p, i).wait_recv()
        for d in (2, 1, ring - 1, 0):
            for h in (0, 1):
                at = group_at(h, d)
                g[p, at] = jnp.dot(xt[at], rb[p], preferred_element_type=F32)
                for k in (0, 1):
                    if d == 2:
                        rs1_copy(p, h, 0, k).start()
                    elif d == sides[k]:
                        rs1_copy(p, h, 1, k).start()
        for i in range(len(peers)):
            r_copy(rb, rg_s, rg_r, p, i).wait_send()

    def pass_g(p):
        for h in (0, 1):
            for k in (0, 1):
                rs1_copy(p, h, 0, k).wait_recv()
                at = pl.ds(group_rows[h][sides[k]] + k * hg, hg)
                g[p, at] = g[p, at] + rs1[p, h, k]
                rs1_copy(p, h, 2, k).start()

    def mid_g(p):
        for h in (0, 1):
            for k in (0, 1):
                rs1_copy(p, h, 1, k).wait_recv()
                rs1_copy(p, h, 2, k).wait_recv()
            for e in far_first + [0]:
                at = part_at(h, e)
                s1[p, h, at] = g[p, chunk_at(h, e)] + near[p, h, at] + far[p, h, at]
                if e:
                    rs2_copy(p, h, e).start()

    def first_gather(buf, s1_, r1_, s2_, r2_, p, h):
        for d in near_first:
            gather1(buf, s1_, r1_, p, h, d).start()
        for k in (0, 1):
            gather2(buf, s2_, r2_, p, h, 0, k).start()

    def end_g(p, last):
        for h in (0, 1):
            for d in range(1, ring):
                rs2_copy(p, h, d).wait_recv()
            total = s1[p, h, part_at(h, 0)]
            for d in range(1, ring):
                total = total + rs2[p, h, d - 1]
            delta = eta[h] * (total / samples - ridge * w[p, h])
            at = chunk_at(h, 0)
            dw[p, at] = delta.astype(BF16)
            first_gather(*ag, p, h)
            new = w[p, h] + COMBINE_WEIGHT * delta
            w[p, h] = new
            if last:
                wo[p, at] = new

    def relay1(buf, s1_, r1_, s2_, r2_, p):
        for e in near_first:
            for h in (0, 1):
                gather1(buf, s1_, r1_, p, h, e).wait_recv()
                for k in (0, 1):
                    gather2(buf, s2_, r2_, p, h, e, k).start()

    def relay2(buf, s1_, r1_, s2_, r2_, p):
        for e in [0] + near_first:
            for h in (0, 1):
                for k in (0, 1):
                    gather2(buf, s2_, r2_, p, h, e, k).wait_recv()
                    gather3(buf, s2_, r2_, p, h, e, k).start()

    def gathered(buf, s1_, r1_, s2_, r2_, p):
        each = [(h, e, k) for e in [0] + near_first for h in (0, 1) for k in (0, 1)]
        for h, e, k in each:
            gather3(buf, s2_, r2_, p, h, e, k).wait_recv()
        for h in (0, 1):
            for d in near_first:
                gather1(buf, s1_, r1_, p, h, d).wait_send()
        for h, e, k in each:
            gather2(buf, s2_, r2_, p, h, e, k).wait_send()
            gather3(buf, s2_, r2_, p, h, e, k).wait_send()

    def sent_g(p):
        for h in (0, 1):
            for kind in range(3):
                for k in (0, 1):
                    rs1_copy(p, h, kind, k).wait_send()
            for d in range(1, ring):
                rs2_copy(p, h, d).wait_send()

    ag = (dw, ag1_s, ag1_r, ag2_s, ag2_r)
    wg = (wo, wg1_s, wg1_r, wg2_s, wg2_r)

    loads = [pltpu.make_async_copy(w_hbm, w_in, load_sem.at[0]),
             pltpu.make_async_copy(x_hbm, x, load_sem.at[1]),
             pltpu.make_async_copy(eta_hbm, eta_in, load_sem.at[2])]
    loads += [pltpu.make_async_copy(y_hbm.at[mine, pl.ds(p * LANES, LANES)], r.at[p], load_sem.at[3 + p])
              for p in range(PARTS)]
    for load in loads:
        load.start()
    barrier = pltpu.get_barrier_semaphore()
    for d in range(1, ring):
        for axis in (0, 1):
            pl.semaphore_signal(barrier, inc=1, device_id=along(axis, d), device_id_type=MESH)
    for i in range(len(peers)):
        pl.semaphore_signal(barrier, inc=1, device_id={"feat": feats[i]}, device_id_type=MESH)
    loads[0].wait()
    for p in range(PARTS):
        dw[p] = w_in[:, p * LANES:(p + 1) * LANES].astype(BF16)
        for h in (0, 1):
            w[p, h] = w_in[chunk_at(h, 0), p * LANES:(p + 1) * LANES]
    loads[1].wait()
    pl.semaphore_wait(barrier, 2 * (ring - 1) + len(peers))

    for p in range(PARTS):
        start_u(p)
    tile = min(width, 256)
    for k in range(width // tile):
        at = pl.ds(k * tile, tile)
        xt[at] = x[:, k * tile:(k + 1) * tile].T
    loads[2].wait()
    for h in (0, 1):
        pos = own_chunks[h][0]
        line = eta_in[pl.ds(lax.div(pos, LANES), 1), :]
        wide = jnp.broadcast_to(line, (LANES, LANES)).T
        eta_t[...] = wide
        eta[h] = eta_t[pl.ds(lax.rem(pos, LANES), chunk), :]
    for p in range(PARTS):
        loads[3 + p].wait()
        r[p] = r[p] - sum_u(p)
        send_r(p)

    def sweep(last):
        for p in range(PARTS):
            start_g(p)
        for p in range(PARTS):
            pass_g(p)
        for p in range(PARTS):
            mid_g(p)
        for p in range(PARTS):
            end_g(p, last)
        for p in range(PARTS):
            relay1(*ag, p)
        for p in range(PARTS):
            relay2(*ag, p)
        if last:
            for p in range(PARTS):
                for h in (0, 1):
                    first_gather(*wg, p, h)
        for p in range(PARTS):
            sent_g(p)
            gathered(*ag, p)
            start_u(p)
        if last:
            for p in range(PARTS):
                relay1(*wg, p)
        for p in range(PARTS):
            r[p] = r[p] - COMBINE_WEIGHT * sum_u(p)
            if last:
                ro[p, mine] = r[p]
                for i in range(len(peers)):
                    r_copy(ro, rf_s, rf_r, p, i).start()
            else:
                send_r(p)
        if last:
            for p in range(PARTS):
                relay2(*wg, p)

    def body(i, carry):
        sweep(False)
        return carry

    lax.fori_loop(0, SWEEPS - 1, body, 0)
    sweep(True)

    stores = []
    for p in range(PARTS):
        for i in range(len(peers)):
            r_copy(ro, rf_s, rf_r, p, i).wait_recv()
        stores.append(pltpu.make_async_copy(ro.at[p], ro_hbm.at[:, pl.ds(p * LANES, LANES)], store_sem.at[p]))
        stores[-1].start()
    for p in range(PARTS):
        gathered(*wg, p)
        stores.append(pltpu.make_async_copy(wo.at[p], wo_hbm.at[:, pl.ds(p * LANES, LANES)], store_sem.at[PARTS + p]))
        stores[-1].start()
    for p in range(PARTS):
        for i in range(len(peers)):
            r_copy(ro, rf_s, rf_r, p, i).wait_send()
    for store in stores:
        store.wait()


def solution(mesh):
    samp_count = mesh.shape["samp"]
    feat_count = mesh.shape["feat"]
    ring = math.isqrt(samp_count)
    chips = feat_count // 2

    def local_solve(x_loc, w_loc, y_loc, eta_loc):
        rows, width = x_loc.shape
        samples = rows * samp_count
        ridge = RIDGE_SCALE * (width * feat_count) / samples
        group = width // 2 // ring
        chunk = group // ring
        piece = rows // feat_count
        npeer = feat_count - 1
        dma = pltpu.SemaphoreType.DMA
        v = pltpu.VMEM
        scratch = [
            v((rows, width), BF16),
            v((width, rows), BF16),
            v((width, PARTS * LANES), F32),
            v((PARTS, 2, chunk, LANES), F32),
            v((PARTS, piece, LANES), F32),
            v((width // LANES, LANES), F32),
            v((LANES, LANES), F32),
            v((2, chunk, LANES), F32),
            v((PARTS, width, LANES), F32),
            v((PARTS, 2, 2, group // 2, LANES), F32),
            v((PARTS, 2, group, LANES), F32),
            v((PARTS, 2, group, LANES), F32),
            v((PARTS, 2, group, LANES), F32),
            v((PARTS, 2, ring - 1, chunk, LANES), F32),
            v((PARTS, width, LANES), BF16),
            v((PARTS, rows, LANES), BF16),
            v((PARTS, npeer, piece, LANES), BF16),
            v((PARTS, rows, LANES), BF16),
            v((PARTS, width, LANES), F32),
            v((PARTS, rows, LANES), F32),
            dma((3 + PARTS,)), dma((2 * PARTS,)),
        ]
        step1 = (PARTS, 2, ring - 1)
        step2 = (PARTS, 2, 2, ring, 2)
        scratch += [dma((PARTS, 2, 3, 2))] * 2 + [dma(step1)] * 4 + [dma(step2)] * 2 + [dma((PARTS, npeer))] * 4
        scratch += [dma(step1)] * 2 + [dma(step2)] * 2 + [dma((PARTS, npeer))] * 2
        return pl.pallas_call(
            functools.partial(ridge_kernel, ring, chips, samples, ridge),
            out_shape=[jax.ShapeDtypeStruct(w_loc.shape, F32), jax.ShapeDtypeStruct(y_loc.shape, F32)],
            in_specs=[pl.BlockSpec(memory_space=pl.ANY)] * 4,
            out_specs=[pl.BlockSpec(memory_space=pl.ANY)] * 2,
            scratch_shapes=scratch,
            compiler_params=pltpu.CompilerParams(
                collective_id=0, has_side_effects=True, vmem_limit_bytes=60 * 1024 * 1024),
        )(x_loc, w_loc, y_loc, eta_loc.reshape(width // LANES, LANES))

    return jax.shard_map(
        local_solve,
        mesh=mesh,
        in_specs=(P(("prob", "samp"), "feat"), P(("prob", "feat"), None), P(("prob", "samp"), None), P(("prob", "feat"))),
        out_specs=(P(("prob", "feat"), None), P(("prob", "samp"), None)),
        check_vma=False,
    )
```

```python
import functools
import math

import jax
import jax.numpy as jnp
from jax import lax
from jax.experimental import pallas as pl
from jax.experimental.pallas import tpu as pltpu
from jax.sharding import PartitionSpec as P

SWEEPS = 4
COMBINE_WEIGHT = 0.8
RIDGE_SCALE = 0.1
PARTS = 2
LANES = 128
QUARTERS = 4
UNITS = ((0, 1), (2, 3))
MESH = pl.DeviceIdType.MESH
F32 = jnp.float32
BF16 = jnp.bfloat16


def ridge_kernel(ring, chips, samples, ridge, x_hbm, w_hbm, y_hbm, eta_hbm, wo, ro,
                 x, xt, w_in, w, r, eta_in, eta_t, eta, g, rs1, near, far, s1, rs2, dw, u, ur, rb,
                 load_sem, rl_r, nf_r, rs2_r, gs_s, ag1_r, ag2_r, ag3_r, ag_s,
                 u_s, u_r, rg_s, rg_r, wg1_r, wg2_r, wg3_r, wg_s, rf_s, rf_r):
    samp = lax.axis_index("samp")
    feat = lax.axis_index("feat")
    rows, width = x.shape
    quarter = width // QUARTERS
    group = quarter // ring
    chunk = group // ring
    hg = group // 2
    piece = rows // (2 * chips)
    cy, cz = lax.rem(samp, ring), lax.div(samp, ring)
    cx, core = lax.div(feat, 2), lax.rem(feat, 2)
    ys = [cy] + [lax.rem(cy + d, ring) for d in range(1, ring)]
    zs = [cz] + [lax.rem(cz + d, ring) for d in range(1, ring)]
    neighbour = [[cz * ring + c for c in ys], [c * ring + cy for c in zs]]
    far_first = sorted(range(1, ring), key=lambda d: -min(d, ring - d))
    near_first = far_first[::-1]
    sides = (1, ring - 1)
    across = sorted(range(1, chips), key=lambda d: -min(d, chips - d))
    peers = [(dx, dc) for dx in across + [0] for dc in (0, 1) if dx or dc]
    xs = [cx] + [lax.rem(cx + d, chips) for d in range(1, chips)]
    cores = [core, 1 - core]
    feats = [xs[dx] * 2 + cores[dc] for dx, dc in peers]
    firsts = [(ys, zs)[h % 2] for h in range(QUARTERS)]
    seconds = [(zs, ys)[h % 2] for h in range(QUARTERS)]
    group_rows = [[h * quarter + c * group for c in firsts[h]] for h in range(QUARTERS)]
    chunk_rows = [[c * chunk for c in seconds[h]] for h in range(QUARTERS)]
    own_chunks = [[group_rows[h][0] + c for c in chunk_rows[h]] for h in range(QUARTERS)]
    piece_rows = [f * piece for f in feats]
    mine = pl.ds(feat * piece, piece)
    everything = tuple(range(QUARTERS))

    def along(axis, d):
        return {"samp": neighbour[axis % 2][d]}

    def remote(src, dst, send, recv, device):
        return pltpu.make_async_remote_copy(
            src_ref=src, dst_ref=dst, send_sem=send, recv_sem=recv, device_id=device, device_id_type=MESH)

    def drain(ref, sem):
        pltpu.make_async_copy(ref, ref, sem).wait()

    def group_at(h, d):
        return pl.ds(group_rows[h][d], group)

    def part_at(h, e):
        return pl.ds(chunk_rows[h][e], chunk)

    def chunk_at(h, e):
        return pl.ds(own_chunks[h][e], chunk)

    def columns(p):
        return pl.ds(p * LANES, LANES)

    def rs1_copy(p, h, kind, k):
        if kind == 0:
            row, dst, sem = group_rows[h][2] + k * hg, rs1.at[p, h, k], rl_r.at[p, h, k]
        elif kind == 1:
            row, dst, sem = group_rows[h][sides[k]] + (1 - k) * hg, near.at[p, h, pl.ds((1 - k) * hg, hg)], nf_r.at[p, h]
        else:
            row, dst, sem = group_rows[h][sides[k]] + k * hg, far.at[p, h, pl.ds(k * hg, hg)], nf_r.at[p, h]
        return remote(g.at[p, pl.ds(row, hg)], dst, gs_s.at[p], sem, along(h, sides[k]))

    def rs2_copy(p, h, d):
        return remote(s1.at[p, h, part_at(h, d)], rs2.at[p, h, d - 1], gs_s.at[p], rs2_r.at[p, h], along(h + 1, d))

    def u_copy(p, i):
        return remote(u.at[p, pl.ds(piece_rows[i], piece)], ur.at[p, i], u_s.at[p], u_r.at[p], {"feat": feats[i]})

    def r_copy(ref, ss, rr, p, i):
        return remote(ref, ref, ss.at[p], rr.at[p], {"feat": feats[i]})

    class Gather:
        def __init__(self, view, r1, r2, r3, s):
            self.view, self.r1, self.r2, self.r3, self.s = view, r1, r2, r3, s

        def first(self, p, h):
            ref = self.view(p, chunk_at(h, 0))
            for d in near_first:
                remote(ref, ref, self.s.at[p], self.r1.at[p, h], along(h + 1, d)).start()

        def second(self, p, h):
            drain(self.view(p, pl.ds(0, (ring - 1) * chunk)), self.r1.at[p, h])
            ref = self.view(p, group_at(h, 0))
            for k in (0, 1):
                remote(ref, ref, self.s.at[p], self.r2.at[p, h, k], along(h, sides[k])).start()

        def third(self, p, h):
            for k in (0, 1):
                drain(self.view(p, pl.ds(0, group)), self.r2.at[p, h, k])
                ref = self.view(p, pl.ds(group_rows[h][ring - sides[k]] + k * hg, hg))
                remote(ref, ref, self.s.at[p], self.r3.at[p, h], along(h, sides[k])).start()

        def last(self, p, h):
            drain(self.view(p, pl.ds(0, group)), self.r3.at[p, h])

        def sent(self, p):
            drain(self.view(p, pl.ds(0, QUARTERS * ((ring - 1) * chunk + 3 * group))), self.s.at[p])

    ag = Gather(lambda p, at: dw.at[p, at], ag1_r, ag2_r, ag3_r, ag_s)
    wg = Gather(lambda p, at: wo.at[at, columns(p)], wg1_r, wg2_r, wg3_r, wg_s)

    def start_u(p):
        step = max(rows // 2, piece)
        for k in range(rows // step):
            at = pl.ds(k * step, step)
            u[p, at] = jnp.dot(x[at], dw[p], preferred_element_type=F32).astype(BF16)
        for i in range(len(peers)):
            u_copy(p, i).start()

    def sum_u(p):
        total = u[p, mine].astype(F32)
        drain(ur.at[p], u_r.at[p])
        for i in range(len(peers)):
            total = total + ur[p, i].astype(F32)
        drain(ur.at[p], u_s.at[p])
        return total

    def send_r(p):
        rb[p, mine] = r[p].astype(BF16)
        for i in range(len(peers)):
            r_copy(rb.at[p, mine], rg_s, rg_r, p, i).start()

    def start_g(p, hs):
        if hs == UNITS[0]:
            drain(ur.at[p], rg_r.at[p])
        for ds in ((2,), (1, ring - 1), (0,)):
            for d in ds:
                for h in hs:
                    at = group_at(h, d)
                    g[p, at] = jnp.dot(xt[at], rb[p], preferred_element_type=F32)
            for h in hs:
                for k in (0, 1):
                    if ds[0] == 2:
                        rs1_copy(p, h, 0, k).start()
                    elif ds[0]:
                        rs1_copy(p, h, 1, k).start()

    def pass_g(p, hs):
        for h in hs:
            for k in (0, 1):
                rs1_copy(p, h, 0, k).wait_recv()
                at = pl.ds(group_rows[h][sides[k]] + k * hg, hg)
                g[p, at] = g[p, at] + rs1[p, h, k]
                rs1_copy(p, h, 2, k).start()

    def mid_g(p, hs):
        for h in hs:
            drain(g.at[p, pl.ds(0, 2 * group)], nf_r.at[p, h])
            for e in far_first + [0]:
                at = part_at(h, e)
                s1[p, h, at] = g[p, chunk_at(h, e)] + near[p, h, at] + far[p, h, at]
                if e:
                    rs2_copy(p, h, e).start()

    def end_g(p, hs, last):
        for h in hs:
            drain(g.at[p, pl.ds(0, (ring - 1) * chunk)], rs2_r.at[p, h])
            total = s1[p, h, part_at(h, 0)]
            for d in range(1, ring):
                total = total + rs2[p, h, d - 1]
            delta = eta[h] * (total / samples - ridge * w[p, h])
            at = chunk_at(h, 0)
            dw[p, at] = delta.astype(BF16)
            ag.first(p, h)
            new = w[p, h] + COMBINE_WEIGHT * delta
            w[p, h] = new
            if last:
                wo[at, p * LANES:(p + 1) * LANES] = new

    loads = [pltpu.make_async_copy(w_hbm, w_in, load_sem.at[0]),
             pltpu.make_async_copy(x_hbm, x, load_sem.at[1]),
             pltpu.make_async_copy(eta_hbm, eta_in, load_sem.at[2])]
    loads += [pltpu.make_async_copy(y_hbm.at[mine, columns(p)], r.at[p], load_sem.at[3 + p]) for p in range(PARTS)]
    for load in loads:
        load.start()
    barrier = pltpu.get_barrier_semaphore()
    for d in range(1, ring):
        for axis in (0, 1):
            pl.semaphore_signal(barrier, inc=1, device_id=along(axis, d), device_id_type=MESH)
    for i in range(len(peers)):
        pl.semaphore_signal(barrier, inc=1, device_id={"feat": feats[i]}, device_id_type=MESH)
    loads[0].wait()
    for p in range(PARTS):
        dw[p] = w_in[:, p * LANES:(p + 1) * LANES].astype(BF16)
        for h in everything:
            w[p, h] = w_in[chunk_at(h, 0), p * LANES:(p + 1) * LANES]
    loads[1].wait()
    pl.semaphore_wait(barrier, 2 * (ring - 1) + len(peers))

    for p in range(PARTS):
        start_u(p)
    tile = min(width, 256)
    for k in range(width // tile):
        xt[k * tile:(k + 1) * tile] = x[:, k * tile:(k + 1) * tile].T
    loads[2].wait()
    for h in everything:
        pos = own_chunks[h][0]
        line = eta_in[pl.ds(lax.div(pos, LANES), 1), :]
        eta_t[...] = jnp.broadcast_to(line, (LANES, LANES)).T
        eta[h] = eta_t[pl.ds(lax.rem(pos, LANES), chunk), :]
    for p in range(PARTS):
        loads[3 + p].wait()
        r[p] = r[p] - sum_u(p)
        send_r(p)

    def sweep(last):
        both = [(p, hs) for p in range(PARTS) for hs in UNITS]
        for p, hs in both:
            start_g(p, hs)
        for p in range(PARTS):
            drain(ur.at[p], rg_s.at[p])
        for p, hs in both:
            pass_g(p, hs)
        for p, hs in both:
            mid_g(p, hs)
        for p, hs in both:
            end_g(p, hs, last)
        for p, hs in both:
            for h in hs:
                ag.second(p, h)
        for p, hs in both:
            for h in hs:
                ag.third(p, h)
        if last:
            for p in range(PARTS):
                for h in everything:
                    wg.first(p, h)
        for p in range(PARTS):
            drain(g.at[p, pl.ds(0, QUARTERS * (3 * group + (ring - 1) * chunk))], gs_s.at[p])
            for h in everything:
                ag.last(p, h)
            ag.sent(p)
            start_u(p)
        if last:
            for p in range(PARTS):
                for h in everything:
                    wg.second(p, h)
        for p in range(PARTS):
            r[p] = r[p] - COMBINE_WEIGHT * sum_u(p)
            if last:
                ro[mine, p * LANES:(p + 1) * LANES] = r[p]
                for i in range(len(peers)):
                    r_copy(ro.at[mine, columns(p)], rf_s, rf_r, p, i).start()
            else:
                send_r(p)
        if last:
            for p in range(PARTS):
                for h in everything:
                    wg.third(p, h)

    def body(i, carry):
        sweep(False)
        return carry

    lax.fori_loop(0, SWEEPS - 1, body, 0)
    sweep(True)
    for p in range(PARTS):
        final = ro.at[pl.ds(0, len(peers) * piece), columns(p)]
        drain(final, rf_r.at[p])
        drain(final, rf_s.at[p])
    for p in range(PARTS):
        for h in everything:
            wg.last(p, h)
        wg.sent(p)


def solution(mesh):
    samp_count = mesh.shape["samp"]
    feat_count = mesh.shape["feat"]
    ring = math.isqrt(samp_count)
    chips = feat_count // 2

    def local_solve(x_loc, w_loc, y_loc, eta_loc):
        rows, width = x_loc.shape
        samples = rows * samp_count
        ridge = RIDGE_SCALE * (width * feat_count) / samples
        group = width // QUARTERS // ring
        chunk = group // ring
        piece = rows // feat_count
        npeer = feat_count - 1
        dma = pltpu.SemaphoreType.DMA
        v = pltpu.VMEM
        each = (PARTS, QUARTERS)
        scratch = [
            v((rows, width), BF16),
            v((width, rows), BF16),
            v((width, PARTS * LANES), F32),
            v(each + (chunk, LANES), F32),
            v((PARTS, piece, LANES), F32),
            v((width // LANES, LANES), F32),
            v((LANES, LANES), F32),
            v((QUARTERS, chunk, LANES), F32),
            v((PARTS, width, LANES), F32),
            v(each + (2, group // 2, LANES), F32),
            v(each + (group, LANES), F32),
            v(each + (group, LANES), F32),
            v(each + (group, LANES), F32),
            v(each + (ring - 1, chunk, LANES), F32),
            v((PARTS, width, LANES), BF16),
            v((PARTS, rows, LANES), BF16),
            v((PARTS, npeer, piece, LANES), BF16),
            v((PARTS, rows, LANES), BF16),
            dma((3 + PARTS,)),
            dma(each + (2,)), dma(each), dma(each), dma((PARTS,)),
            dma(each), dma(each + (2,)), dma(each), dma((PARTS,)),
            dma((PARTS,)), dma((PARTS,)), dma((PARTS,)), dma((PARTS,)),
            dma(each), dma(each + (2,)), dma(each), dma((PARTS,)),
            dma((PARTS,)), dma((PARTS,)),
        ]
        return pl.pallas_call(
            functools.partial(ridge_kernel, ring, chips, samples, ridge),
            out_shape=[pltpu.VMEM(w_loc.shape, F32), pltpu.VMEM(y_loc.shape, F32)],
            in_specs=[pl.BlockSpec(memory_space=pltpu.HBM)] * 4,
            out_specs=[pl.BlockSpec(memory_space=pltpu.VMEM)] * 2,
            scratch_shapes=scratch,
            compiler_params=pltpu.CompilerParams(
                collective_id=0, has_side_effects=True, vmem_limit_bytes=56 * 1024 * 1024),
        )(x_loc, w_loc, y_loc, eta_loc.reshape(width // LANES, LANES))

    return jax.shard_map(
        local_solve,
        mesh=mesh,
        in_specs=(P(("prob", "samp"), "feat"), P(("prob", "feat"), None), P(("prob", "samp"), None), P(("prob", "feat"))),
        out_specs=(P(("prob", "feat"), None), P(("prob", "samp"), None)),
        check_vma=False,
    )
```

```python
import functools
import math

import jax
import jax.numpy as jnp
from jax import lax
from jax.experimental import pallas as pl
from jax.experimental.pallas import tpu as pltpu
from jax.sharding import PartitionSpec as P

SWEEPS = 4
COMBINE_WEIGHT = 0.8
RIDGE_SCALE = 0.1
PARTS = 2
LANES = 128
QUARTERS = 4
UNITS = ((0, 1), (2, 3))
MESH = pl.DeviceIdType.MESH
F32 = jnp.float32
BF16 = jnp.bfloat16


def ridge_kernel(ring, chips, samples, ridge, x_hbm, w_hbm, y_hbm, eta_hbm, wo, ro,
                 x, xt, w_in, w, r, eta_in, eta_t, eta, g, rs1, near, far, s1, rs2, dw, u, ur, rb,
                 load_sem, rl_r, nf_r, rs2_r, gs_s, ag1_r, ag3_r, ag_s,
                 u_s, u_r, rg_s, rg_r, wg1_r, wg2_r, wg3_r, wg_s, rf_s, rf_r):
    samp = lax.axis_index("samp")
    feat = lax.axis_index("feat")
    rows, width = x.shape
    quarter = width // QUARTERS
    group = quarter // ring
    chunk = group // ring
    hg = group // 2
    piece = rows // (2 * chips)
    cy, cz = lax.rem(samp, ring), lax.div(samp, ring)
    cx, core = lax.div(feat, 2), lax.rem(feat, 2)
    ys = [cy] + [lax.rem(cy + d, ring) for d in range(1, ring)]
    zs = [cz] + [lax.rem(cz + d, ring) for d in range(1, ring)]
    neighbour = [[cz * ring + c for c in ys], [c * ring + cy for c in zs]]
    far_first = sorted(range(1, ring), key=lambda d: -min(d, ring - d))
    near_first = far_first[::-1]
    sides = (1, ring - 1)
    across = sorted(range(1, chips), key=lambda d: -min(d, chips - d))
    peers = [(dx, dc) for dx in across + [0] for dc in (0, 1) if dx or dc]
    xs = [cx] + [lax.rem(cx + d, chips) for d in range(1, chips)]
    cores = [core, 1 - core]
    feats = [xs[dx] * 2 + cores[dc] for dx, dc in peers]
    firsts = [(ys, zs)[h % 2] for h in range(QUARTERS)]
    seconds = [(zs, ys)[h % 2] for h in range(QUARTERS)]
    group_rows = [[h * quarter + c * group for c in firsts[h]] for h in range(QUARTERS)]
    chunk_rows = [[c * chunk for c in seconds[h]] for h in range(QUARTERS)]
    own_chunks = [[group_rows[h][0] + c for c in chunk_rows[h]] for h in range(QUARTERS)]
    piece_rows = [f * piece for f in feats]
    mine = pl.ds(feat * piece, piece)
    everything = tuple(range(QUARTERS))

    def along(axis, d):
        return {"samp": neighbour[axis % 2][d]}

    def remote(src, dst, send, recv, device):
        return pltpu.make_async_remote_copy(
            src_ref=src, dst_ref=dst, send_sem=send, recv_sem=recv, device_id=device, device_id_type=MESH)

    def drain(ref, sem):
        pltpu.make_async_copy(ref, ref, sem).wait()

    def group_at(h, d):
        return pl.ds(group_rows[h][d], group)

    def part_at(h, e):
        return pl.ds(chunk_rows[h][e], chunk)

    def chunk_at(h, e):
        return pl.ds(own_chunks[h][e], chunk)

    def columns(p):
        return pl.ds(p * LANES, LANES)

    def rs1_copy(p, h, kind, k):
        if kind == 0:
            row, dst, sem = group_rows[h][2] + k * hg, rs1.at[p, h, k], rl_r.at[p, h, k]
        elif kind == 1:
            row, dst, sem = group_rows[h][sides[k]] + (1 - k) * hg, near.at[p, h, pl.ds((1 - k) * hg, hg)], nf_r.at[p, h]
        else:
            row, dst, sem = group_rows[h][sides[k]] + k * hg, far.at[p, h, pl.ds(k * hg, hg)], nf_r.at[p, h]
        return remote(g.at[p, pl.ds(row, hg)], dst, gs_s.at[p], sem, along(h, sides[k]))

    def rs2_copy(p, h, d):
        return remote(s1.at[p, h, part_at(h, d)], rs2.at[p, h, d - 1], gs_s.at[p], rs2_r.at[p, h], along(h + 1, d))

    def u_copy(p, i):
        return remote(u.at[p, pl.ds(piece_rows[i], piece)], ur.at[p, i], u_s.at[p], u_r.at[p], {"feat": feats[i]})

    def r_copy(ref, ss, rr, p, i):
        return remote(ref, ref, ss.at[p], rr.at[p], {"feat": feats[i]})

    class Gather:
        def __init__(self, view, r1, r2, r3, s):
            self.view, self.r1, self.r2, self.r3, self.s = view, r1, r2, r3, s

        def first(self, p, h):
            ref = self.view(p, chunk_at(h, 0))
            for d in near_first:
                remote(ref, ref, self.s.at[p], self.r1.at[p, h], along(h + 1, d)).start()

        def second(self, p, h):
            drain(self.view(p, pl.ds(0, (ring - 1) * chunk)), self.r1.at[p, h])
            ref = self.view(p, group_at(h, 0))
            if self.r2 is None:
                for d in far_first:
                    remote(ref, ref, self.s.at[p], self.r3.at[p, h], along(h, d)).start()
            else:
                for k in (0, 1):
                    remote(ref, ref, self.s.at[p], self.r2.at[p, h, k], along(h, sides[k])).start()

        def third(self, p, h):
            for k in (0, 1):
                drain(self.view(p, pl.ds(0, group)), self.r2.at[p, h, k])
                ref = self.view(p, pl.ds(group_rows[h][ring - sides[k]] + k * hg, hg))
                remote(ref, ref, self.s.at[p], self.r3.at[p, h], along(h, sides[k])).start()

        def last(self, p, h):
            drain(self.view(p, pl.ds(0, group if self.r2 is not None else (ring - 1) * group)), self.r3.at[p, h])

        def sent(self, p):
            drain(self.view(p, pl.ds(0, QUARTERS * ((ring - 1) * chunk + 3 * group))), self.s.at[p])

    ag = Gather(lambda p, at: dw.at[p, at], ag1_r, None, ag3_r, ag_s)
    wg = Gather(lambda p, at: wo.at[at, columns(p)], wg1_r, wg2_r, wg3_r, wg_s)

    def start_u(p):
        step = max(rows // 2, piece)
        for k in range(rows // step):
            at = pl.ds(k * step, step)
            u[p, at] = jnp.dot(x[at], dw[p], preferred_element_type=F32).astype(BF16)
        for i in range(len(peers)):
            u_copy(p, i).start()

    def sum_u(p):
        total = u[p, mine].astype(F32)
        drain(ur.at[p], u_r.at[p])
        for i in range(len(peers)):
            total = total + ur[p, i].astype(F32)
        drain(ur.at[p], u_s.at[p])
        return total

    def send_r(p):
        rb[p, mine] = r[p].astype(BF16)
        for i in range(len(peers)):
            r_copy(rb.at[p, mine], rg_s, rg_r, p, i).start()

    def start_g(p, hs):
        if hs == UNITS[0]:
            drain(ur.at[p], rg_r.at[p])
        for ds in ((2,), (1, ring - 1), (0,)):
            for d in ds:
                for h in hs:
                    at = group_at(h, d)
                    g[p, at] = jnp.dot(xt[at], rb[p], preferred_element_type=F32)
            for h in hs:
                for k in (0, 1):
                    if ds[0] == 2:
                        rs1_copy(p, h, 0, k).start()
                    elif ds[0]:
                        rs1_copy(p, h, 1, k).start()

    def pass_g(p, hs):
        for h in hs:
            for k in (0, 1):
                rs1_copy(p, h, 0, k).wait_recv()
                at = pl.ds(group_rows[h][sides[k]] + k * hg, hg)
                g[p, at] = g[p, at] + rs1[p, h, k]
                rs1_copy(p, h, 2, k).start()

    def mid_g(p, hs):
        for h in hs:
            drain(g.at[p, pl.ds(0, 2 * group)], nf_r.at[p, h])
            for e in far_first + [0]:
                at = part_at(h, e)
                s1[p, h, at] = g[p, chunk_at(h, e)] + near[p, h, at] + far[p, h, at]
                if e:
                    rs2_copy(p, h, e).start()

    def end_g(p, hs, last):
        for h in hs:
            drain(g.at[p, pl.ds(0, (ring - 1) * chunk)], rs2_r.at[p, h])
            total = s1[p, h, part_at(h, 0)]
            for d in range(1, ring):
                total = total + rs2[p, h, d - 1]
            delta = eta[h] * (total / samples - ridge * w[p, h])
            at = chunk_at(h, 0)
            dw[p, at] = delta.astype(BF16)
            ag.first(p, h)
            new = w[p, h] + COMBINE_WEIGHT * delta
            w[p, h] = new
            if last:
                wo[at, p * LANES:(p + 1) * LANES] = new

    loads = [pltpu.make_async_copy(w_hbm, w_in, load_sem.at[0]),
             pltpu.make_async_copy(x_hbm, x, load_sem.at[1]),
             pltpu.make_async_copy(eta_hbm, eta_in, load_sem.at[2])]
    loads += [pltpu.make_async_copy(y_hbm.at[mine, columns(p)], r.at[p], load_sem.at[3 + p]) for p in range(PARTS)]
    for load in loads:
        load.start()
    barrier = pltpu.get_barrier_semaphore()
    for d in range(1, ring):
        for axis in (0, 1):
            pl.semaphore_signal(barrier, inc=1, device_id=along(axis, d), device_id_type=MESH)
    for i in range(len(peers)):
        pl.semaphore_signal(barrier, inc=1, device_id={"feat": feats[i]}, device_id_type=MESH)
    loads[0].wait()
    for p in range(PARTS):
        dw[p] = w_in[:, p * LANES:(p + 1) * LANES].astype(BF16)
        for h in everything:
            w[p, h] = w_in[chunk_at(h, 0), p * LANES:(p + 1) * LANES]
    loads[1].wait()
    pl.semaphore_wait(barrier, 2 * (ring - 1) + len(peers))

    for p in range(PARTS):
        start_u(p)
    tile = min(width, 256)
    for k in range(width // tile):
        xt[k * tile:(k + 1) * tile] = x[:, k * tile:(k + 1) * tile].T
    loads[2].wait()
    for h in everything:
        pos = own_chunks[h][0]
        line = eta_in[pl.ds(lax.div(pos, LANES), 1), :]
        eta_t[...] = jnp.broadcast_to(line, (LANES, LANES)).T
        eta[h] = eta_t[pl.ds(lax.rem(pos, LANES), chunk), :]
    for p in range(PARTS):
        loads[3 + p].wait()
        r[p] = r[p] - sum_u(p)
        send_r(p)

    def sweep(last):
        both = [(p, hs) for p in range(PARTS) for hs in UNITS]
        for p, hs in both:
            start_g(p, hs)
        for p in range(PARTS):
            drain(ur.at[p], rg_s.at[p])
        for p, hs in both:
            pass_g(p, hs)
        for p, hs in both:
            mid_g(p, hs)
        for p, hs in both:
            end_g(p, hs, last)
        for p, hs in both:
            for h in hs:
                ag.second(p, h)
        if last:
            for p in range(PARTS):
                for h in everything:
                    wg.first(p, h)
        for p in range(PARTS):
            drain(g.at[p, pl.ds(0, QUARTERS * (3 * group + (ring - 1) * chunk))], gs_s.at[p])
            for h in everything:
                ag.last(p, h)
            ag.sent(p)
            start_u(p)
        if last:
            for p in range(PARTS):
                for h in everything:
                    wg.second(p, h)
        for p in range(PARTS):
            r[p] = r[p] - COMBINE_WEIGHT * sum_u(p)
            if last:
                ro[mine, p * LANES:(p + 1) * LANES] = r[p]
                for i in range(len(peers)):
                    r_copy(ro.at[mine, columns(p)], rf_s, rf_r, p, i).start()
            else:
                send_r(p)
        if last:
            for p in range(PARTS):
                for h in everything:
                    wg.third(p, h)

    def body(i, carry):
        sweep(False)
        return carry

    lax.fori_loop(0, SWEEPS - 1, body, 0)
    sweep(True)
    for p in range(PARTS):
        final = ro.at[pl.ds(0, len(peers) * piece), columns(p)]
        drain(final, rf_r.at[p])
        drain(final, rf_s.at[p])
    for p in range(PARTS):
        for h in everything:
            wg.last(p, h)
        wg.sent(p)


def solution(mesh):
    samp_count = mesh.shape["samp"]
    feat_count = mesh.shape["feat"]
    ring = math.isqrt(samp_count)
    chips = feat_count // 2

    def local_solve(x_loc, w_loc, y_loc, eta_loc):
        rows, width = x_loc.shape
        samples = rows * samp_count
        ridge = RIDGE_SCALE * (width * feat_count) / samples
        group = width // QUARTERS // ring
        chunk = group // ring
        piece = rows // feat_count
        npeer = feat_count - 1
        dma = pltpu.SemaphoreType.DMA
        v = pltpu.VMEM
        each = (PARTS, QUARTERS)
        scratch = [
            v((rows, width), BF16),
            v((width, rows), BF16),
            v((width, PARTS * LANES), F32),
            v(each + (chunk, LANES), F32),
            v((PARTS, piece, LANES), F32),
            v((width // LANES, LANES), F32),
            v((LANES, LANES), F32),
            v((QUARTERS, chunk, LANES), F32),
            v((PARTS, width, LANES), F32),
            v(each + (2, group // 2, LANES), F32),
            v(each + (group, LANES), F32),
            v(each + (group, LANES), F32),
            v(each + (group, LANES), F32),
            v(each + (ring - 1, chunk, LANES), F32),
            v((PARTS, width, LANES), BF16),
            v((PARTS, rows, LANES), BF16),
            v((PARTS, npeer, piece, LANES), BF16),
            v((PARTS, rows, LANES), BF16),
            dma((3 + PARTS,)),
            dma(each + (2,)), dma(each), dma(each), dma((PARTS,)),
            dma(each), dma(each), dma((PARTS,)),
            dma((PARTS,)), dma((PARTS,)), dma((PARTS,)), dma((PARTS,)),
            dma(each), dma(each + (2,)), dma(each), dma((PARTS,)),
            dma((PARTS,)), dma((PARTS,)),
        ]
        return pl.pallas_call(
            functools.partial(ridge_kernel, ring, chips, samples, ridge),
            out_shape=[pltpu.VMEM(w_loc.shape, F32), pltpu.VMEM(y_loc.shape, F32)],
            in_specs=[pl.BlockSpec(memory_space=pltpu.HBM)] * 4,
            out_specs=[pl.BlockSpec(memory_space=pltpu.VMEM)] * 2,
            scratch_shapes=scratch,
            compiler_params=pltpu.CompilerParams(
                collective_id=0, has_side_effects=True, vmem_limit_bytes=56 * 1024 * 1024),
        )(x_loc, w_loc, y_loc, eta_loc.reshape(width // LANES, LANES))

    return jax.shard_map(
        local_solve,
        mesh=mesh,
        in_specs=(P(("prob", "samp"), "feat"), P(("prob", "feat"), None), P(("prob", "samp"), None), P(("prob", "feat"))),
        out_specs=(P(("prob", "feat"), None), P(("prob", "samp"), None)),
        check_vma=False,
    )
```

```python
import functools
import math

import jax
import jax.numpy as jnp
from jax import lax
from jax.experimental import pallas as pl
from jax.experimental.pallas import tpu as pltpu
from jax.sharding import PartitionSpec as P

SWEEPS = 4
COMBINE_WEIGHT = 0.8
RIDGE_SCALE = 0.1
PARTS = 2
LANES = 128
QUARTERS = 4
UNITS = ((0, 1), (2, 3))
MESH = pl.DeviceIdType.MESH
F32 = jnp.float32
BF16 = jnp.bfloat16


def ridge_kernel(ring, chips, samples, ridge, x_hbm, w_hbm, y_hbm, eta_hbm, wo, ro,
                 x, xt, w_in, w, r, eta_in, eta_t, eta, g, rs1, s1, rs2, dw, u, ur, rb,
                 load_sem, rs1_r, rs2_r, gs_s, ag1_r, ag3_r, ag_s,
                 u_s, u_r, rg_s, rg_r, wg1_r, wg2_r, wg3_r, wg_s, rf_s, rf_r):
    samp = lax.axis_index("samp")
    feat = lax.axis_index("feat")
    rows, width = x.shape
    quarter = width // QUARTERS
    group = quarter // ring
    chunk = group // ring
    hg = group // 2
    piece = rows // (2 * chips)
    cy, cz = lax.rem(samp, ring), lax.div(samp, ring)
    cx, core = lax.div(feat, 2), lax.rem(feat, 2)
    ys = [cy] + [lax.rem(cy + d, ring) for d in range(1, ring)]
    zs = [cz] + [lax.rem(cz + d, ring) for d in range(1, ring)]
    neighbour = [[cz * ring + c for c in ys], [c * ring + cy for c in zs]]
    far_first = sorted(range(1, ring), key=lambda d: -min(d, ring - d))
    near_first = far_first[::-1]
    sides = (1, ring - 1)
    across = sorted(range(1, chips), key=lambda d: -min(d, chips - d))
    peers = [(dx, dc) for dx in across + [0] for dc in (0, 1) if dx or dc]
    xs = [cx] + [lax.rem(cx + d, chips) for d in range(1, chips)]
    cores = [core, 1 - core]
    feats = [xs[dx] * 2 + cores[dc] for dx, dc in peers]
    firsts = [(ys, zs)[h % 2] for h in range(QUARTERS)]
    seconds = [(zs, ys)[h % 2] for h in range(QUARTERS)]
    group_rows = [[h * quarter + c * group for c in firsts[h]] for h in range(QUARTERS)]
    chunk_rows = [[c * chunk for c in seconds[h]] for h in range(QUARTERS)]
    own_chunks = [[group_rows[h][0] + c for c in chunk_rows[h]] for h in range(QUARTERS)]
    piece_rows = [f * piece for f in feats]
    mine = pl.ds(feat * piece, piece)
    everything = tuple(range(QUARTERS))

    def along(axis, d):
        return {"samp": neighbour[axis % 2][d]}

    def remote(src, dst, send, recv, device):
        return pltpu.make_async_remote_copy(
            src_ref=src, dst_ref=dst, send_sem=send, recv_sem=recv, device_id=device, device_id_type=MESH)

    def drain(ref, sem):
        pltpu.make_async_copy(ref, ref, sem).wait()

    def group_at(h, d):
        return pl.ds(group_rows[h][d], group)

    def part_at(h, e):
        return pl.ds(chunk_rows[h][e], chunk)

    def chunk_at(h, e):
        return pl.ds(own_chunks[h][e], chunk)

    def columns(p):
        return pl.ds(p * LANES, LANES)

    def rs1_copy(p, h, d):
        return remote(g.at[p, group_at(h, d)], rs1.at[p, h, d - 1], gs_s.at[p], rs1_r.at[p, h], along(h, d))

    def rs2_copy(p, h, d):
        return remote(s1.at[p, h, part_at(h, d)], rs2.at[p, h, d - 1], gs_s.at[p], rs2_r.at[p, h], along(h + 1, d))

    def u_copy(p, i):
        return remote(u.at[p, pl.ds(piece_rows[i], piece)], ur.at[p, i], u_s.at[p], u_r.at[p], {"feat": feats[i]})

    def r_copy(ref, ss, rr, p, i):
        return remote(ref, ref, ss.at[p], rr.at[p], {"feat": feats[i]})

    class Gather:
        def __init__(self, view, r1, r2, r3, s):
            self.view, self.r1, self.r2, self.r3, self.s = view, r1, r2, r3, s

        def first(self, p, h):
            ref = self.view(p, chunk_at(h, 0))
            for d in near_first:
                remote(ref, ref, self.s.at[p], self.r1.at[p, h], along(h + 1, d)).start()

        def second(self, p, h):
            drain(self.view(p, pl.ds(0, (ring - 1) * chunk)), self.r1.at[p, h])
            ref = self.view(p, group_at(h, 0))
            if self.r2 is None:
                for d in far_first:
                    remote(ref, ref, self.s.at[p], self.r3.at[p, h], along(h, d)).start()
            else:
                for k in (0, 1):
                    remote(ref, ref, self.s.at[p], self.r2.at[p, h, k], along(h, sides[k])).start()

        def third(self, p, h):
            for k in (0, 1):
                drain(self.view(p, pl.ds(0, group)), self.r2.at[p, h, k])
                ref = self.view(p, pl.ds(group_rows[h][ring - sides[k]] + k * hg, hg))
                remote(ref, ref, self.s.at[p], self.r3.at[p, h], along(h, sides[k])).start()

        def last(self, p, h):
            drain(self.view(p, pl.ds(0, group if self.r2 is not None else (ring - 1) * group)), self.r3.at[p, h])

        def sent(self, p):
            drain(self.view(p, pl.ds(0, QUARTERS * ((ring - 1) * chunk + 3 * group))), self.s.at[p])

    ag = Gather(lambda p, at: dw.at[p, at], ag1_r, None, ag3_r, ag_s)
    wg = Gather(lambda p, at: wo.at[at, columns(p)], wg1_r, wg2_r, wg3_r, wg_s)

    def start_u(p):
        step = max(rows // 2, piece)
        for k in range(rows // step):
            at = pl.ds(k * step, step)
            u[p, at] = jnp.dot(x[at], dw[p], preferred_element_type=F32).astype(BF16)
        for i in range(len(peers)):
            u_copy(p, i).start()

    def sum_u(p):
        total = u[p, mine].astype(F32)
        drain(ur.at[p], u_r.at[p])
        for i in range(len(peers)):
            total = total + ur[p, i].astype(F32)
        drain(ur.at[p], u_s.at[p])
        return total

    def send_r(p):
        rb[p, mine] = r[p].astype(BF16)
        for i in range(len(peers)):
            r_copy(rb.at[p, mine], rg_s, rg_r, p, i).start()

    def start_g(p, hs):
        if hs == UNITS[0]:
            drain(ur.at[p], rg_r.at[p])
        for ds in ((2,), (1, ring - 1), (0,)):
            for d in ds:
                for h in hs:
                    at = group_at(h, d)
                    g[p, at] = jnp.dot(xt[at], rb[p], preferred_element_type=F32)
            for d in ds:
                for h in hs:
                    if d:
                        rs1_copy(p, h, d).start()

    def mid_g(p, hs):
        for h in hs:
            drain(g.at[p, pl.ds(0, (ring - 1) * group)], rs1_r.at[p, h])
            for e in far_first + [0]:
                at = part_at(h, e)
                total = g[p, chunk_at(h, e)]
                for d in range(ring - 1):
                    total = total + rs1[p, h, d, at]
                s1[p, h, at] = total
                if e:
                    rs2_copy(p, h, e).start()

    def end_g(p, hs, last):
        for h in hs:
            drain(g.at[p, pl.ds(0, (ring - 1) * chunk)], rs2_r.at[p, h])
            total = s1[p, h, part_at(h, 0)]
            for d in range(1, ring):
                total = total + rs2[p, h, d - 1]
            delta = eta[h] * (total / samples - ridge * w[p, h])
            at = chunk_at(h, 0)
            dw[p, at] = delta.astype(BF16)
            ag.first(p, h)
            new = w[p, h] + COMBINE_WEIGHT * delta
            w[p, h] = new
            if last:
                wo[at, p * LANES:(p + 1) * LANES] = new

    loads = [pltpu.make_async_copy(w_hbm, w_in, load_sem.at[0]),
             pltpu.make_async_copy(x_hbm, x, load_sem.at[1]),
             pltpu.make_async_copy(eta_hbm, eta_in, load_sem.at[2])]
    loads += [pltpu.make_async_copy(y_hbm.at[mine, columns(p)], r.at[p], load_sem.at[3 + p]) for p in range(PARTS)]
    for load in loads:
        load.start()
    barrier = pltpu.get_barrier_semaphore()
    for d in range(1, ring):
        for axis in (0, 1):
            pl.semaphore_signal(barrier, inc=1, device_id=along(axis, d), device_id_type=MESH)
    for i in range(len(peers)):
        pl.semaphore_signal(barrier, inc=1, device_id={"feat": feats[i]}, device_id_type=MESH)
    loads[0].wait()
    for p in range(PARTS):
        dw[p] = w_in[:, p * LANES:(p + 1) * LANES].astype(BF16)
        for h in everything:
            w[p, h] = w_in[chunk_at(h, 0), p * LANES:(p + 1) * LANES]
    loads[1].wait()
    pl.semaphore_wait(barrier, 2 * (ring - 1) + len(peers))

    for p in range(PARTS):
        start_u(p)
    tile = min(width, 256)
    for k in range(width // tile):
        xt[k * tile:(k + 1) * tile] = x[:, k * tile:(k + 1) * tile].T
    loads[2].wait()
    for h in everything:
        pos = own_chunks[h][0]
        line = eta_in[pl.ds(lax.div(pos, LANES), 1), :]
        eta_t[...] = jnp.broadcast_to(line, (LANES, LANES)).T
        eta[h] = eta_t[pl.ds(lax.rem(pos, LANES), chunk), :]
    for p in range(PARTS):
        loads[3 + p].wait()
        r[p] = r[p] - sum_u(p)
        send_r(p)

    def sweep(last):
        both = [(p, hs) for p in range(PARTS) for hs in UNITS]
        for p, hs in both:
            start_g(p, hs)
        for p in range(PARTS):
            drain(ur.at[p], rg_s.at[p])
        for p, hs in both:
            mid_g(p, hs)
        for p, hs in both:
            end_g(p, hs, last)
        for p, hs in both:
            for h in hs:
                ag.second(p, h)
        if last:
            for p in range(PARTS):
                for h in everything:
                    wg.first(p, h)
        for p in range(PARTS):
            drain(g.at[p, pl.ds(0, QUARTERS * (3 * group + (ring - 1) * chunk))], gs_s.at[p])
            for h in everything:
                ag.last(p, h)
            ag.sent(p)
            start_u(p)
        if last:
            for p in range(PARTS):
                for h in everything:
                    wg.second(p, h)
        for p in range(PARTS):
            r[p] = r[p] - COMBINE_WEIGHT * sum_u(p)
            if last:
                ro[mine, p * LANES:(p + 1) * LANES] = r[p]
                for i in range(len(peers)):
                    r_copy(ro.at[mine, columns(p)], rf_s, rf_r, p, i).start()
            else:
                send_r(p)
        if last:
            for p in range(PARTS):
                for h in everything:
                    wg.third(p, h)

    def body(i, carry):
        sweep(False)
        return carry

    lax.fori_loop(0, SWEEPS - 1, body, 0)
    sweep(True)
    for p in range(PARTS):
        final = ro.at[pl.ds(0, len(peers) * piece), columns(p)]
        drain(final, rf_r.at[p])
        drain(final, rf_s.at[p])
    for p in range(PARTS):
        for h in everything:
            wg.last(p, h)
        wg.sent(p)


def solution(mesh):
    samp_count = mesh.shape["samp"]
    feat_count = mesh.shape["feat"]
    ring = math.isqrt(samp_count)
    chips = feat_count // 2

    def local_solve(x_loc, w_loc, y_loc, eta_loc):
        rows, width = x_loc.shape
        samples = rows * samp_count
        ridge = RIDGE_SCALE * (width * feat_count) / samples
        group = width // QUARTERS // ring
        chunk = group // ring
        piece = rows // feat_count
        npeer = feat_count - 1
        dma = pltpu.SemaphoreType.DMA
        v = pltpu.VMEM
        each = (PARTS, QUARTERS)
        scratch = [
            v((rows, width), BF16),
            v((width, rows), BF16),
            v((width, PARTS * LANES), F32),
            v(each + (chunk, LANES), F32),
            v((PARTS, piece, LANES), F32),
            v((width // LANES, LANES), F32),
            v((LANES, LANES), F32),
            v((QUARTERS, chunk, LANES), F32),
            v((PARTS, width, LANES), F32),
            v(each + (ring - 1, group, LANES), F32),
            v(each + (group, LANES), F32),
            v(each + (ring - 1, chunk, LANES), F32),
            v((PARTS, width, LANES), BF16),
            v((PARTS, rows, LANES), BF16),
            v((PARTS, npeer, piece, LANES), BF16),
            v((PARTS, rows, LANES), BF16),
            dma((3 + PARTS,)),
            dma(each), dma(each), dma((PARTS,)),
            dma(each), dma(each), dma((PARTS,)),
            dma((PARTS,)), dma((PARTS,)), dma((PARTS,)), dma((PARTS,)),
            dma(each), dma(each + (2,)), dma(each), dma((PARTS,)),
            dma((PARTS,)), dma((PARTS,)),
        ]
        return pl.pallas_call(
            functools.partial(ridge_kernel, ring, chips, samples, ridge),
            out_shape=[pltpu.VMEM(w_loc.shape, F32), pltpu.VMEM(y_loc.shape, F32)],
            in_specs=[pl.BlockSpec(memory_space=pltpu.HBM)] * 4,
            out_specs=[pl.BlockSpec(memory_space=pltpu.VMEM)] * 2,
            scratch_shapes=scratch,
            compiler_params=pltpu.CompilerParams(
                collective_id=0, has_side_effects=True, vmem_limit_bytes=56 * 1024 * 1024),
        )(x_loc, w_loc, y_loc, eta_loc.reshape(width // LANES, LANES))

    return jax.shard_map(
        local_solve,
        mesh=mesh,
        in_specs=(P(("prob", "samp"), "feat"), P(("prob", "feat"), None), P(("prob", "samp"), None), P(("prob", "feat"))),
        out_specs=(P(("prob", "feat"), None), P(("prob", "samp"), None)),
        check_vma=False,
    )
```

```python
import functools
import math

import jax
import jax.numpy as jnp
from jax import lax
from jax.experimental import pallas as pl
from jax.experimental.pallas import tpu as pltpu
from jax.sharding import PartitionSpec as P

SWEEPS = 4
COMBINE_WEIGHT = 0.8
RIDGE_SCALE = 0.1
PARTS = 2
LANES = 128
QUARTERS = 4
UNITS = ((0, 1), (2, 3))
MESH = pl.DeviceIdType.MESH
F32 = jnp.float32
BF16 = jnp.bfloat16


def ridge_kernel(ring, chips, samples, ridge, x_hbm, w_hbm, y_hbm, eta_hbm, wo, ro,
                 x, xt, w_in, w, r, eta_in, eta_t, eta, g, rs1, near, far, s1, rs2, dw, acc, u, ur, rb,
                 load_sem, rl_r, nf_r, rs2_r, gs_s, ag1_r, ag3_r, ag_s,
                 u_s, u_r, rg_s, rg_r, wg1_r, wg2_r, wg3_r, wg_s, rf_s, rf_r):
    samp = lax.axis_index("samp")
    feat = lax.axis_index("feat")
    rows, width = x.shape
    quarter = width // QUARTERS
    group = quarter // ring
    chunk = group // ring
    hg = group // 2
    piece = rows // (2 * chips)
    cy, cz = lax.rem(samp, ring), lax.div(samp, ring)
    cx, core = lax.div(feat, 2), lax.rem(feat, 2)
    ys = [cy] + [lax.rem(cy + d, ring) for d in range(1, ring)]
    zs = [cz] + [lax.rem(cz + d, ring) for d in range(1, ring)]
    neighbour = [[cz * ring + c for c in ys], [c * ring + cy for c in zs]]
    far_first = sorted(range(1, ring), key=lambda d: -min(d, ring - d))
    near_first = far_first[::-1]
    sides = (1, ring - 1)
    across = sorted(range(1, chips), key=lambda d: -min(d, chips - d))
    peers = [(dx, dc) for dx in across + [0] for dc in (0, 1) if dx or dc]
    xs = [cx] + [lax.rem(cx + d, chips) for d in range(1, chips)]
    cores = [core, 1 - core]
    feats = [xs[dx] * 2 + cores[dc] for dx, dc in peers]
    firsts = [(ys, zs)[h % 2] for h in range(QUARTERS)]
    seconds = [(zs, ys)[h % 2] for h in range(QUARTERS)]
    group_rows = [[h * quarter + c * group for c in firsts[h]] for h in range(QUARTERS)]
    chunk_rows = [[c * chunk for c in seconds[h]] for h in range(QUARTERS)]
    own_chunks = [[group_rows[h][0] + c for c in chunk_rows[h]] for h in range(QUARTERS)]
    piece_rows = [f * piece for f in feats]
    mine = pl.ds(feat * piece, piece)
    everything = tuple(range(QUARTERS))

    def along(axis, d):
        return {"samp": neighbour[axis % 2][d]}

    def remote(src, dst, send, recv, device):
        return pltpu.make_async_remote_copy(
            src_ref=src, dst_ref=dst, send_sem=send, recv_sem=recv, device_id=device, device_id_type=MESH)

    def drain(ref, sem):
        pltpu.make_async_copy(ref, ref, sem).wait()

    def group_at(h, d):
        return pl.ds(group_rows[h][d], group)

    def part_at(h, e):
        return pl.ds(chunk_rows[h][e], chunk)

    def chunk_at(h, e):
        return pl.ds(own_chunks[h][e], chunk)

    def columns(p):
        return pl.ds(p * LANES, LANES)

    def rs1_copy(p, h, kind, k):
        if kind == 0:
            row, dst, sem = group_rows[h][2] + k * hg, rs1.at[p, h, k], rl_r.at[p, h, k]
        elif kind == 1:
            row, dst, sem = group_rows[h][sides[k]] + (1 - k) * hg, near.at[p, h, pl.ds((1 - k) * hg, hg)], nf_r.at[p, h]
        else:
            row, dst, sem = group_rows[h][sides[k]] + k * hg, far.at[p, h, pl.ds(k * hg, hg)], nf_r.at[p, h]
        return remote(g.at[p, pl.ds(row, hg)], dst, gs_s.at[p], sem, along(h, sides[k]))

    def rs2_copy(p, h, d):
        return remote(s1.at[p, h, part_at(h, d)], rs2.at[p, h, d - 1], gs_s.at[p], rs2_r.at[p, h], along(h + 1, d))

    def u_copy(p, i):
        return remote(u.at[p, pl.ds(piece_rows[i], piece)], ur.at[p, i], u_s.at[p], u_r.at[p], {"feat": feats[i]})

    def r_copy(ref, ss, rr, p, i):
        return remote(ref, ref, ss.at[p], rr.at[p], {"feat": feats[i]})

    class Gather:
        def __init__(self, view, r1, r2, r3, s):
            self.view, self.r1, self.r2, self.r3, self.s = view, r1, r2, r3, s

        def first(self, p, h):
            ref = self.view(p, chunk_at(h, 0))
            for d in near_first:
                remote(ref, ref, self.s.at[p], self.r1.at[p, h], along(h + 1, d)).start()

        def second(self, p, h):
            drain(self.view(p, pl.ds(0, (ring - 1) * chunk)), self.r1.at[p, h])
            ref = self.view(p, group_at(h, 0))
            if self.r2 is None:
                for d in far_first:
                    remote(ref, ref, self.s.at[p], self.r3.at[p, h], along(h, d)).start()
            else:
                for k in (0, 1):
                    remote(ref, ref, self.s.at[p], self.r2.at[p, h, k], along(h, sides[k])).start()

        def third(self, p, h):
            for k in (0, 1):
                drain(self.view(p, pl.ds(0, group)), self.r2.at[p, h, k])
                ref = self.view(p, pl.ds(group_rows[h][ring - sides[k]] + k * hg, hg))
                remote(ref, ref, self.s.at[p], self.r3.at[p, h], along(h, sides[k])).start()

        def last(self, p, h):
            drain(self.view(p, pl.ds(0, group if self.r2 is not None else (ring - 1) * group)), self.r3.at[p, h])

        def sent(self, p):
            drain(self.view(p, pl.ds(0, QUARTERS * ((ring - 1) * chunk + 3 * group))), self.s.at[p])

    ag = Gather(lambda p, at: dw.at[p, at], ag1_r, None, ag3_r, ag_s)
    wg = Gather(lambda p, at: wo.at[at, columns(p)], wg1_r, wg2_r, wg3_r, wg_s)

    def take_u(p, h, fresh):
        step = max(rows // 2, piece)
        for k in range(rows // step):
            at = pl.ds(k * step, step)
            term = jnp.dot(x[at, h * quarter:(h + 1) * quarter], dw[p, h * quarter:(h + 1) * quarter], preferred_element_type=F32)
            if not fresh:
                term = acc[at] + term
            if h == QUARTERS - 1:
                u[p, at] = term.astype(BF16)
            else:
                acc[at] = term

    def send_u(p):
        for i in range(len(peers)):
            u_copy(p, i).start()

    def sum_u(p):
        total = u[p, mine].astype(F32)
        drain(ur.at[p], u_r.at[p])
        for i in range(len(peers)):
            total = total + ur[p, i].astype(F32)
        drain(ur.at[p], u_s.at[p])
        return total

    def send_r(p):
        rb[p, mine] = r[p].astype(BF16)
        for i in range(len(peers)):
            r_copy(rb.at[p, mine], rg_s, rg_r, p, i).start()

    def start_g(p, hs):
        if hs == UNITS[0]:
            drain(ur.at[p], rg_r.at[p])
        for ds in ((2,), (1, ring - 1), (0,)):
            for d in ds:
                for h in hs:
                    at = group_at(h, d)
                    g[p, at] = jnp.dot(xt[at], rb[p], preferred_element_type=F32)
            for h in hs:
                for k in (0, 1):
                    if ds[0] == 2:
                        rs1_copy(p, h, 0, k).start()
                    elif ds[0]:
                        rs1_copy(p, h, 1, k).start()

    def pass_g(p, hs):
        for h in hs:
            for k in (0, 1):
                rs1_copy(p, h, 0, k).wait_recv()
                at = pl.ds(group_rows[h][sides[k]] + k * hg, hg)
                g[p, at] = g[p, at] + rs1[p, h, k]
                rs1_copy(p, h, 2, k).start()

    def mid_g(p, hs):
        for h in hs:
            drain(g.at[p, pl.ds(0, 2 * group)], nf_r.at[p, h])
            for e in far_first + [0]:
                at = part_at(h, e)
                s1[p, h, at] = g[p, chunk_at(h, e)] + near[p, h, at] + far[p, h, at]
                if e:
                    rs2_copy(p, h, e).start()

    def end_g(p, hs, last):
        for h in hs:
            drain(g.at[p, pl.ds(0, (ring - 1) * chunk)], rs2_r.at[p, h])
            total = s1[p, h, part_at(h, 0)]
            for d in range(1, ring):
                total = total + rs2[p, h, d - 1]
            delta = eta[h] * (total / samples - ridge * w[p, h])
            at = chunk_at(h, 0)
            dw[p, at] = delta.astype(BF16)
            ag.first(p, h)
            new = w[p, h] + COMBINE_WEIGHT * delta
            w[p, h] = new
            if last:
                wo[at, p * LANES:(p + 1) * LANES] = new

    loads = [pltpu.make_async_copy(w_hbm, w_in, load_sem.at[0]),
             pltpu.make_async_copy(x_hbm, x, load_sem.at[1]),
             pltpu.make_async_copy(eta_hbm, eta_in, load_sem.at[2])]
    loads += [pltpu.make_async_copy(y_hbm.at[mine, columns(p)], r.at[p], load_sem.at[3 + p]) for p in range(PARTS)]
    for load in loads:
        load.start()
    barrier = pltpu.get_barrier_semaphore()
    for d in range(1, ring):
        for axis in (0, 1):
            pl.semaphore_signal(barrier, inc=1, device_id=along(axis, d), device_id_type=MESH)
    for i in range(len(peers)):
        pl.semaphore_signal(barrier, inc=1, device_id={"feat": feats[i]}, device_id_type=MESH)
    loads[0].wait()
    for p in range(PARTS):
        dw[p] = w_in[:, p * LANES:(p + 1) * LANES].astype(BF16)
        for h in everything:
            w[p, h] = w_in[chunk_at(h, 0), p * LANES:(p + 1) * LANES]
    loads[1].wait()
    for p in range(PARTS):
        step = max(rows // 2, piece)
        for k in range(rows // step):
            at = pl.ds(k * step, step)
            u[p, at] = jnp.dot(x[at], dw[p], preferred_element_type=F32).astype(BF16)
    pl.semaphore_wait(barrier, 2 * (ring - 1) + len(peers))
    for p in range(PARTS):
        send_u(p)
    tile = min(width, 256)
    for k in range(width // tile):
        xt[k * tile:(k + 1) * tile] = x[:, k * tile:(k + 1) * tile].T
    loads[2].wait()
    for h in everything:
        pos = own_chunks[h][0]
        line = eta_in[pl.ds(lax.div(pos, LANES), 1), :]
        eta_t[...] = jnp.broadcast_to(line, (LANES, LANES)).T
        eta[h] = eta_t[pl.ds(lax.rem(pos, LANES), chunk), :]
    for p in range(PARTS):
        loads[3 + p].wait()
        r[p] = r[p] - sum_u(p)
        send_r(p)

    def sweep(last):
        both = [(p, hs) for p in range(PARTS) for hs in UNITS]
        for p, hs in both:
            start_g(p, hs)
        for p in range(PARTS):
            drain(ur.at[p], rg_s.at[p])
        for p, hs in both:
            pass_g(p, hs)
        for p, hs in both:
            mid_g(p, hs)
        for p, hs in both:
            end_g(p, hs, last)
        for p, hs in both:
            for h in hs:
                ag.second(p, h)
        if last:
            for p in range(PARTS):
                for h in everything:
                    wg.first(p, h)
        for p in range(PARTS):
            drain(g.at[p, pl.ds(0, QUARTERS * (3 * group + (ring - 1) * chunk))], gs_s.at[p])
            for h in everything:
                ag.last(p, h)
                take_u(p, h, h == 0)
            send_u(p)
            ag.sent(p)
        if last:
            for p in range(PARTS):
                for h in everything:
                    wg.second(p, h)
        for p in range(PARTS):
            r[p] = r[p] - COMBINE_WEIGHT * sum_u(p)
            if last:
                ro[mine, p * LANES:(p + 1) * LANES] = r[p]
                for i in range(len(peers)):
                    r_copy(ro.at[mine, columns(p)], rf_s, rf_r, p, i).start()
            else:
                send_r(p)
        if last:
            for p in range(PARTS):
                for h in everything:
                    wg.third(p, h)

    def body(i, carry):
        sweep(False)
        return carry

    lax.fori_loop(0, SWEEPS - 1, body, 0)
    sweep(True)
    for p in range(PARTS):
        final = ro.at[pl.ds(0, len(peers) * piece), columns(p)]
        drain(final, rf_r.at[p])
        drain(final, rf_s.at[p])
    for p in range(PARTS):
        for h in everything:
            wg.last(p, h)
        wg.sent(p)


def solution(mesh):
    samp_count = mesh.shape["samp"]
    feat_count = mesh.shape["feat"]
    ring = math.isqrt(samp_count)
    chips = feat_count // 2

    def local_solve(x_loc, w_loc, y_loc, eta_loc):
        rows, width = x_loc.shape
        samples = rows * samp_count
        ridge = RIDGE_SCALE * (width * feat_count) / samples
        group = width // QUARTERS // ring
        chunk = group // ring
        piece = rows // feat_count
        npeer = feat_count - 1
        dma = pltpu.SemaphoreType.DMA
        v = pltpu.VMEM
        each = (PARTS, QUARTERS)
        scratch = [
            v((rows, width), BF16),
            v((width, rows), BF16),
            v((width, PARTS * LANES), F32),
            v(each + (chunk, LANES), F32),
            v((PARTS, piece, LANES), F32),
            v((width // LANES, LANES), F32),
            v((LANES, LANES), F32),
            v((QUARTERS, chunk, LANES), F32),
            v((PARTS, width, LANES), F32),
            v(each + (2, group // 2, LANES), F32),
            v(each + (group, LANES), F32),
            v(each + (group, LANES), F32),
            v(each + (group, LANES), F32),
            v(each + (ring - 1, chunk, LANES), F32),
            v((PARTS, width, LANES), BF16),
            v((rows, LANES), F32),
            v((PARTS, rows, LANES), BF16),
            v((PARTS, npeer, piece, LANES), BF16),
            v((PARTS, rows, LANES), BF16),
            dma((3 + PARTS,)),
            dma(each + (2,)), dma(each), dma(each), dma((PARTS,)),
            dma(each), dma(each), dma((PARTS,)),
            dma((PARTS,)), dma((PARTS,)), dma((PARTS,)), dma((PARTS,)),
            dma(each), dma(each + (2,)), dma(each), dma((PARTS,)),
            dma((PARTS,)), dma((PARTS,)),
        ]
        return pl.pallas_call(
            functools.partial(ridge_kernel, ring, chips, samples, ridge),
            out_shape=[pltpu.VMEM(w_loc.shape, F32), pltpu.VMEM(y_loc.shape, F32)],
            in_specs=[pl.BlockSpec(memory_space=pltpu.HBM)] * 4,
            out_specs=[pl.BlockSpec(memory_space=pltpu.VMEM)] * 2,
            scratch_shapes=scratch,
            compiler_params=pltpu.CompilerParams(
                collective_id=0, has_side_effects=True, vmem_limit_bytes=56 * 1024 * 1024),
        )(x_loc, w_loc, y_loc, eta_loc.reshape(width // LANES, LANES))

    return jax.shard_map(
        local_solve,
        mesh=mesh,
        in_specs=(P(("prob", "samp"), "feat"), P(("prob", "feat"), None), P(("prob", "samp"), None), P(("prob", "feat"))),
        out_specs=(P(("prob", "feat"), None), P(("prob", "samp"), None)),
        check_vma=False,
    )
```

```python
import functools
import math

import jax
import jax.numpy as jnp
from jax import lax
from jax.experimental import pallas as pl
from jax.experimental.pallas import tpu as pltpu
from jax.sharding import PartitionSpec as P

SWEEPS = 4
COMBINE_WEIGHT = 0.8
RIDGE_SCALE = 0.1
PARTS = 2
LANES = 128
QUARTERS = 4
UNITS = ((0, 1), (2, 3))
MESH = pl.DeviceIdType.MESH
F32 = jnp.float32
BF16 = jnp.bfloat16


def ridge_kernel(ring, chips, samples, ridge, x_hbm, w_hbm, y_hbm, eta_hbm, wo, ro,
                 x, xt, w_in, w, r, eta_in, eta_t, eta, g, rs1, near, far, s1, rs2, dw, u, ur, rb,
                 load_sem, rl_r, nf_r, rs2_r, gs_s, ag1_r, ag3_r, ag_s,
                 u_s, u_r, rg_s, rg_r, wg1_r, wg2_r, wg3_r, wg_s, rf_s, rf_r):
    samp = lax.axis_index("samp")
    feat = lax.axis_index("feat")
    rows, width = x.shape
    quarter = width // QUARTERS
    group = quarter // ring
    chunk = group // ring
    hg = group // 2
    piece = rows // (2 * chips)
    cy, cz = lax.rem(samp, ring), lax.div(samp, ring)
    cx, core = lax.div(feat, 2), lax.rem(feat, 2)
    ys = [cy] + [lax.rem(cy + d, ring) for d in range(1, ring)]
    zs = [cz] + [lax.rem(cz + d, ring) for d in range(1, ring)]
    neighbour = [[cz * ring + c for c in ys], [c * ring + cy for c in zs]]
    far_first = sorted(range(1, ring), key=lambda d: -min(d, ring - d))
    near_first = far_first[::-1]
    sides = (1, ring - 1)
    across = sorted(range(1, chips), key=lambda d: -min(d, chips - d))
    peers = [(dx, dc) for dx in across + [0] for dc in (0, 1) if dx or dc]
    xs = [cx] + [lax.rem(cx + d, chips) for d in range(1, chips)]
    cores = [core, 1 - core]
    feats = [xs[dx] * 2 + cores[dc] for dx, dc in peers]
    firsts = [(ys, zs)[h % 2] for h in range(QUARTERS)]
    seconds = [(zs, ys)[h % 2] for h in range(QUARTERS)]
    group_rows = [[h * quarter + c * group for c in firsts[h]] for h in range(QUARTERS)]
    chunk_rows = [[c * chunk for c in seconds[h]] for h in range(QUARTERS)]
    own_chunks = [[group_rows[h][0] + c for c in chunk_rows[h]] for h in range(QUARTERS)]
    piece_rows = [f * piece for f in feats]
    mine = pl.ds(feat * piece, piece)
    everything = tuple(range(QUARTERS))

    def along(axis, d):
        return {"samp": neighbour[axis % 2][d]}

    def remote(src, dst, send, recv, device):
        return pltpu.make_async_remote_copy(
            src_ref=src, dst_ref=dst, send_sem=send, recv_sem=recv, device_id=device, device_id_type=MESH)

    def drain(ref, sem):
        pltpu.make_async_copy(ref, ref, sem).wait()

    def group_at(h, d):
        return pl.ds(group_rows[h][d], group)

    def part_at(h, e):
        return pl.ds(chunk_rows[h][e], chunk)

    def chunk_at(h, e):
        return pl.ds(own_chunks[h][e], chunk)

    def columns(p):
        return pl.ds(p * LANES, LANES)

    def rs1_copy(p, h, kind, k):
        if kind == 0:
            row, dst, sem = group_rows[h][2] + k * hg, rs1.at[p, h, k], rl_r.at[p, h, k]
        elif kind == 1:
            row, dst, sem = group_rows[h][sides[k]] + (1 - k) * hg, near.at[p, h, pl.ds((1 - k) * hg, hg)], nf_r.at[p, h]
        else:
            row, dst, sem = group_rows[h][sides[k]] + k * hg, far.at[p, h, pl.ds(k * hg, hg)], nf_r.at[p, h]
        return remote(g.at[p, pl.ds(row, hg)], dst, gs_s.at[p], sem, along(h, sides[k]))

    def rs2_copy(p, h, d):
        return remote(s1.at[p, h, part_at(h, d)], rs2.at[p, h, d - 1], gs_s.at[p], rs2_r.at[p, h], along(h + 1, d))

    def u_copy(p, i):
        return remote(u.at[p, pl.ds(piece_rows[i], piece)], ur.at[p, i], u_s.at[p], u_r.at[p], {"feat": feats[i]})

    def r_copy(ref, ss, rr, p, i):
        return remote(ref, ref, ss.at[p], rr.at[p], {"feat": feats[i]})

    class Gather:
        def __init__(self, view, r1, r2, r3, s):
            self.view, self.r1, self.r2, self.r3, self.s = view, r1, r2, r3, s

        def first(self, p, h):
            ref = self.view(p, chunk_at(h, 0))
            for d in near_first:
                remote(ref, ref, self.s.at[p], self.r1.at[p, h], along(h + 1, d)).start()

        def second(self, p, h):
            drain(self.view(p, pl.ds(0, (ring - 1) * chunk)), self.r1.at[p, h])
            ref = self.view(p, group_at(h, 0))
            if self.r2 is None:
                for d in far_first:
                    remote(ref, ref, self.s.at[p], self.r3.at[p, h], along(h, d)).start()
            else:
                for k in (0, 1):
                    remote(ref, ref, self.s.at[p], self.r2.at[p, h, k], along(h, sides[k])).start()

        def third(self, p, h):
            for k in (0, 1):
                drain(self.view(p, pl.ds(0, group)), self.r2.at[p, h, k])
                ref = self.view(p, pl.ds(group_rows[h][ring - sides[k]] + k * hg, hg))
                remote(ref, ref, self.s.at[p], self.r3.at[p, h], along(h, sides[k])).start()

        def last(self, p, h):
            drain(self.view(p, pl.ds(0, group if self.r2 is not None else (ring - 1) * group)), self.r3.at[p, h])

        def sent(self, p):
            drain(self.view(p, pl.ds(0, QUARTERS * ((ring - 1) * chunk + 3 * group))), self.s.at[p])

    ag = Gather(lambda p, at: dw.at[p, at], ag1_r, None, ag3_r, ag_s)
    wg = Gather(lambda p, at: wo.at[at, columns(p)], wg1_r, wg2_r, wg3_r, wg_s)

    def take_u(p):
        step = max(rows // 2, piece)
        for k in range(rows // step):
            at = pl.ds(k * step, step)
            u[p, at] = jnp.dot(x[at], dw[p], preferred_element_type=F32).astype(BF16)

    def send_u(p):
        for i in range(len(peers)):
            u_copy(p, i).start()

    def sum_u(p):
        total = u[p, mine].astype(F32)
        drain(ur.at[p], u_r.at[p])
        for i in range(len(peers)):
            total = total + ur[p, i].astype(F32)
        drain(ur.at[p], u_s.at[p])
        return total

    def send_r(p):
        rb[p, mine] = r[p].astype(BF16)
        for i in range(len(peers)):
            r_copy(rb.at[p, mine], rg_s, rg_r, p, i).start()

    def start_g(p, hs):
        if hs == UNITS[0]:
            drain(ur.at[p], rg_r.at[p])
        for ds in ((2,), (1, ring - 1), (0,)):
            for d in ds:
                for h in hs:
                    at = group_at(h, d)
                    g[p, at] = jnp.dot(xt[at], rb[p], preferred_element_type=F32)
            for h in hs:
                for k in (0, 1):
                    if ds[0] == 2:
                        rs1_copy(p, h, 0, k).start()
                    elif ds[0]:
                        rs1_copy(p, h, 1, k).start()

    def pass_g(p, hs):
        for h in hs:
            for k in (0, 1):
                rs1_copy(p, h, 0, k).wait_recv()
                at = pl.ds(group_rows[h][sides[k]] + k * hg, hg)
                g[p, at] = g[p, at] + rs1[p, h, k]
                rs1_copy(p, h, 2, k).start()

    def mid_g(p, hs):
        for h in hs:
            drain(g.at[p, pl.ds(0, 2 * group)], nf_r.at[p, h])
            for e in far_first + [0]:
                at = part_at(h, e)
                s1[p, h, at] = g[p, chunk_at(h, e)] + near[p, h, at] + far[p, h, at]
                if e:
                    rs2_copy(p, h, e).start()

    def end_g(p, hs, last):
        for h in hs:
            drain(g.at[p, pl.ds(0, (ring - 1) * chunk)], rs2_r.at[p, h])
            total = s1[p, h, part_at(h, 0)]
            for d in range(1, ring):
                total = total + rs2[p, h, d - 1]
            delta = eta[h] * (total / samples - ridge * w[p, h])
            at = chunk_at(h, 0)
            dw[p, at] = delta.astype(BF16)
            ag.first(p, h)
            new = w[p, h] + COMBINE_WEIGHT * delta
            w[p, h] = new
            if last:
                wo[at, p * LANES:(p + 1) * LANES] = new

    loads = [pltpu.make_async_copy(w_hbm, w_in, load_sem.at[0]),
             pltpu.make_async_copy(x_hbm, x, load_sem.at[1]),
             pltpu.make_async_copy(eta_hbm, eta_in, load_sem.at[2])]
    loads += [pltpu.make_async_copy(y_hbm.at[mine, columns(p)], r.at[p], load_sem.at[3 + p]) for p in range(PARTS)]
    for load in loads:
        load.start()
    barrier = pltpu.get_barrier_semaphore()
    for d in range(1, ring):
        for axis in (0, 1):
            pl.semaphore_signal(barrier, inc=1, device_id=along(axis, d), device_id_type=MESH)
    for i in range(len(peers)):
        pl.semaphore_signal(barrier, inc=1, device_id={"feat": feats[i]}, device_id_type=MESH)
    loads[0].wait()
    for p in range(PARTS):
        dw[p] = w_in[:, p * LANES:(p + 1) * LANES].astype(BF16)
        for h in everything:
            w[p, h] = w_in[chunk_at(h, 0), p * LANES:(p + 1) * LANES]
    loads[1].wait()
    for p in range(PARTS):
        take_u(p)
    pl.semaphore_wait(barrier, 2 * (ring - 1) + len(peers))
    for p in range(PARTS):
        send_u(p)
    tile = min(width, 256)
    for k in range(width // tile):
        xt[k * tile:(k + 1) * tile] = x[:, k * tile:(k + 1) * tile].T
    loads[2].wait()
    for h in everything:
        pos = own_chunks[h][0]
        line = eta_in[pl.ds(lax.div(pos, LANES), 1), :]
        eta_t[...] = jnp.broadcast_to(line, (LANES, LANES)).T
        eta[h] = eta_t[pl.ds(lax.rem(pos, LANES), chunk), :]
    for p in range(PARTS):
        loads[3 + p].wait()
        r[p] = r[p] - sum_u(p)
        send_r(p)

    def sweep(last):
        both = [(p, hs) for p in range(PARTS) for hs in UNITS]
        for p, hs in both:
            start_g(p, hs)
        for p in range(PARTS):
            drain(ur.at[p], rg_s.at[p])
        for p, hs in both:
            pass_g(p, hs)
        for p, hs in both:
            mid_g(p, hs)
        for p, hs in both:
            end_g(p, hs, last)
        for p, hs in both:
            for h in hs:
                ag.second(p, h)
        if last:
            for p in range(PARTS):
                for h in everything:
                    wg.first(p, h)
        for p in range(PARTS):
            drain(g.at[p, pl.ds(0, QUARTERS * (3 * group + (ring - 1) * chunk))], gs_s.at[p])
            for h in everything:
                ag.last(p, h)
            take_u(p)
            send_u(p)
            ag.sent(p)
        if last:
            for p in range(PARTS):
                for h in everything:
                    wg.second(p, h)
        for p in range(PARTS):
            r[p] = r[p] - COMBINE_WEIGHT * sum_u(p)
            if last:
                ro[mine, p * LANES:(p + 1) * LANES] = r[p]
                for i in range(len(peers)):
                    r_copy(ro.at[mine, columns(p)], rf_s, rf_r, p, i).start()
            else:
                send_r(p)
        if last:
            for p in range(PARTS):
                for h in everything:
                    wg.third(p, h)

    def body(i, carry):
        sweep(False)
        return carry

    lax.fori_loop(0, SWEEPS - 1, body, 0)
    sweep(True)
    for p in range(PARTS):
        final = ro.at[pl.ds(0, len(peers) * piece), columns(p)]
        drain(final, rf_r.at[p])
        drain(final, rf_s.at[p])
    for p in range(PARTS):
        for h in everything:
            wg.last(p, h)
        wg.sent(p)


def solution(mesh):
    samp_count = mesh.shape["samp"]
    feat_count = mesh.shape["feat"]
    ring = math.isqrt(samp_count)
    chips = feat_count // 2

    def local_solve(x_loc, w_loc, y_loc, eta_loc):
        rows, width = x_loc.shape
        samples = rows * samp_count
        ridge = RIDGE_SCALE * (width * feat_count) / samples
        group = width // QUARTERS // ring
        chunk = group // ring
        piece = rows // feat_count
        npeer = feat_count - 1
        dma = pltpu.SemaphoreType.DMA
        v = pltpu.VMEM
        each = (PARTS, QUARTERS)
        scratch = [
            v((rows, width), BF16),
            v((width, rows), BF16),
            v((width, PARTS * LANES), F32),
            v(each + (chunk, LANES), F32),
            v((PARTS, piece, LANES), F32),
            v((width // LANES, LANES), F32),
            v((LANES, LANES), F32),
            v((QUARTERS, chunk, LANES), F32),
            v((PARTS, width, LANES), F32),
            v(each + (2, group // 2, LANES), F32),
            v(each + (group, LANES), F32),
            v(each + (group, LANES), F32),
            v(each + (group, LANES), F32),
            v(each + (ring - 1, chunk, LANES), F32),
            v((PARTS, width, LANES), BF16),
            v((PARTS, rows, LANES), BF16),
            v((PARTS, npeer, piece, LANES), BF16),
            v((PARTS, rows, LANES), BF16),
            dma((3 + PARTS,)),
            dma(each + (2,)), dma(each), dma(each), dma((PARTS,)),
            dma(each), dma(each), dma((PARTS,)),
            dma((PARTS,)), dma((PARTS,)), dma((PARTS,)), dma((PARTS,)),
            dma(each), dma(each + (2,)), dma(each), dma((PARTS,)),
            dma((PARTS,)), dma((PARTS,)),
        ]
        return pl.pallas_call(
            functools.partial(ridge_kernel, ring, chips, samples, ridge),
            out_shape=[pltpu.VMEM(w_loc.shape, F32), pltpu.VMEM(y_loc.shape, F32)],
            in_specs=[pl.BlockSpec(memory_space=pltpu.HBM)] * 4,
            out_specs=[pl.BlockSpec(memory_space=pltpu.VMEM)] * 2,
            scratch_shapes=scratch,
            compiler_params=pltpu.CompilerParams(
                collective_id=0, has_side_effects=True, vmem_limit_bytes=56 * 1024 * 1024),
        )(x_loc, w_loc, y_loc, eta_loc.reshape(width // LANES, LANES))

    return jax.shard_map(
        local_solve,
        mesh=mesh,
        in_specs=(P(("prob", "samp"), "feat"), P(("prob", "feat"), None), P(("prob", "samp"), None), P(("prob", "feat"))),
        out_specs=(P(("prob", "feat"), None), P(("prob", "samp"), None)),
        check_vma=False,
    )
```

```python
import functools
import math

import jax
import jax.numpy as jnp
from jax import lax
from jax.experimental import pallas as pl
from jax.experimental.pallas import tpu as pltpu
from jax.sharding import PartitionSpec as P

SWEEPS = 4
COMBINE_WEIGHT = 0.8
RIDGE_SCALE = 0.1
PARTS = 2
LANES = 128
QUARTERS = 2
UNITS = ((0, 1),)
MESH = pl.DeviceIdType.MESH
F32 = jnp.float32
BF16 = jnp.bfloat16


def ridge_kernel(ring, chips, samples, ridge, x_hbm, w_hbm, y_hbm, eta_hbm, wo, ro,
                 x, xt, w_in, w, r, eta_in, eta_t, eta, g, rs1, near, far, s1, rs2, dw, u, ur, rb,
                 load_sem, rl_r, nf_r, rs2_r, gs_s, ag1_r, ag3_r, ag_s,
                 u_s, u_r, rg_s, rg_r, wg1_r, wg2_r, wg3_r, wg_s, rf_s, rf_r):
    samp = lax.axis_index("samp")
    feat = lax.axis_index("feat")
    rows, width = x.shape
    quarter = width // QUARTERS
    group = quarter // ring
    chunk = group // ring
    hg = group // 2
    piece = rows // (2 * chips)
    cy, cz = lax.rem(samp, ring), lax.div(samp, ring)
    cx, core = lax.div(feat, 2), lax.rem(feat, 2)
    ys = [cy] + [lax.rem(cy + d, ring) for d in range(1, ring)]
    zs = [cz] + [lax.rem(cz + d, ring) for d in range(1, ring)]
    neighbour = [[cz * ring + c for c in ys], [c * ring + cy for c in zs]]
    far_first = sorted(range(1, ring), key=lambda d: -min(d, ring - d))
    near_first = far_first[::-1]
    sides = (1, ring - 1)
    across = sorted(range(1, chips), key=lambda d: -min(d, chips - d))
    peers = [(dx, dc) for dx in across + [0] for dc in (0, 1) if dx or dc]
    xs = [cx] + [lax.rem(cx + d, chips) for d in range(1, chips)]
    cores = [core, 1 - core]
    feats = [xs[dx] * 2 + cores[dc] for dx, dc in peers]
    firsts = [(ys, zs)[h % 2] for h in range(QUARTERS)]
    seconds = [(zs, ys)[h % 2] for h in range(QUARTERS)]
    group_rows = [[h * quarter + c * group for c in firsts[h]] for h in range(QUARTERS)]
    chunk_rows = [[c * chunk for c in seconds[h]] for h in range(QUARTERS)]
    own_chunks = [[group_rows[h][0] + c for c in chunk_rows[h]] for h in range(QUARTERS)]
    piece_rows = [f * piece for f in feats]
    mine = pl.ds(feat * piece, piece)
    everything = tuple(range(QUARTERS))

    def along(axis, d):
        return {"samp": neighbour[axis % 2][d]}

    def remote(src, dst, send, recv, device):
        return pltpu.make_async_remote_copy(
            src_ref=src, dst_ref=dst, send_sem=send, recv_sem=recv, device_id=device, device_id_type=MESH)

    def drain(ref, sem):
        pltpu.make_async_copy(ref, ref, sem).wait()

    def group_at(h, d):
        return pl.ds(group_rows[h][d], group)

    def part_at(h, e):
        return pl.ds(chunk_rows[h][e], chunk)

    def chunk_at(h, e):
        return pl.ds(own_chunks[h][e], chunk)

    def columns(p):
        return pl.ds(p * LANES, LANES)

    def rs1_copy(p, h, kind, k):
        if kind == 0:
            row, dst, sem = group_rows[h][2] + k * hg, rs1.at[p, h, k], rl_r.at[p, h, k]
        elif kind == 1:
            row, dst, sem = group_rows[h][sides[k]] + (1 - k) * hg, near.at[p, h, pl.ds((1 - k) * hg, hg)], nf_r.at[p, h]
        else:
            row, dst, sem = group_rows[h][sides[k]] + k * hg, far.at[p, h, pl.ds(k * hg, hg)], nf_r.at[p, h]
        return remote(g.at[p, pl.ds(row, hg)], dst, gs_s.at[p], sem, along(h, sides[k]))

    def rs2_copy(p, h, d):
        return remote(s1.at[p, h, part_at(h, d)], rs2.at[p, h, d - 1], gs_s.at[p], rs2_r.at[p, h], along(h + 1, d))

    def u_copy(p, i):
        return remote(u.at[p, pl.ds(piece_rows[i], piece)], ur.at[p, i], u_s.at[p], u_r.at[p], {"feat": feats[i]})

    def r_copy(ref, ss, rr, p, i):
        return remote(ref, ref, ss.at[p], rr.at[p], {"feat": feats[i]})

    class Gather:
        def __init__(self, view, r1, r2, r3, s):
            self.view, self.r1, self.r2, self.r3, self.s = view, r1, r2, r3, s

        def first(self, p, h):
            ref = self.view(p, chunk_at(h, 0))
            for d in near_first:
                remote(ref, ref, self.s.at[p], self.r1.at[p, h], along(h + 1, d)).start()

        def second(self, p, h):
            drain(self.view(p, pl.ds(0, (ring - 1) * chunk)), self.r1.at[p, h])
            ref = self.view(p, group_at(h, 0))
            if self.r2 is None:
                for d in far_first:
                    remote(ref, ref, self.s.at[p], self.r3.at[p, h], along(h, d)).start()
            else:
                for k in (0, 1):
                    remote(ref, ref, self.s.at[p], self.r2.at[p, h, k], along(h, sides[k])).start()

        def third(self, p, h):
            for k in (0, 1):
                drain(self.view(p, pl.ds(0, group)), self.r2.at[p, h, k])
                ref = self.view(p, pl.ds(group_rows[h][ring - sides[k]] + k * hg, hg))
                remote(ref, ref, self.s.at[p], self.r3.at[p, h], along(h, sides[k])).start()

        def last(self, p, h):
            drain(self.view(p, pl.ds(0, group if self.r2 is not None else (ring - 1) * group)), self.r3.at[p, h])

        def sent(self, p):
            drain(self.view(p, pl.ds(0, QUARTERS * ((ring - 1) * chunk + 3 * group))), self.s.at[p])

    ag = Gather(lambda p, at: dw.at[p, at], ag1_r, None, ag3_r, ag_s)
    wg = Gather(lambda p, at: wo.at[at, columns(p)], wg1_r, wg2_r, wg3_r, wg_s)

    def start_u(p):
        step = max(rows // 2, piece)
        for k in range(rows // step):
            at = pl.ds(k * step, step)
            u[p, at] = jnp.dot(x[at], dw[p], preferred_element_type=F32).astype(BF16)
        for i in range(len(peers)):
            u_copy(p, i).start()

    def sum_u(p):
        total = u[p, mine].astype(F32)
        drain(ur.at[p], u_r.at[p])
        for i in range(len(peers)):
            total = total + ur[p, i].astype(F32)
        drain(ur.at[p], u_s.at[p])
        return total

    def send_r(p):
        rb[p, mine] = r[p].astype(BF16)
        for i in range(len(peers)):
            r_copy(rb.at[p, mine], rg_s, rg_r, p, i).start()

    def start_g(p, hs):
        if hs == UNITS[0]:
            drain(ur.at[p], rg_r.at[p])
        for ds in ((2,), (1, ring - 1), (0,)):
            for d in ds:
                for h in hs:
                    at = group_at(h, d)
                    g[p, at] = jnp.dot(xt[at], rb[p], preferred_element_type=F32)
            for h in hs:
                for k in (0, 1):
                    if ds[0] == 2:
                        rs1_copy(p, h, 0, k).start()
                    elif ds[0]:
                        rs1_copy(p, h, 1, k).start()

    def pass_g(p, hs):
        for h in hs:
            for k in (0, 1):
                rs1_copy(p, h, 0, k).wait_recv()
                at = pl.ds(group_rows[h][sides[k]] + k * hg, hg)
                g[p, at] = g[p, at] + rs1[p, h, k]
                rs1_copy(p, h, 2, k).start()

    def mid_g(p, hs):
        for h in hs:
            drain(g.at[p, pl.ds(0, 2 * group)], nf_r.at[p, h])
            for e in far_first + [0]:
                at = part_at(h, e)
                s1[p, h, at] = g[p, chunk_at(h, e)] + near[p, h, at] + far[p, h, at]
                if e:
                    rs2_copy(p, h, e).start()

    def end_g(p, hs, last):
        for h in hs:
            drain(g.at[p, pl.ds(0, (ring - 1) * chunk)], rs2_r.at[p, h])
            total = s1[p, h, part_at(h, 0)]
            for d in range(1, ring):
                total = total + rs2[p, h, d - 1]
            delta = eta[h] * (total / samples - ridge * w[p, h])
            at = chunk_at(h, 0)
            dw[p, at] = delta.astype(BF16)
            ag.first(p, h)
            new = w[p, h] + COMBINE_WEIGHT * delta
            w[p, h] = new
            if last:
                wo[at, p * LANES:(p + 1) * LANES] = new

    loads = [pltpu.make_async_copy(w_hbm, w_in, load_sem.at[0]),
             pltpu.make_async_copy(x_hbm, x, load_sem.at[1]),
             pltpu.make_async_copy(eta_hbm, eta_in, load_sem.at[2])]
    loads += [pltpu.make_async_copy(y_hbm.at[mine, columns(p)], r.at[p], load_sem.at[3 + p]) for p in range(PARTS)]
    for load in loads:
        load.start()
    barrier = pltpu.get_barrier_semaphore()
    for d in range(1, ring):
        for axis in (0, 1):
            pl.semaphore_signal(barrier, inc=1, device_id=along(axis, d), device_id_type=MESH)
    for i in range(len(peers)):
        pl.semaphore_signal(barrier, inc=1, device_id={"feat": feats[i]}, device_id_type=MESH)
    loads[0].wait()
    for p in range(PARTS):
        dw[p] = w_in[:, p * LANES:(p + 1) * LANES].astype(BF16)
        for h in everything:
            w[p, h] = w_in[chunk_at(h, 0), p * LANES:(p + 1) * LANES]
    loads[1].wait()
    pl.semaphore_wait(barrier, 2 * (ring - 1) + len(peers))

    for p in range(PARTS):
        start_u(p)
    tile = min(width, 256)
    for k in range(width // tile):
        xt[k * tile:(k + 1) * tile] = x[:, k * tile:(k + 1) * tile].T
    loads[2].wait()
    for h in everything:
        pos = own_chunks[h][0]
        line = eta_in[pl.ds(lax.div(pos, LANES), 1), :]
        eta_t[...] = jnp.broadcast_to(line, (LANES, LANES)).T
        eta[h] = eta_t[pl.ds(lax.rem(pos, LANES), chunk), :]
    for p in range(PARTS):
        loads[3 + p].wait()
        r[p] = r[p] - sum_u(p)
        send_r(p)

    def sweep(last):
        both = [(p, hs) for p in range(PARTS) for hs in UNITS]
        for p, hs in both:
            start_g(p, hs)
        for p in range(PARTS):
            drain(ur.at[p], rg_s.at[p])
        for p, hs in both:
            pass_g(p, hs)
        for p, hs in both:
            mid_g(p, hs)
        for p, hs in both:
            end_g(p, hs, last)
        for p, hs in both:
            for h in hs:
                ag.second(p, h)
        if last:
            for p in range(PARTS):
                for h in everything:
                    wg.first(p, h)
        for p in range(PARTS):
            drain(g.at[p, pl.ds(0, QUARTERS * (3 * group + (ring - 1) * chunk))], gs_s.at[p])
            for h in everything:
                ag.last(p, h)
            ag.sent(p)
            start_u(p)
        if last:
            for p in range(PARTS):
                for h in everything:
                    wg.second(p, h)
        for p in range(PARTS):
            r[p] = r[p] - COMBINE_WEIGHT * sum_u(p)
            if last:
                ro[mine, p * LANES:(p + 1) * LANES] = r[p]
                for i in range(len(peers)):
                    r_copy(ro.at[mine, columns(p)], rf_s, rf_r, p, i).start()
            else:
                send_r(p)
        if last:
            for p in range(PARTS):
                for h in everything:
                    wg.third(p, h)

    def body(i, carry):
        sweep(False)
        return carry

    lax.fori_loop(0, SWEEPS - 1, body, 0)
    sweep(True)
    for p in range(PARTS):
        final = ro.at[pl.ds(0, len(peers) * piece), columns(p)]
        drain(final, rf_r.at[p])
        drain(final, rf_s.at[p])
    for p in range(PARTS):
        for h in everything:
            wg.last(p, h)
        wg.sent(p)


def solution(mesh):
    samp_count = mesh.shape["samp"]
    feat_count = mesh.shape["feat"]
    ring = math.isqrt(samp_count)
    chips = feat_count // 2

    def local_solve(x_loc, w_loc, y_loc, eta_loc):
        rows, width = x_loc.shape
        samples = rows * samp_count
        ridge = RIDGE_SCALE * (width * feat_count) / samples
        group = width // QUARTERS // ring
        chunk = group // ring
        piece = rows // feat_count
        npeer = feat_count - 1
        dma = pltpu.SemaphoreType.DMA
        v = pltpu.VMEM
        each = (PARTS, QUARTERS)
        scratch = [
            v((rows, width), BF16),
            v((width, rows), BF16),
            v((width, PARTS * LANES), F32),
            v(each + (chunk, LANES), F32),
            v((PARTS, piece, LANES), F32),
            v((width // LANES, LANES), F32),
            v((LANES, LANES), F32),
            v((QUARTERS, chunk, LANES), F32),
            v((PARTS, width, LANES), F32),
            v(each + (2, group // 2, LANES), F32),
            v(each + (group, LANES), F32),
            v(each + (group, LANES), F32),
            v(each + (group, LANES), F32),
            v(each + (ring - 1, chunk, LANES), F32),
            v((PARTS, width, LANES), BF16),
            v((PARTS, rows, LANES), BF16),
            v((PARTS, npeer, piece, LANES), BF16),
            v((PARTS, rows, LANES), BF16),
            dma((3 + PARTS,)),
            dma(each + (2,)), dma(each), dma(each), dma((PARTS,)),
            dma(each), dma(each), dma((PARTS,)),
            dma((PARTS,)), dma((PARTS,)), dma((PARTS,)), dma((PARTS,)),
            dma(each), dma(each + (2,)), dma(each), dma((PARTS,)),
            dma((PARTS,)), dma((PARTS,)),
        ]
        return pl.pallas_call(
            functools.partial(ridge_kernel, ring, chips, samples, ridge),
            out_shape=[pltpu.VMEM(w_loc.shape, F32), pltpu.VMEM(y_loc.shape, F32)],
            in_specs=[pl.BlockSpec(memory_space=pltpu.HBM)] * 4,
            out_specs=[pl.BlockSpec(memory_space=pltpu.VMEM)] * 2,
            scratch_shapes=scratch,
            compiler_params=pltpu.CompilerParams(
                collective_id=0, has_side_effects=True, vmem_limit_bytes=56 * 1024 * 1024),
        )(x_loc, w_loc, y_loc, eta_loc.reshape(width // LANES, LANES))

    return jax.shard_map(
        local_solve,
        mesh=mesh,
        in_specs=(P(("prob", "samp"), "feat"), P(("prob", "feat"), None), P(("prob", "samp"), None), P(("prob", "feat"))),
        out_specs=(P(("prob", "feat"), None), P(("prob", "samp"), None)),
        check_vma=False,
    )
```

```python
import functools
import math

import jax
import jax.numpy as jnp
from jax import lax
from jax.experimental import pallas as pl
from jax.experimental.pallas import tpu as pltpu
from jax.sharding import PartitionSpec as P

SWEEPS = 4
COMBINE_WEIGHT = 0.8
RIDGE_SCALE = 0.1
PARTS = 2
LANES = 128
QUARTERS = 8
UNITS = ((0, 1), (2, 3), (4, 5), (6, 7))
MESH = pl.DeviceIdType.MESH
F32 = jnp.float32
BF16 = jnp.bfloat16


def ridge_kernel(ring, chips, samples, ridge, x_hbm, w_hbm, y_hbm, eta_hbm, wo, ro,
                 x, xt, w_in, w, r, eta_in, eta_t, eta, g, rs1, near, far, s1, rs2, dw, u, ur, rb,
                 load_sem, rl_r, nf_r, rs2_r, gs_s, ag1_r, ag3_r, ag_s,
                 u_s, u_r, rg_s, rg_r, wg1_r, wg2_r, wg3_r, wg_s, rf_s, rf_r):
    samp = lax.axis_index("samp")
    feat = lax.axis_index("feat")
    rows, width = x.shape
    quarter = width // QUARTERS
    group = quarter // ring
    chunk = group // ring
    hg = group // 2
    piece = rows // (2 * chips)
    cy, cz = lax.rem(samp, ring), lax.div(samp, ring)
    cx, core = lax.div(feat, 2), lax.rem(feat, 2)
    ys = [cy] + [lax.rem(cy + d, ring) for d in range(1, ring)]
    zs = [cz] + [lax.rem(cz + d, ring) for d in range(1, ring)]
    neighbour = [[cz * ring + c for c in ys], [c * ring + cy for c in zs]]
    far_first = sorted(range(1, ring), key=lambda d: -min(d, ring - d))
    near_first = far_first[::-1]
    sides = (1, ring - 1)
    across = sorted(range(1, chips), key=lambda d: -min(d, chips - d))
    peers = [(dx, dc) for dx in across + [0] for dc in (0, 1) if dx or dc]
    xs = [cx] + [lax.rem(cx + d, chips) for d in range(1, chips)]
    cores = [core, 1 - core]
    feats = [xs[dx] * 2 + cores[dc] for dx, dc in peers]
    firsts = [(ys, zs)[h % 2] for h in range(QUARTERS)]
    seconds = [(zs, ys)[h % 2] for h in range(QUARTERS)]
    group_rows = [[h * quarter + c * group for c in firsts[h]] for h in range(QUARTERS)]
    chunk_rows = [[c * chunk for c in seconds[h]] for h in range(QUARTERS)]
    own_chunks = [[group_rows[h][0] + c for c in chunk_rows[h]] for h in range(QUARTERS)]
    piece_rows = [f * piece for f in feats]
    mine = pl.ds(feat * piece, piece)
    everything = tuple(range(QUARTERS))

    def along(axis, d):
        return {"samp": neighbour[axis % 2][d]}

    def remote(src, dst, send, recv, device):
        return pltpu.make_async_remote_copy(
            src_ref=src, dst_ref=dst, send_sem=send, recv_sem=recv, device_id=device, device_id_type=MESH)

    def drain(ref, sem):
        pltpu.make_async_copy(ref, ref, sem).wait()

    def group_at(h, d):
        return pl.ds(group_rows[h][d], group)

    def part_at(h, e):
        return pl.ds(chunk_rows[h][e], chunk)

    def chunk_at(h, e):
        return pl.ds(own_chunks[h][e], chunk)

    def columns(p):
        return pl.ds(p * LANES, LANES)

    def rs1_copy(p, h, kind, k):
        if kind == 0:
            row, dst, sem = group_rows[h][2] + k * hg, rs1.at[p, h, k], rl_r.at[p, h, k]
        elif kind == 1:
            row, dst, sem = group_rows[h][sides[k]] + (1 - k) * hg, near.at[p, h, pl.ds((1 - k) * hg, hg)], nf_r.at[p, h]
        else:
            row, dst, sem = group_rows[h][sides[k]] + k * hg, far.at[p, h, pl.ds(k * hg, hg)], nf_r.at[p, h]
        return remote(g.at[p, pl.ds(row, hg)], dst, gs_s.at[p], sem, along(h, sides[k]))

    def rs2_copy(p, h, d):
        return remote(s1.at[p, h, part_at(h, d)], rs2.at[p, h, d - 1], gs_s.at[p], rs2_r.at[p, h], along(h + 1, d))

    def u_copy(p, i):
        return remote(u.at[p, pl.ds(piece_rows[i], piece)], ur.at[p, i], u_s.at[p], u_r.at[p], {"feat": feats[i]})

    def r_copy(ref, ss, rr, p, i):
        return remote(ref, ref, ss.at[p], rr.at[p], {"feat": feats[i]})

    class Gather:
        def __init__(self, view, r1, r2, r3, s):
            self.view, self.r1, self.r2, self.r3, self.s = view, r1, r2, r3, s

        def first(self, p, h):
            ref = self.view(p, chunk_at(h, 0))
            for d in near_first:
                remote(ref, ref, self.s.at[p], self.r1.at[p, h], along(h + 1, d)).start()

        def second(self, p, h):
            drain(self.view(p, pl.ds(0, (ring - 1) * chunk)), self.r1.at[p, h])
            ref = self.view(p, group_at(h, 0))
            if self.r2 is None:
                for d in far_first:
                    remote(ref, ref, self.s.at[p], self.r3.at[p, h], along(h, d)).start()
            else:
                for k in (0, 1):
                    remote(ref, ref, self.s.at[p], self.r2.at[p, h, k], along(h, sides[k])).start()

        def third(self, p, h):
            for k in (0, 1):
                drain(self.view(p, pl.ds(0, group)), self.r2.at[p, h, k])
                ref = self.view(p, pl.ds(group_rows[h][ring - sides[k]] + k * hg, hg))
                remote(ref, ref, self.s.at[p], self.r3.at[p, h], along(h, sides[k])).start()

        def last(self, p, h):
            drain(self.view(p, pl.ds(0, group if self.r2 is not None else (ring - 1) * group)), self.r3.at[p, h])

        def sent(self, p):
            drain(self.view(p, pl.ds(0, QUARTERS * ((ring - 1) * chunk + 3 * group))), self.s.at[p])

    ag = Gather(lambda p, at: dw.at[p, at], ag1_r, None, ag3_r, ag_s)
    wg = Gather(lambda p, at: wo.at[at, columns(p)], wg1_r, wg2_r, wg3_r, wg_s)

    def start_u(p):
        step = max(rows // 2, piece)
        for k in range(rows // step):
            at = pl.ds(k * step, step)
            u[p, at] = jnp.dot(x[at], dw[p], preferred_element_type=F32).astype(BF16)
        for i in range(len(peers)):
            u_copy(p, i).start()

    def sum_u(p):
        total = u[p, mine].astype(F32)
        drain(ur.at[p], u_r.at[p])
        for i in range(len(peers)):
            total = total + ur[p, i].astype(F32)
        drain(ur.at[p], u_s.at[p])
        return total

    def send_r(p):
        rb[p, mine] = r[p].astype(BF16)
        for i in range(len(peers)):
            r_copy(rb.at[p, mine], rg_s, rg_r, p, i).start()

    def start_g(p, hs):
        if hs == UNITS[0]:
            drain(ur.at[p], rg_r.at[p])
        for ds in ((2,), (1, ring - 1), (0,)):
            for d in ds:
                for h in hs:
                    at = group_at(h, d)
                    g[p, at] = jnp.dot(xt[at], rb[p], preferred_element_type=F32)
            for h in hs:
                for k in (0, 1):
                    if ds[0] == 2:
                        rs1_copy(p, h, 0, k).start()
                    elif ds[0]:
                        rs1_copy(p, h, 1, k).start()

    def pass_g(p, hs):
        for h in hs:
            for k in (0, 1):
                rs1_copy(p, h, 0, k).wait_recv()
                at = pl.ds(group_rows[h][sides[k]] + k * hg, hg)
                g[p, at] = g[p, at] + rs1[p, h, k]
                rs1_copy(p, h, 2, k).start()

    def mid_g(p, hs):
        for h in hs:
            drain(g.at[p, pl.ds(0, 2 * group)], nf_r.at[p, h])
            for e in far_first + [0]:
                at = part_at(h, e)
                s1[p, h, at] = g[p, chunk_at(h, e)] + near[p, h, at] + far[p, h, at]
                if e:
                    rs2_copy(p, h, e).start()

    def end_g(p, hs, last):
        for h in hs:
            drain(g.at[p, pl.ds(0, (ring - 1) * chunk)], rs2_r.at[p, h])
            total = s1[p, h, part_at(h, 0)]
            for d in range(1, ring):
                total = total + rs2[p, h, d - 1]
            delta = eta[h] * (total / samples - ridge * w[p, h])
            at = chunk_at(h, 0)
            dw[p, at] = delta.astype(BF16)
            ag.first(p, h)
            new = w[p, h] + COMBINE_WEIGHT * delta
            w[p, h] = new
            if last:
                wo[at, p * LANES:(p + 1) * LANES] = new

    loads = [pltpu.make_async_copy(w_hbm, w_in, load_sem.at[0]),
             pltpu.make_async_copy(x_hbm, x, load_sem.at[1]),
             pltpu.make_async_copy(eta_hbm, eta_in, load_sem.at[2])]
    loads += [pltpu.make_async_copy(y_hbm.at[mine, columns(p)], r.at[p], load_sem.at[3 + p]) for p in range(PARTS)]
    for load in loads:
        load.start()
    barrier = pltpu.get_barrier_semaphore()
    for d in range(1, ring):
        for axis in (0, 1):
            pl.semaphore_signal(barrier, inc=1, device_id=along(axis, d), device_id_type=MESH)
    for i in range(len(peers)):
        pl.semaphore_signal(barrier, inc=1, device_id={"feat": feats[i]}, device_id_type=MESH)
    loads[0].wait()
    for p in range(PARTS):
        dw[p] = w_in[:, p * LANES:(p + 1) * LANES].astype(BF16)
        for h in everything:
            w[p, h] = w_in[chunk_at(h, 0), p * LANES:(p + 1) * LANES]
    loads[1].wait()
    pl.semaphore_wait(barrier, 2 * (ring - 1) + len(peers))

    for p in range(PARTS):
        start_u(p)
    tile = min(width, 256)
    for k in range(width // tile):
        xt[k * tile:(k + 1) * tile] = x[:, k * tile:(k + 1) * tile].T
    loads[2].wait()
    for h in everything:
        pos = own_chunks[h][0]
        line = eta_in[pl.ds(lax.div(pos, LANES), 1), :]
        eta_t[...] = jnp.broadcast_to(line, (LANES, LANES)).T
        eta[h] = eta_t[pl.ds(lax.rem(pos, LANES), chunk), :]
    for p in range(PARTS):
        loads[3 + p].wait()
        r[p] = r[p] - sum_u(p)
        send_r(p)

    def sweep(last):
        both = [(p, hs) for p in range(PARTS) for hs in UNITS]
        for p, hs in both:
            start_g(p, hs)
        for p in range(PARTS):
            drain(ur.at[p], rg_s.at[p])
        for p, hs in both:
            pass_g(p, hs)
        for p, hs in both:
            mid_g(p, hs)
        for p, hs in both:
            end_g(p, hs, last)
        for p, hs in both:
            for h in hs:
                ag.second(p, h)
        if last:
            for p in range(PARTS):
                for h in everything:
                    wg.first(p, h)
        for p in range(PARTS):
            drain(g.at[p, pl.ds(0, QUARTERS * (3 * group + (ring - 1) * chunk))], gs_s.at[p])
            for h in everything:
                ag.last(p, h)
            ag.sent(p)
            start_u(p)
        if last:
            for p in range(PARTS):
                for h in everything:
                    wg.second(p, h)
        for p in range(PARTS):
            r[p] = r[p] - COMBINE_WEIGHT * sum_u(p)
            if last:
                ro[mine, p * LANES:(p + 1) * LANES] = r[p]
                for i in range(len(peers)):
                    r_copy(ro.at[mine, columns(p)], rf_s, rf_r, p, i).start()
            else:
                send_r(p)
        if last:
            for p in range(PARTS):
                for h in everything:
                    wg.third(p, h)

    def body(i, carry):
        sweep(False)
        return carry

    lax.fori_loop(0, SWEEPS - 1, body, 0)
    sweep(True)
    for p in range(PARTS):
        final = ro.at[pl.ds(0, len(peers) * piece), columns(p)]
        drain(final, rf_r.at[p])
        drain(final, rf_s.at[p])
    for p in range(PARTS):
        for h in everything:
            wg.last(p, h)
        wg.sent(p)


def solution(mesh):
    samp_count = mesh.shape["samp"]
    feat_count = mesh.shape["feat"]
    ring = math.isqrt(samp_count)
    chips = feat_count // 2

    def local_solve(x_loc, w_loc, y_loc, eta_loc):
        rows, width = x_loc.shape
        samples = rows * samp_count
        ridge = RIDGE_SCALE * (width * feat_count) / samples
        group = width // QUARTERS // ring
        chunk = group // ring
        piece = rows // feat_count
        npeer = feat_count - 1
        dma = pltpu.SemaphoreType.DMA
        v = pltpu.VMEM
        each = (PARTS, QUARTERS)
        scratch = [
            v((rows, width), BF16),
            v((width, rows), BF16),
            v((width, PARTS * LANES), F32),
            v(each + (chunk, LANES), F32),
            v((PARTS, piece, LANES), F32),
            v((width // LANES, LANES), F32),
            v((LANES, LANES), F32),
            v((QUARTERS, chunk, LANES), F32),
            v((PARTS, width, LANES), F32),
            v(each + (2, group // 2, LANES), F32),
            v(each + (group, LANES), F32),
            v(each + (group, LANES), F32),
            v(each + (group, LANES), F32),
            v(each + (ring - 1, chunk, LANES), F32),
            v((PARTS, width, LANES), BF16),
            v((PARTS, rows, LANES), BF16),
            v((PARTS, npeer, piece, LANES), BF16),
            v((PARTS, rows, LANES), BF16),
            dma((3 + PARTS,)),
            dma(each + (2,)), dma(each), dma(each), dma((PARTS,)),
            dma(each), dma(each), dma((PARTS,)),
            dma((PARTS,)), dma((PARTS,)), dma((PARTS,)), dma((PARTS,)),
            dma(each), dma(each + (2,)), dma(each), dma((PARTS,)),
            dma((PARTS,)), dma((PARTS,)),
        ]
        return pl.pallas_call(
            functools.partial(ridge_kernel, ring, chips, samples, ridge),
            out_shape=[pltpu.VMEM(w_loc.shape, F32), pltpu.VMEM(y_loc.shape, F32)],
            in_specs=[pl.BlockSpec(memory_space=pltpu.HBM)] * 4,
            out_specs=[pl.BlockSpec(memory_space=pltpu.VMEM)] * 2,
            scratch_shapes=scratch,
            compiler_params=pltpu.CompilerParams(
                collective_id=0, has_side_effects=True, vmem_limit_bytes=56 * 1024 * 1024),
        )(x_loc, w_loc, y_loc, eta_loc.reshape(width // LANES, LANES))

    return jax.shard_map(
        local_solve,
        mesh=mesh,
        in_specs=(P(("prob", "samp"), "feat"), P(("prob", "feat"), None), P(("prob", "samp"), None), P(("prob", "feat"))),
        out_specs=(P(("prob", "feat"), None), P(("prob", "samp"), None)),
        check_vma=False,
    )
```

```python
import functools
import math

import jax
import jax.numpy as jnp
from jax import lax
from jax.experimental import pallas as pl
from jax.experimental.pallas import tpu as pltpu
from jax.sharding import PartitionSpec as P

SWEEPS = 4
COMBINE_WEIGHT = 0.8
RIDGE_SCALE = 0.1
PARTS = 2
LANES = 128
QUARTERS = 8
UNITS = ((0, 1), (2, 3), (4, 5), (6, 7))
MESH = pl.DeviceIdType.MESH
F32 = jnp.float32
BF16 = jnp.bfloat16


def ridge_kernel(ring, chips, samples, ridge, x_hbm, w_hbm, y_hbm, eta_hbm, wo, ro,
                 x, xt, w_in, w, r, eta_in, eta_t, eta, g, rs1, near, far, s1, rs2, dw, u, ur, rb,
                 load_sem, rl_r, nf_r, rs2_r, gs_s, ag1_r, ag3_r, ag_s,
                 u_s, u_r, rg_s, rg_r, wg1_r, wg2_r, wg3_r, wg_s, rf_s, rf_r):
    samp = lax.axis_index("samp")
    feat = lax.axis_index("feat")
    rows, width = x.shape
    quarter = width // QUARTERS
    group = quarter // ring
    chunk = group // ring
    hg = group // 2
    piece = rows // (2 * chips)
    cy, cz = lax.rem(samp, ring), lax.div(samp, ring)
    cx, core = lax.div(feat, 2), lax.rem(feat, 2)
    ys = [cy] + [lax.rem(cy + d, ring) for d in range(1, ring)]
    zs = [cz] + [lax.rem(cz + d, ring) for d in range(1, ring)]
    neighbour = [[cz * ring + c for c in ys], [c * ring + cy for c in zs]]
    far_first = sorted(range(1, ring), key=lambda d: -min(d, ring - d))
    near_first = far_first[::-1]
    sides = (1, ring - 1)
    across = sorted(range(1, chips), key=lambda d: -min(d, chips - d))
    peers = [(dx, dc) for dx in across + [0] for dc in (0, 1) if dx or dc]
    xs = [cx] + [lax.rem(cx + d, chips) for d in range(1, chips)]
    cores = [core, 1 - core]
    feats = [xs[dx] * 2 + cores[dc] for dx, dc in peers]
    firsts = [(ys, zs)[h % 2] for h in range(QUARTERS)]
    seconds = [(zs, ys)[h % 2] for h in range(QUARTERS)]
    group_rows = [[h * quarter + c * group for c in firsts[h]] for h in range(QUARTERS)]
    chunk_rows = [[c * chunk for c in seconds[h]] for h in range(QUARTERS)]
    own_chunks = [[group_rows[h][0] + c for c in chunk_rows[h]] for h in range(QUARTERS)]
    piece_rows = [f * piece for f in feats]
    mine = pl.ds(feat * piece, piece)
    everything = tuple(range(QUARTERS))

    def along(axis, d):
        return {"samp": neighbour[axis % 2][d]}

    def remote(src, dst, send, recv, device):
        return pltpu.make_async_remote_copy(
            src_ref=src, dst_ref=dst, send_sem=send, recv_sem=recv, device_id=device, device_id_type=MESH)

    def drain(ref, sem):
        pltpu.make_async_copy(ref, ref, sem).wait()

    def group_at(h, d):
        return pl.ds(group_rows[h][d], group)

    def part_at(h, e):
        return pl.ds(chunk_rows[h][e], chunk)

    def chunk_at(h, e):
        return pl.ds(own_chunks[h][e], chunk)

    def columns(p):
        return pl.ds(p * LANES, LANES)

    def rs1_copy(p, h, kind, k):
        if kind == 0:
            row, dst, sem = group_rows[h][2] + k * hg, rs1.at[p, h, k], rl_r.at[p, h, k]
        elif kind == 1:
            row, dst, sem = group_rows[h][sides[k]] + (1 - k) * hg, near.at[p, h, pl.ds((1 - k) * hg, hg)], nf_r.at[p, h]
        else:
            row, dst, sem = group_rows[h][sides[k]] + k * hg, far.at[p, h, pl.ds(k * hg, hg)], nf_r.at[p, h]
        return remote(g.at[p, pl.ds(row, hg)], dst, gs_s.at[p], sem, along(h, sides[k]))

    def rs2_copy(p, h, d):
        return remote(s1.at[p, h, part_at(h, d)], rs2.at[p, h, d - 1], gs_s.at[p], rs2_r.at[p, h], along(h + 1, d))

    def u_copy(p, i):
        return remote(u.at[p, pl.ds(piece_rows[i], piece)], ur.at[p, i], u_s.at[p], u_r.at[p], {"feat": feats[i]})

    def r_copy(ref, ss, rr, p, i):
        return remote(ref, ref, ss.at[p], rr.at[p], {"feat": feats[i]})

    class Gather:
        def __init__(self, view, r1, r2, r3, s):
            self.view, self.r1, self.r2, self.r3, self.s = view, r1, r2, r3, s

        def first(self, p, h):
            ref = self.view(p, chunk_at(h, 0))
            for d in near_first:
                remote(ref, ref, self.s.at[p], self.r1.at[p, h], along(h + 1, d)).start()

        def second(self, p, h):
            drain(self.view(p, pl.ds(0, (ring - 1) * chunk)), self.r1.at[p, h])
            ref = self.view(p, group_at(h, 0))
            if self.r2 is None:
                for d in far_first:
                    remote(ref, ref, self.s.at[p], self.r3.at[p, h], along(h, d)).start()
            else:
                for k in (0, 1):
                    remote(ref, ref, self.s.at[p], self.r2.at[p, h, k], along(h, sides[k])).start()

        def third(self, p, h):
            for k in (0, 1):
                drain(self.view(p, pl.ds(0, group)), self.r2.at[p, h, k])
                ref = self.view(p, pl.ds(group_rows[h][ring - sides[k]] + k * hg, hg))
                remote(ref, ref, self.s.at[p], self.r3.at[p, h], along(h, sides[k])).start()

        def last(self, p, h):
            drain(self.view(p, pl.ds(0, group if self.r2 is not None else (ring - 1) * group)), self.r3.at[p, h])

        def sent(self, p):
            drain(self.view(p, pl.ds(0, QUARTERS * ((ring - 1) * chunk + 3 * group))), self.s.at[p])

    ag = Gather(lambda p, at: dw.at[p, at], ag1_r, None, ag3_r, ag_s)
    wg = Gather(lambda p, at: wo.at[at, columns(p)], wg1_r, wg2_r, wg3_r, wg_s)

    def start_u(p):
        step = max(rows // 2, piece)
        for k in range(rows // step):
            at = pl.ds(k * step, step)
            u[p, at] = jnp.dot(x[at], dw[p], preferred_element_type=F32).astype(BF16)
        for i in range(len(peers)):
            u_copy(p, i).start()

    def sum_u(p):
        total = u[p, mine].astype(F32)
        drain(ur.at[p], u_r.at[p])
        for i in range(len(peers)):
            total = total + ur[p, i].astype(F32)
        drain(ur.at[p], u_s.at[p])
        return total

    def send_r(p):
        rb[p, mine] = r[p].astype(BF16)
        for i in range(len(peers)):
            r_copy(rb.at[p, mine], rg_s, rg_r, p, i).start()

    def start_g(p, hs):
        if hs == UNITS[0]:
            drain(ur.at[p], rg_r.at[p])
        at = slice(hs[0] * quarter, (hs[-1] + 1) * quarter)
        g[p, at] = jnp.dot(xt[at], rb[p], preferred_element_type=F32)
        for kind in (0, 1):
            for h in hs:
                for k in (0, 1):
                    rs1_copy(p, h, kind, k).start()

    def pass_g(p, hs):
        for h in hs:
            for k in (0, 1):
                rs1_copy(p, h, 0, k).wait_recv()
                at = pl.ds(group_rows[h][sides[k]] + k * hg, hg)
                g[p, at] = g[p, at] + rs1[p, h, k]
                rs1_copy(p, h, 2, k).start()

    def mid_g(p, hs):
        for h in hs:
            drain(g.at[p, pl.ds(0, 2 * group)], nf_r.at[p, h])
            for e in far_first + [0]:
                at = part_at(h, e)
                s1[p, h, at] = g[p, chunk_at(h, e)] + near[p, h, at] + far[p, h, at]
                if e:
                    rs2_copy(p, h, e).start()

    def end_g(p, hs, last):
        for h in hs:
            drain(g.at[p, pl.ds(0, (ring - 1) * chunk)], rs2_r.at[p, h])
            total = s1[p, h, part_at(h, 0)]
            for d in range(1, ring):
                total = total + rs2[p, h, d - 1]
            delta = eta[h] * (total / samples - ridge * w[p, h])
            at = chunk_at(h, 0)
            dw[p, at] = delta.astype(BF16)
            ag.first(p, h)
            new = w[p, h] + COMBINE_WEIGHT * delta
            w[p, h] = new
            if last:
                wo[at, p * LANES:(p + 1) * LANES] = new

    loads = [pltpu.make_async_copy(w_hbm, w_in, load_sem.at[0]),
             pltpu.make_async_copy(x_hbm, x, load_sem.at[1]),
             pltpu.make_async_copy(eta_hbm, eta_in, load_sem.at[2])]
    loads += [pltpu.make_async_copy(y_hbm.at[mine, columns(p)], r.at[p], load_sem.at[3 + p]) for p in range(PARTS)]
    for load in loads:
        load.start()
    barrier = pltpu.get_barrier_semaphore()
    for d in range(1, ring):
        for axis in (0, 1):
            pl.semaphore_signal(barrier, inc=1, device_id=along(axis, d), device_id_type=MESH)
    for i in range(len(peers)):
        pl.semaphore_signal(barrier, inc=1, device_id={"feat": feats[i]}, device_id_type=MESH)
    loads[0].wait()
    for p in range(PARTS):
        dw[p] = w_in[:, p * LANES:(p + 1) * LANES].astype(BF16)
        for h in everything:
            w[p, h] = w_in[chunk_at(h, 0), p * LANES:(p + 1) * LANES]
    loads[1].wait()
    pl.semaphore_wait(barrier, 2 * (ring - 1) + len(peers))

    for p in range(PARTS):
        start_u(p)
    tile = min(width, 256)
    for k in range(width // tile):
        xt[k * tile:(k + 1) * tile] = x[:, k * tile:(k + 1) * tile].T
    loads[2].wait()
    for h in everything:
        pos = own_chunks[h][0]
        line = eta_in[pl.ds(lax.div(pos, LANES), 1), :]
        eta_t[...] = jnp.broadcast_to(line, (LANES, LANES)).T
        eta[h] = eta_t[pl.ds(lax.rem(pos, LANES), chunk), :]
    for p in range(PARTS):
        loads[3 + p].wait()
        r[p] = r[p] - sum_u(p)
        send_r(p)

    def sweep(last):
        both = [(p, hs) for p in range(PARTS) for hs in UNITS]
        for p, hs in both:
            start_g(p, hs)
        for p in range(PARTS):
            drain(ur.at[p], rg_s.at[p])
        for p, hs in both:
            pass_g(p, hs)
        for p, hs in both:
            mid_g(p, hs)
        for p, hs in both:
            end_g(p, hs, last)
        for p, hs in both:
            for h in hs:
                ag.second(p, h)
        if last:
            for p in range(PARTS):
                for h in everything:
                    wg.first(p, h)
        for p in range(PARTS):
            drain(g.at[p, pl.ds(0, QUARTERS * (3 * group + (ring - 1) * chunk))], gs_s.at[p])
            for h in everything:
                ag.last(p, h)
            ag.sent(p)
            start_u(p)
        if last:
            for p in range(PARTS):
                for h in everything:
                    wg.second(p, h)
        for p in range(PARTS):
            r[p] = r[p] - COMBINE_WEIGHT * sum_u(p)
            if last:
                ro[mine, p * LANES:(p + 1) * LANES] = r[p]
                for i in range(len(peers)):
                    r_copy(ro.at[mine, columns(p)], rf_s, rf_r, p, i).start()
            else:
                send_r(p)
        if last:
            for p in range(PARTS):
                for h in everything:
                    wg.third(p, h)

    def body(i, carry):
        sweep(False)
        return carry

    lax.fori_loop(0, SWEEPS - 1, body, 0)
    sweep(True)
    for p in range(PARTS):
        final = ro.at[pl.ds(0, len(peers) * piece), columns(p)]
        drain(final, rf_r.at[p])
        drain(final, rf_s.at[p])
    for p in range(PARTS):
        for h in everything:
            wg.last(p, h)
        wg.sent(p)


def solution(mesh):
    samp_count = mesh.shape["samp"]
    feat_count = mesh.shape["feat"]
    ring = math.isqrt(samp_count)
    chips = feat_count // 2

    def local_solve(x_loc, w_loc, y_loc, eta_loc):
        rows, width = x_loc.shape
        samples = rows * samp_count
        ridge = RIDGE_SCALE * (width * feat_count) / samples
        group = width // QUARTERS // ring
        chunk = group // ring
        piece = rows // feat_count
        npeer = feat_count - 1
        dma = pltpu.SemaphoreType.DMA
        v = pltpu.VMEM
        each = (PARTS, QUARTERS)
        scratch = [
            v((rows, width), BF16),
            v((width, rows), BF16),
            v((width, PARTS * LANES), F32),
            v(each + (chunk, LANES), F32),
            v((PARTS, piece, LANES), F32),
            v((width // LANES, LANES), F32),
            v((LANES, LANES), F32),
            v((QUARTERS, chunk, LANES), F32),
            v((PARTS, width, LANES), F32),
            v(each + (2, group // 2, LANES), F32),
            v(each + (group, LANES), F32),
            v(each + (group, LANES), F32),
            v(each + (group, LANES), F32),
            v(each + (ring - 1, chunk, LANES), F32),
            v((PARTS, width, LANES), BF16),
            v((PARTS, rows, LANES), BF16),
            v((PARTS, npeer, piece, LANES), BF16),
            v((PARTS, rows, LANES), BF16),
            dma((3 + PARTS,)),
            dma(each + (2,)), dma(each), dma(each), dma((PARTS,)),
            dma(each), dma(each), dma((PARTS,)),
            dma((PARTS,)), dma((PARTS,)), dma((PARTS,)), dma((PARTS,)),
            dma(each), dma(each + (2,)), dma(each), dma((PARTS,)),
            dma((PARTS,)), dma((PARTS,)),
        ]
        return pl.pallas_call(
            functools.partial(ridge_kernel, ring, chips, samples, ridge),
            out_shape=[pltpu.VMEM(w_loc.shape, F32), pltpu.VMEM(y_loc.shape, F32)],
            in_specs=[pl.BlockSpec(memory_space=pltpu.HBM)] * 4,
            out_specs=[pl.BlockSpec(memory_space=pltpu.VMEM)] * 2,
            scratch_shapes=scratch,
            compiler_params=pltpu.CompilerParams(
                collective_id=0, has_side_effects=True, vmem_limit_bytes=56 * 1024 * 1024),
        )(x_loc, w_loc, y_loc, eta_loc.reshape(width // LANES, LANES))

    return jax.shard_map(
        local_solve,
        mesh=mesh,
        in_specs=(P(("prob", "samp"), "feat"), P(("prob", "feat"), None), P(("prob", "samp"), None), P(("prob", "feat"))),
        out_specs=(P(("prob", "feat"), None), P(("prob", "samp"), None)),
        check_vma=False,
    )
```

```python
import functools
import math

import jax
import jax.numpy as jnp
from jax import lax
from jax.experimental import pallas as pl
from jax.experimental.pallas import tpu as pltpu
from jax.sharding import PartitionSpec as P

SWEEPS = 4
COMBINE_WEIGHT = 0.8
RIDGE_SCALE = 0.1
PARTS = 2
LANES = 128
QUARTERS = 8
UNITS = ((0, 1), (2, 3), (4, 5), (6, 7))
MESH = pl.DeviceIdType.MESH
F32 = jnp.float32
BF16 = jnp.bfloat16


def ridge_kernel(ring, chips, samples, ridge, x_hbm, w_hbm, y_hbm, eta_hbm, wo, ro,
                 x, xt, w_in, w, r, eta_in, eta_t, eta, g, rs1, near, far, s1, rs2, dw, u, ur, rb,
                 load_sem, rl_r, nf_r, rs2_r, gs_s, ag1_r, ag3_r, ag_s,
                 u_s, u_r, rg_s, rg_r, wg1_r, wg2_r, wg3_r, wg_s, rf_s, rf_r):
    samp = lax.axis_index("samp")
    feat = lax.axis_index("feat")
    rows, width = x.shape
    quarter = width // QUARTERS
    group = quarter // ring
    chunk = group // ring
    hg = group // 2
    piece = rows // (2 * chips)
    cy, cz = lax.rem(samp, ring), lax.div(samp, ring)
    cx, core = lax.div(feat, 2), lax.rem(feat, 2)
    ys = [cy] + [lax.rem(cy + d, ring) for d in range(1, ring)]
    zs = [cz] + [lax.rem(cz + d, ring) for d in range(1, ring)]
    neighbour = [[cz * ring + c for c in ys], [c * ring + cy for c in zs]]
    far_first = sorted(range(1, ring), key=lambda d: -min(d, ring - d))
    near_first = far_first[::-1]
    sides = (1, ring - 1)
    across = sorted(range(1, chips), key=lambda d: -min(d, chips - d))
    peers = [(dx, dc) for dx in across + [0] for dc in (0, 1) if dx or dc]
    xs = [cx] + [lax.rem(cx + d, chips) for d in range(1, chips)]
    cores = [core, 1 - core]
    feats = [xs[dx] * 2 + cores[dc] for dx, dc in peers]
    firsts = [(ys, zs)[h % 2] for h in range(QUARTERS)]
    seconds = [(zs, ys)[h % 2] for h in range(QUARTERS)]
    group_rows = [[h * quarter + c * group for c in firsts[h]] for h in range(QUARTERS)]
    chunk_rows = [[c * chunk for c in seconds[h]] for h in range(QUARTERS)]
    own_chunks = [[group_rows[h][0] + c for c in chunk_rows[h]] for h in range(QUARTERS)]
    piece_rows = [f * piece for f in feats]
    mine = pl.ds(feat * piece, piece)
    everything = tuple(range(QUARTERS))

    def along(axis, d):
        return {"samp": neighbour[axis % 2][d]}

    def remote(src, dst, send, recv, device):
        return pltpu.make_async_remote_copy(
            src_ref=src, dst_ref=dst, send_sem=send, recv_sem=recv, device_id=device, device_id_type=MESH)

    def drain(ref, sem):
        pltpu.make_async_copy(ref, ref, sem).wait()

    def group_at(h, d):
        return pl.ds(group_rows[h][d], group)

    def part_at(h, e):
        return pl.ds(chunk_rows[h][e], chunk)

    def chunk_at(h, e):
        return pl.ds(own_chunks[h][e], chunk)

    def columns(p):
        return pl.ds(p * LANES, LANES)

    def rs1_copy(p, h, kind, k):
        if kind == 0:
            row, dst, sem = group_rows[h][2] + k * hg, rs1.at[p, h, k], rl_r.at[p, h, k]
        elif kind == 1:
            row, dst, sem = group_rows[h][sides[k]] + (1 - k) * hg, near.at[p, h, pl.ds((1 - k) * hg, hg)], nf_r.at[p, h]
        else:
            row, dst, sem = group_rows[h][sides[k]] + k * hg, far.at[p, h, pl.ds(k * hg, hg)], nf_r.at[p, h]
        return remote(g.at[p, pl.ds(row, hg)], dst, gs_s.at[p], sem, along(h, sides[k]))

    def rs2_copy(p, h, d):
        return remote(s1.at[p, h, part_at(h, d)], rs2.at[p, h, d - 1], gs_s.at[p], rs2_r.at[p, h], along(h + 1, d))

    def u_copy(p, i):
        return remote(u.at[p, pl.ds(piece_rows[i], piece)], ur.at[p, i], u_s.at[p], u_r.at[p], {"feat": feats[i]})

    def r_copy(ref, ss, rr, p, i):
        return remote(ref, ref, ss.at[p], rr.at[p], {"feat": feats[i]})

    class Gather:
        def __init__(self, view, r1, r2, r3, s):
            self.view, self.r1, self.r2, self.r3, self.s = view, r1, r2, r3, s

        def first(self, p, h):
            ref = self.view(p, chunk_at(h, 0))
            for d in near_first:
                remote(ref, ref, self.s.at[p], self.r1.at[p, h], along(h + 1, d)).start()

        def second(self, p, h):
            drain(self.view(p, pl.ds(0, (ring - 1) * chunk)), self.r1.at[p, h])
            ref = self.view(p, group_at(h, 0))
            if self.r2 is None:
                for d in far_first:
                    remote(ref, ref, self.s.at[p], self.r3.at[p, h], along(h, d)).start()
            else:
                for k in (0, 1):
                    remote(ref, ref, self.s.at[p], self.r2.at[p, h, k], along(h, sides[k])).start()

        def third(self, p, h):
            for k in (0, 1):
                drain(self.view(p, pl.ds(0, group)), self.r2.at[p, h, k])
                ref = self.view(p, pl.ds(group_rows[h][ring - sides[k]] + k * hg, hg))
                remote(ref, ref, self.s.at[p], self.r3.at[p, h], along(h, sides[k])).start()

        def last(self, p, h):
            drain(self.view(p, pl.ds(0, group if self.r2 is not None else (ring - 1) * group)), self.r3.at[p, h])

        def sent(self, p):
            drain(self.view(p, pl.ds(0, QUARTERS * ((ring - 1) * chunk + 3 * group))), self.s.at[p])

    ag = Gather(lambda p, at: dw.at[p, at], ag1_r, None, ag3_r, ag_s)
    wg = Gather(lambda p, at: wo.at[at, columns(p)], wg1_r, wg2_r, wg3_r, wg_s)

    def start_u(p):
        step = max(rows // 2, piece)
        for k in range(rows // step):
            at = pl.ds(k * step, step)
            u[p, at] = jnp.dot(x[at], dw[p], preferred_element_type=F32).astype(BF16)
        for i in range(len(peers)):
            u_copy(p, i).start()

    def sum_u(p):
        total = u[p, mine].astype(F32)
        drain(ur.at[p], u_r.at[p])
        for i in range(len(peers)):
            total = total + ur[p, i].astype(F32)
        drain(ur.at[p], u_s.at[p])
        return total

    def send_r(p):
        rb[p, mine] = r[p].astype(BF16)
        for i in range(len(peers)):
            r_copy(rb.at[p, mine], rg_s, rg_r, p, i).start()

    def start_g(p, hs):
        if hs == UNITS[0]:
            drain(ur.at[p], rg_r.at[p])
        at = slice(hs[0] * quarter, (hs[-1] + 1) * quarter)
        g[p, at] = jnp.dot(xt[at], rb[p], preferred_element_type=F32)
        for kind in (0, 1):
            for h in hs:
                for k in (0, 1):
                    rs1_copy(p, h, kind, k).start()

    def pass_g(p, hs):
        for h in hs:
            for k in (0, 1):
                rs1_copy(p, h, 0, k).wait_recv()
                at = pl.ds(group_rows[h][sides[k]] + k * hg, hg)
                g[p, at] = g[p, at] + rs1[p, h, k]
                rs1_copy(p, h, 2, k).start()

    def mid_g(p, hs):
        for h in hs:
            drain(g.at[p, pl.ds(0, 2 * group)], nf_r.at[p, h])
            for e in far_first + [0]:
                at = part_at(h, e)
                s1[p, h, at] = g[p, chunk_at(h, e)] + near[p, h, at] + far[p, h, at]
                if e:
                    rs2_copy(p, h, e).start()

    def end_g(p, hs, last):
        for h in hs:
            drain(g.at[p, pl.ds(0, (ring - 1) * chunk)], rs2_r.at[p, h])
            total = s1[p, h, part_at(h, 0)]
            for d in range(1, ring):
                total = total + rs2[p, h, d - 1]
            delta = eta[h] * (total / samples - ridge * w[p, h])
            at = chunk_at(h, 0)
            dw[p, at] = delta.astype(BF16)
            ag.first(p, h)
            new = w[p, h] + COMBINE_WEIGHT * delta
            w[p, h] = new
            if last:
                wo[at, p * LANES:(p + 1) * LANES] = new

    loads = [pltpu.make_async_copy(w_hbm, w_in, load_sem.at[0]),
             pltpu.make_async_copy(x_hbm, x, load_sem.at[1]),
             pltpu.make_async_copy(eta_hbm, eta_in, load_sem.at[2])]
    loads += [pltpu.make_async_copy(y_hbm.at[mine, columns(p)], r.at[p], load_sem.at[3 + p]) for p in range(PARTS)]
    for load in loads:
        load.start()
    barrier = pltpu.get_barrier_semaphore()
    for d in range(1, ring):
        for axis in (0, 1):
            pl.semaphore_signal(barrier, inc=1, device_id=along(axis, d), device_id_type=MESH)
    for i in range(len(peers)):
        pl.semaphore_signal(barrier, inc=1, device_id={"feat": feats[i]}, device_id_type=MESH)
    loads[0].wait()
    for p in range(PARTS):
        dw[p] = w_in[:, p * LANES:(p + 1) * LANES].astype(BF16)
        for h in everything:
            w[p, h] = w_in[chunk_at(h, 0), p * LANES:(p + 1) * LANES]
    loads[1].wait()
    pl.semaphore_wait(barrier, 2 * (ring - 1) + len(peers))

    for p in range(PARTS):
        start_u(p)
    tile = min(width, 256)
    for k in range(width // tile):
        xt[k * tile:(k + 1) * tile] = x[:, k * tile:(k + 1) * tile].T
    loads[2].wait()
    for h in everything:
        pos = own_chunks[h][0]
        line = eta_in[pl.ds(lax.div(pos, LANES), 1), :]
        eta_t[...] = jnp.broadcast_to(line, (LANES, LANES)).T
        eta[h] = eta_t[pl.ds(lax.rem(pos, LANES), chunk), :]
    for p in range(PARTS):
        loads[3 + p].wait()
        r[p] = r[p] - sum_u(p)
        send_r(p)

    def sweep(last):
        def first_g(p):
            for hs in UNITS:
                start_g(p, hs)
            drain(ur.at[p], rg_s.at[p])

        def each_unit(stage, p, *more):
            for hs in UNITS:
                stage(p, hs, *more)

        def second(p):
            for h in everything:
                ag.second(p, h)

        def finish(p):
            drain(g.at[p, pl.ds(0, QUARTERS * (3 * group + (ring - 1) * chunk))], gs_s.at[p])
            for h in everything:
                ag.last(p, h)
            ag.sent(p)
            start_u(p)

        def update(p):
            r[p] = r[p] - COMBINE_WEIGHT * sum_u(p)
            if last:
                ro[mine, p * LANES:(p + 1) * LANES] = r[p]
                for i in range(len(peers)):
                    r_copy(ro.at[mine, columns(p)], rf_s, rf_r, p, i).start()
            else:
                send_r(p)

        def start_w(p):
            if last:
                for h in everything:
                    wg.first(p, h)

        first_g(0)
        each_unit(pass_g, 0)
        first_g(1)
        each_unit(mid_g, 0)
        each_unit(pass_g, 1)
        each_unit(end_g, 0, last)
        each_unit(mid_g, 1)
        second(0)
        each_unit(end_g, 1, last)
        start_w(0)
        finish(0)
        second(1)
        start_w(1)
        update(0)
        finish(1)
        if last:
            for p in range(PARTS):
                for h in everything:
                    wg.second(p, h)
        update(1)
        if last:
            for p in range(PARTS):
                for h in everything:
                    wg.third(p, h)

    def body(i, carry):
        sweep(False)
        return carry

    lax.fori_loop(0, SWEEPS - 1, body, 0)
    sweep(True)
    for p in range(PARTS):
        final = ro.at[pl.ds(0, len(peers) * piece), columns(p)]
        drain(final, rf_r.at[p])
        drain(final, rf_s.at[p])
    for p in range(PARTS):
        for h in everything:
            wg.last(p, h)
        wg.sent(p)


def solution(mesh):
    samp_count = mesh.shape["samp"]
    feat_count = mesh.shape["feat"]
    ring = math.isqrt(samp_count)
    chips = feat_count // 2

    def local_solve(x_loc, w_loc, y_loc, eta_loc):
        rows, width = x_loc.shape
        samples = rows * samp_count
        ridge = RIDGE_SCALE * (width * feat_count) / samples
        group = width // QUARTERS // ring
        chunk = group // ring
        piece = rows // feat_count
        npeer = feat_count - 1
        dma = pltpu.SemaphoreType.DMA
        v = pltpu.VMEM
        each = (PARTS, QUARTERS)
        scratch = [
            v((rows, width), BF16),
            v((width, rows), BF16),
            v((width, PARTS * LANES), F32),
            v(each + (chunk, LANES), F32),
            v((PARTS, piece, LANES), F32),
            v((width // LANES, LANES), F32),
            v((LANES, LANES), F32),
            v((QUARTERS, chunk, LANES), F32),
            v((PARTS, width, LANES), F32),
            v(each + (2, group // 2, LANES), F32),
            v(each + (group, LANES), F32),
            v(each + (group, LANES), F32),
            v(each + (group, LANES), F32),
            v(each + (ring - 1, chunk, LANES), F32),
            v((PARTS, width, LANES), BF16),
            v((PARTS, rows, LANES), BF16),
            v((PARTS, npeer, piece, LANES), BF16),
            v((PARTS, rows, LANES), BF16),
            dma((3 + PARTS,)),
            dma(each + (2,)), dma(each), dma(each), dma((PARTS,)),
            dma(each), dma(each), dma((PARTS,)),
            dma((PARTS,)), dma((PARTS,)), dma((PARTS,)), dma((PARTS,)),
            dma(each), dma(each + (2,)), dma(each), dma((PARTS,)),
            dma((PARTS,)), dma((PARTS,)),
        ]
        return pl.pallas_call(
            functools.partial(ridge_kernel, ring, chips, samples, ridge),
            out_shape=[pltpu.VMEM(w_loc.shape, F32), pltpu.VMEM(y_loc.shape, F32)],
            in_specs=[pl.BlockSpec(memory_space=pltpu.HBM)] * 4,
            out_specs=[pl.BlockSpec(memory_space=pltpu.VMEM)] * 2,
            scratch_shapes=scratch,
            compiler_params=pltpu.CompilerParams(
                collective_id=0, has_side_effects=True, vmem_limit_bytes=56 * 1024 * 1024),
        )(x_loc, w_loc, y_loc, eta_loc.reshape(width // LANES, LANES))

    return jax.shard_map(
        local_solve,
        mesh=mesh,
        in_specs=(P(("prob", "samp"), "feat"), P(("prob", "feat"), None), P(("prob", "samp"), None), P(("prob", "feat"))),
        out_specs=(P(("prob", "feat"), None), P(("prob", "samp"), None)),
        check_vma=False,
    )
```

```python
import functools
import math

import jax
import jax.numpy as jnp
from jax import lax
from jax.experimental import pallas as pl
from jax.experimental.pallas import tpu as pltpu
from jax.sharding import PartitionSpec as P

SWEEPS = 4
COMBINE_WEIGHT = 0.8
RIDGE_SCALE = 0.1
PARTS = 2
LANES = 128
STORES = 4
QUARTERS = 8
UNITS = ((0, 1), (2, 3), (4, 5), (6, 7))
MESH = pl.DeviceIdType.MESH
F32 = jnp.float32
BF16 = jnp.bfloat16


def ridge_kernel(ring, chips, samples, ridge, x_hbm, w_hbm, y_hbm, eta_hbm, wo, ro,
                 x, xt, w_in, w, r, eta_in, eta_t, eta, g, rs1, near, far, s1, rs2, dw, u, ur, rb,
                 load_sem, rl_r, nf_r, rs2_r, gs_s, ag1_r, ag3_r, ag_s,
                 u_s, u_r, rg_s, rg_r, wg1_r, wg2_r, wg3_r, wg_s, rf_s, rf_r):
    samp = lax.axis_index("samp")
    feat = lax.axis_index("feat")
    rows, width = x.shape
    quarter = width // QUARTERS
    group = quarter // ring
    chunk = group // ring
    hg = group // 2
    piece = rows // (2 * chips)
    cy, cz = lax.rem(samp, ring), lax.div(samp, ring)
    cx, core = lax.div(feat, 2), lax.rem(feat, 2)
    ys = [cy] + [lax.rem(cy + d, ring) for d in range(1, ring)]
    zs = [cz] + [lax.rem(cz + d, ring) for d in range(1, ring)]
    neighbour = [[cz * ring + c for c in ys], [c * ring + cy for c in zs]]
    far_first = sorted(range(1, ring), key=lambda d: -min(d, ring - d))
    near_first = far_first[::-1]
    sides = (1, ring - 1)
    across = sorted(range(1, chips), key=lambda d: -min(d, chips - d))
    peers = [(dx, dc) for dx in across + [0] for dc in (0, 1) if dx or dc]
    xs = [cx] + [lax.rem(cx + d, chips) for d in range(1, chips)]
    cores = [core, 1 - core]
    feats = [xs[dx] * 2 + cores[dc] for dx, dc in peers]
    firsts = [(ys, zs)[h % 2] for h in range(QUARTERS)]
    seconds = [(zs, ys)[h % 2] for h in range(QUARTERS)]
    group_rows = [[h * quarter + c * group for c in firsts[h]] for h in range(QUARTERS)]
    chunk_rows = [[c * chunk for c in seconds[h]] for h in range(QUARTERS)]
    own_chunks = [[group_rows[h][0] + c for c in chunk_rows[h]] for h in range(QUARTERS)]
    piece_rows = [f * piece for f in feats]
    mine = pl.ds(feat * piece, piece)
    everything = tuple(range(QUARTERS))

    def along(axis, d):
        return {"samp": neighbour[axis % 2][d]}

    def remote(src, dst, send, recv, device):
        return pltpu.make_async_remote_copy(
            src_ref=src, dst_ref=dst, send_sem=send, recv_sem=recv, device_id=device, device_id_type=MESH)

    def drain(ref, sem):
        pltpu.make_async_copy(ref, ref, sem).wait()

    def group_at(h, d):
        return pl.ds(group_rows[h][d], group)

    def part_at(h, e):
        return pl.ds(chunk_rows[h][e], chunk)

    def chunk_at(h, e):
        return pl.ds(own_chunks[h][e], chunk)

    def columns(p):
        return pl.ds(p * LANES, LANES)

    def rs1_copy(p, h, kind, k):
        if kind == 0:
            row, dst, sem = group_rows[h][2] + k * hg, rs1.at[p, h, k], rl_r.at[p, h, k]
        elif kind == 1:
            row, dst, sem = group_rows[h][sides[k]] + (1 - k) * hg, near.at[p, h, pl.ds((1 - k) * hg, hg)], nf_r.at[p, h]
        else:
            row, dst, sem = group_rows[h][sides[k]] + k * hg, far.at[p, h, pl.ds(k * hg, hg)], nf_r.at[p, h]
        return remote(g.at[p, pl.ds(row, hg)], dst, gs_s.at[p], sem, along(h, sides[k]))

    def rs2_copy(p, h, d):
        return remote(s1.at[p, h, part_at(h, d)], rs2.at[p, h, d - 1], gs_s.at[p], rs2_r.at[p, h], along(h + 1, d))

    def u_copy(p, i):
        return remote(u.at[p, pl.ds(piece_rows[i], piece)], ur.at[p, i], u_s.at[p], u_r.at[p], {"feat": feats[i]})

    def r_copy(ref, ss, rr, p, i):
        return remote(ref, ref, ss.at[p], rr.at[p], {"feat": feats[i]})

    class Gather:
        def __init__(self, view, r1, r2, r3, s):
            self.view, self.r1, self.r2, self.r3, self.s = view, r1, r2, r3, s

        def first(self, p, h):
            ref = self.view(p, chunk_at(h, 0))
            for d in near_first:
                remote(ref, ref, self.s.at[p], self.r1.at[p, h], along(h + 1, d)).start()

        def second(self, p, h):
            drain(self.view(p, pl.ds(0, (ring - 1) * chunk)), self.r1.at[p, h])
            ref = self.view(p, group_at(h, 0))
            if self.r2 is None:
                for d in far_first:
                    remote(ref, ref, self.s.at[p], self.r3.at[p, h], along(h, d)).start()
            else:
                for k in (0, 1):
                    remote(ref, ref, self.s.at[p], self.r2.at[p, h, k], along(h, sides[k])).start()

        def third(self, p, h):
            for k in (0, 1):
                drain(self.view(p, pl.ds(0, group)), self.r2.at[p, h, k])
                ref = self.view(p, pl.ds(group_rows[h][ring - sides[k]] + k * hg, hg))
                remote(ref, ref, self.s.at[p], self.r3.at[p, h], along(h, sides[k])).start()

        def last(self, p, h):
            drain(self.view(p, pl.ds(0, group if self.r2 is not None else (ring - 1) * group)), self.r3.at[p, h])

        def sent(self, p):
            drain(self.view(p, pl.ds(0, QUARTERS * ((ring - 1) * chunk + 3 * group))), self.s.at[p])

    ag = Gather(lambda p, at: dw.at[p, at], ag1_r, None, ag3_r, ag_s)
    wg = Gather(lambda p, at: wo.at[at, columns(p)], wg1_r, wg2_r, wg3_r, wg_s)

    def take_u(p):
        step = max(rows // 2, piece)
        for k in range(rows // step):
            at = pl.ds(k * step, step)
            u[p, at] = jnp.dot(x[at], dw[p], preferred_element_type=F32).astype(BF16)

    def send_u(p):
        for i in range(len(peers)):
            u_copy(p, i).start()

    def sum_u(p):
        total = u[p, mine].astype(F32)
        drain(ur.at[p], u_r.at[p])
        for i in range(len(peers)):
            total = total + ur[p, i].astype(F32)
        drain(ur.at[p], u_s.at[p])
        return total

    def send_r(p):
        rb[p, mine] = r[p].astype(BF16)
        for i in range(len(peers)):
            r_copy(rb.at[p, mine], rg_s, rg_r, p, i).start()

    def start_g(p, hs):
        if hs == UNITS[0]:
            drain(ur.at[p], rg_r.at[p])
        for ds in ((2,), (1, ring - 1), (0,)):
            for d in ds:
                for h in hs:
                    at = group_at(h, d)
                    g[p, at] = jnp.dot(xt[at], rb[p], preferred_element_type=F32)
            for h in hs:
                for k in (0, 1):
                    if ds[0] == 2:
                        rs1_copy(p, h, 0, k).start()
                    elif ds[0]:
                        rs1_copy(p, h, 1, k).start()

    def pass_g(p, hs):
        for h in hs:
            for k in (0, 1):
                rs1_copy(p, h, 0, k).wait_recv()
                at = pl.ds(group_rows[h][sides[k]] + k * hg, hg)
                g[p, at] = g[p, at] + rs1[p, h, k]
                rs1_copy(p, h, 2, k).start()

    def mid_g(p, hs):
        for h in hs:
            drain(g.at[p, pl.ds(0, 2 * group)], nf_r.at[p, h])
            for e in far_first + [0]:
                at = part_at(h, e)
                s1[p, h, at] = g[p, chunk_at(h, e)] + near[p, h, at] + far[p, h, at]
                if e:
                    rs2_copy(p, h, e).start()

    def end_g(p, hs, last):
        for h in hs:
            drain(g.at[p, pl.ds(0, (ring - 1) * chunk)], rs2_r.at[p, h])
            total = s1[p, h, part_at(h, 0)]
            for d in range(1, ring):
                total = total + rs2[p, h, d - 1]
            delta = eta[h] * (total / samples - ridge * w[p, h])
            at = chunk_at(h, 0)
            dw[p, at] = delta.astype(BF16)
            ag.first(p, h)
            new = w[p, h] + COMBINE_WEIGHT * delta
            w[p, h] = new
            if last:
                wo[at, p * LANES:(p + 1) * LANES] = new

    loads = [pltpu.make_async_copy(w_hbm, w_in, load_sem.at[0]),
             pltpu.make_async_copy(x_hbm, x, load_sem.at[1]),
             pltpu.make_async_copy(eta_hbm, eta_in, load_sem.at[2])]
    loads += [pltpu.make_async_copy(y_hbm.at[mine, columns(p)], r.at[p], load_sem.at[3 + p]) for p in range(PARTS)]
    for load in loads:
        load.start()
    barrier = pltpu.get_barrier_semaphore()
    for d in range(1, ring):
        for axis in (0, 1):
            pl.semaphore_signal(barrier, inc=1, device_id=along(axis, d), device_id_type=MESH)
    for i in range(len(peers)):
        pl.semaphore_signal(barrier, inc=1, device_id={"feat": feats[i]}, device_id_type=MESH)
    loads[0].wait()
    for p in range(PARTS):
        dw[p] = w_in[:, p * LANES:(p + 1) * LANES].astype(BF16)
        for h in everything:
            w[p, h] = w_in[chunk_at(h, 0), p * LANES:(p + 1) * LANES]
    loads[1].wait()
    take_u(0)
    pl.semaphore_wait(barrier, 2 * (ring - 1) + len(peers))
    send_u(0)
    for p in range(1, PARTS):
        take_u(p)
        send_u(p)
    tile = min(width, 256)
    for k in range(width // tile):
        xt[k * tile:(k + 1) * tile] = x[:, k * tile:(k + 1) * tile].T
    loads[2].wait()
    for h in everything:
        pos = own_chunks[h][0]
        line = eta_in[pl.ds(lax.div(pos, LANES), 1), :]
        eta_t[...] = jnp.broadcast_to(line, (LANES, LANES)).T
        eta[h] = eta_t[pl.ds(lax.rem(pos, LANES), chunk), :]
    for p in range(PARTS):
        loads[3 + p].wait()
        r[p] = r[p] - sum_u(p)
        send_r(p)

    def sweep(last):
        both = [(p, hs) for p in range(PARTS) for hs in UNITS]
        for p, hs in both:
            start_g(p, hs)
        for p in range(PARTS):
            drain(ur.at[p], rg_s.at[p])
        for p, hs in both:
            pass_g(p, hs)
        for p, hs in both:
            mid_g(p, hs)
        for p, hs in both:
            end_g(p, hs, last)
        for p, hs in both:
            for h in hs:
                ag.second(p, h)
        if last:
            for p in range(PARTS):
                for h in everything:
                    wg.first(p, h)
        for p in range(PARTS):
            drain(g.at[p, pl.ds(0, QUARTERS * (3 * group + (ring - 1) * chunk))], gs_s.at[p])
            for h in everything:
                ag.last(p, h)
            ag.sent(p)
            take_u(p)
            send_u(p)
        if last:
            for p in range(PARTS):
                for h in everything:
                    wg.second(p, h)
        for p in range(PARTS):
            r[p] = r[p] - COMBINE_WEIGHT * sum_u(p)
            if last:
                ro[mine, p * LANES:(p + 1) * LANES] = r[p]
                for i in range(len(peers)):
                    r_copy(ro.at[mine, columns(p)], rf_s, rf_r, p, i).start()
            else:
                send_r(p)
        if last:
            for p in range(PARTS):
                for h in everything:
                    wg.third(p, h)

    def body(i, carry):
        sweep(False)
        return carry

    lax.fori_loop(0, SWEEPS - 1, body, 0)
    sweep(True)
    for p in range(PARTS):
        final = ro.at[pl.ds(0, len(peers) * piece), columns(p)]
        drain(final, rf_r.at[p])
        drain(final, rf_s.at[p])
    for p in range(PARTS):
        for h in everything:
            wg.last(p, h)
        wg.sent(p)


def store_kernel(w_in, r_in, w_out, r_out, sem):
    rows = w_in.shape[0] // STORES
    stores = [pltpu.make_async_copy(w_in.at[pl.ds(k * rows, rows)], w_out.at[pl.ds(k * rows, rows)], sem.at[k]) for k in range(STORES)]
    stores.append(pltpu.make_async_copy(r_in, r_out, sem.at[STORES]))
    for store in stores:
        store.start()
    for store in stores:
        store.wait()


def solution(mesh):
    samp_count = mesh.shape["samp"]
    feat_count = mesh.shape["feat"]
    ring = math.isqrt(samp_count)
    chips = feat_count // 2

    def local_solve(x_loc, w_loc, y_loc, eta_loc):
        rows, width = x_loc.shape
        samples = rows * samp_count
        ridge = RIDGE_SCALE * (width * feat_count) / samples
        group = width // QUARTERS // ring
        chunk = group // ring
        piece = rows // feat_count
        npeer = feat_count - 1
        dma = pltpu.SemaphoreType.DMA
        v = pltpu.VMEM
        each = (PARTS, QUARTERS)
        scratch = [
            v((rows, width), BF16),
            v((width, rows), BF16),
            v((width, PARTS * LANES), F32),
            v(each + (chunk, LANES), F32),
            v((PARTS, piece, LANES), F32),
            v((width // LANES, LANES), F32),
            v((LANES, LANES), F32),
            v((QUARTERS, chunk, LANES), F32),
            v((PARTS, width, LANES), F32),
            v(each + (2, group // 2, LANES), F32),
            v(each + (group, LANES), F32),
            v(each + (group, LANES), F32),
            v(each + (group, LANES), F32),
            v(each + (ring - 1, chunk, LANES), F32),
            v((PARTS, width, LANES), BF16),
            v((PARTS, rows, LANES), BF16),
            v((PARTS, npeer, piece, LANES), BF16),
            v((PARTS, rows, LANES), BF16),
            dma((3 + PARTS,)),
            dma(each + (2,)), dma(each), dma(each), dma((PARTS,)),
            dma(each), dma(each), dma((PARTS,)),
            dma((PARTS,)), dma((PARTS,)), dma((PARTS,)), dma((PARTS,)),
            dma(each), dma(each + (2,)), dma(each), dma((PARTS,)),
            dma((PARTS,)), dma((PARTS,)),
        ]
        solved = pl.pallas_call(
            functools.partial(ridge_kernel, ring, chips, samples, ridge),
            out_shape=[pltpu.VMEM(w_loc.shape, F32), pltpu.VMEM(y_loc.shape, F32)],
            in_specs=[pl.BlockSpec(memory_space=pltpu.HBM)] * 4,
            out_specs=[pl.BlockSpec(memory_space=pltpu.VMEM)] * 2,
            scratch_shapes=scratch,
            compiler_params=pltpu.CompilerParams(
                collective_id=0, has_side_effects=True, vmem_limit_bytes=56 * 1024 * 1024),
        )(x_loc, w_loc, y_loc, eta_loc.reshape(width // LANES, LANES))
        return pl.pallas_call(
            store_kernel,
            out_shape=[jax.ShapeDtypeStruct(w_loc.shape, F32), jax.ShapeDtypeStruct(y_loc.shape, F32)],
            in_specs=[pl.BlockSpec(memory_space=pltpu.VMEM)] * 2,
            out_specs=[pl.BlockSpec(memory_space=pltpu.HBM)] * 2,
            scratch_shapes=[dma((STORES + 1,))],
            compiler_params=pltpu.CompilerParams(vmem_limit_bytes=4 * 1024 * 1024),
        )(*solved)

    return jax.shard_map(
        local_solve,
        mesh=mesh,
        in_specs=(P(("prob", "samp"), "feat"), P(("prob", "feat"), None), P(("prob", "samp"), None), P(("prob", "feat"))),
        out_specs=(P(("prob", "feat"), None), P(("prob", "samp"), None)),
        check_vma=False,
    )
```

```python
import functools
import math

import jax
import jax.numpy as jnp
from jax import lax
from jax.experimental import pallas as pl
from jax.experimental.pallas import tpu as pltpu
from jax.sharding import PartitionSpec as P

SWEEPS = 4
COMBINE_WEIGHT = 0.8
RIDGE_SCALE = 0.1
PARTS = 2
LANES = 128
STORES = 4
QUARTERS = 8
UNITS = ((0, 1), (2, 3), (4, 5), (6, 7))
MESH = pl.DeviceIdType.MESH
F32 = jnp.float32
BF16 = jnp.bfloat16


def ridge_kernel(ring, chips, samples, ridge, x_hbm, w_hbm, y_hbm, eta_hbm, wo, ro,
                 x, xt, w_in, w, r, eta_in, eta_t, eta, g, rs1, near, far, s1, rs2, dw, u, ur, rb,
                 load_sem, rl_r, nf_r, rs2_r, gs_s, ag1_r, ag3_r, ag_s,
                 u_s, u_r, rg_s, rg_r, wg1_r, wg2_r, wg3_r, wg_s, rf_s, rf_r):
    samp = lax.axis_index("samp")
    feat = lax.axis_index("feat")
    rows, width = x.shape
    quarter = width // QUARTERS
    group = quarter // ring
    chunk = group // ring
    hg = group // 2
    piece = rows // (2 * chips)
    cy, cz = lax.rem(samp, ring), lax.div(samp, ring)
    cx, core = lax.div(feat, 2), lax.rem(feat, 2)
    ys = [cy] + [lax.rem(cy + d, ring) for d in range(1, ring)]
    zs = [cz] + [lax.rem(cz + d, ring) for d in range(1, ring)]
    neighbour = [[cz * ring + c for c in ys], [c * ring + cy for c in zs]]
    far_first = sorted(range(1, ring), key=lambda d: -min(d, ring - d))
    near_first = far_first[::-1]
    sides = (1, ring - 1)
    across = sorted(range(1, chips), key=lambda d: -min(d, chips - d))
    peers = [(dx, dc) for dx in across + [0] for dc in (0, 1) if dx or dc]
    xs = [cx] + [lax.rem(cx + d, chips) for d in range(1, chips)]
    cores = [core, 1 - core]
    feats = [xs[dx] * 2 + cores[dc] for dx, dc in peers]
    firsts = [(ys, zs)[h % 2] for h in range(QUARTERS)]
    seconds = [(zs, ys)[h % 2] for h in range(QUARTERS)]
    group_rows = [[h * quarter + c * group for c in firsts[h]] for h in range(QUARTERS)]
    chunk_rows = [[c * chunk for c in seconds[h]] for h in range(QUARTERS)]
    own_chunks = [[group_rows[h][0] + c for c in chunk_rows[h]] for h in range(QUARTERS)]
    piece_rows = [f * piece for f in feats]
    mine = pl.ds(feat * piece, piece)
    everything = tuple(range(QUARTERS))

    def along(axis, d):
        return {"samp": neighbour[axis % 2][d]}

    def remote(src, dst, send, recv, device):
        return pltpu.make_async_remote_copy(
            src_ref=src, dst_ref=dst, send_sem=send, recv_sem=recv, device_id=device, device_id_type=MESH)

    def drain(ref, sem):
        pltpu.make_async_copy(ref, ref, sem).wait()

    def group_at(h, d):
        return pl.ds(group_rows[h][d], group)

    def part_at(h, e):
        return pl.ds(chunk_rows[h][e], chunk)

    def chunk_at(h, e):
        return pl.ds(own_chunks[h][e], chunk)

    def columns(p):
        return pl.ds(p * LANES, LANES)

    def rs1_copy(p, h, kind, k):
        if kind == 0:
            row, dst, sem = group_rows[h][2] + k * hg, rs1.at[p, h, k], rl_r.at[p, h, k]
        elif kind == 1:
            row, dst, sem = group_rows[h][sides[k]] + (1 - k) * hg, near.at[p, h, pl.ds((1 - k) * hg, hg)], nf_r.at[p, h]
        else:
            row, dst, sem = group_rows[h][sides[k]] + k * hg, far.at[p, h, pl.ds(k * hg, hg)], nf_r.at[p, h]
        return remote(g.at[p, pl.ds(row, hg)], dst, gs_s.at[p], sem, along(h, sides[k]))

    def rs2_copy(p, h, d):
        return remote(s1.at[p, h, part_at(h, d)], rs2.at[p, h, d - 1], gs_s.at[p], rs2_r.at[p, h], along(h + 1, d))

    def u_copy(p, i):
        return remote(u.at[p, pl.ds(piece_rows[i], piece)], ur.at[p, i], u_s.at[p], u_r.at[p], {"feat": feats[i]})

    def r_copy(ref, ss, rr, p, i):
        return remote(ref, ref, ss.at[p], rr.at[p], {"feat": feats[i]})

    class Gather:
        def __init__(self, view, r1, r2, r3, s):
            self.view, self.r1, self.r2, self.r3, self.s = view, r1, r2, r3, s

        def first(self, p, h):
            ref = self.view(p, chunk_at(h, 0))
            for d in near_first:
                remote(ref, ref, self.s.at[p], self.r1.at[p, h], along(h + 1, d)).start()

        def second(self, p, h):
            drain(self.view(p, pl.ds(0, (ring - 1) * chunk)), self.r1.at[p, h])
            ref = self.view(p, group_at(h, 0))
            if self.r2 is None:
                for d in far_first:
                    remote(ref, ref, self.s.at[p], self.r3.at[p, h], along(h, d)).start()
            else:
                for k in (0, 1):
                    remote(ref, ref, self.s.at[p], self.r2.at[p, h, k], along(h, sides[k])).start()

        def third(self, p, h):
            for k in (0, 1):
                drain(self.view(p, pl.ds(0, group)), self.r2.at[p, h, k])
                ref = self.view(p, pl.ds(group_rows[h][ring - sides[k]] + k * hg, hg))
                remote(ref, ref, self.s.at[p], self.r3.at[p, h], along(h, sides[k])).start()

        def last(self, p, h):
            drain(self.view(p, pl.ds(0, group if self.r2 is not None else (ring - 1) * group)), self.r3.at[p, h])

        def sent(self, p):
            drain(self.view(p, pl.ds(0, QUARTERS * ((ring - 1) * chunk + 3 * group))), self.s.at[p])

    ag = Gather(lambda p, at: dw.at[p, at], ag1_r, None, ag3_r, ag_s)
    wg = Gather(lambda p, at: wo.at[at, columns(p)], wg1_r, wg2_r, wg3_r, wg_s)

    def take_u(p):
        step = max(rows // 2, piece)
        for k in range(rows // step):
            at = pl.ds(k * step, step)
            u[p, at] = jnp.dot(x[at], dw[p], preferred_element_type=F32).astype(BF16)

    def send_u(p):
        for i in range(len(peers)):
            u_copy(p, i).start()

    def sum_u(p):
        total = u[p, mine].astype(F32)
        drain(ur.at[p], u_r.at[p])
        for i in range(len(peers)):
            total = total + ur[p, i].astype(F32)
        drain(ur.at[p], u_s.at[p])
        return total

    def send_r(p):
        rb[p, mine] = r[p].astype(BF16)
        for i in range(len(peers)):
            r_copy(rb.at[p, mine], rg_s, rg_r, p, i).start()

    def start_g(p, hs):
        if hs == UNITS[0]:
            drain(ur.at[p], rg_r.at[p])
        at = slice(hs[0] * quarter, (hs[-1] + 1) * quarter)
        g[p, at] = jnp.dot(xt[at], rb[p], preferred_element_type=F32)
        send_g(p, hs, 0)
        if p == 0:
            send_g(p, hs, 1)

    def send_g(p, hs, kind):
        for h in hs:
            for k in (0, 1):
                rs1_copy(p, h, kind, k).start()

    def pass_g(p, hs):
        for h in hs:
            for k in (0, 1):
                rs1_copy(p, h, 0, k).wait_recv()
                at = pl.ds(group_rows[h][sides[k]] + k * hg, hg)
                g[p, at] = g[p, at] + rs1[p, h, k]
                rs1_copy(p, h, 2, k).start()

    def mid_g(p, hs):
        for h in hs:
            drain(g.at[p, pl.ds(0, 2 * group)], nf_r.at[p, h])
            for e in far_first + [0]:
                at = part_at(h, e)
                s1[p, h, at] = g[p, chunk_at(h, e)] + near[p, h, at] + far[p, h, at]
                if e:
                    rs2_copy(p, h, e).start()

    def end_g(p, hs, last):
        for h in hs:
            drain(g.at[p, pl.ds(0, (ring - 1) * chunk)], rs2_r.at[p, h])
            total = s1[p, h, part_at(h, 0)]
            for d in range(1, ring):
                total = total + rs2[p, h, d - 1]
            delta = eta[h] * (total / samples - ridge * w[p, h])
            at = chunk_at(h, 0)
            dw[p, at] = delta.astype(BF16)
            ag.first(p, h)
            new = w[p, h] + COMBINE_WEIGHT * delta
            w[p, h] = new
            if last:
                wo[at, p * LANES:(p + 1) * LANES] = new

    loads = [pltpu.make_async_copy(w_hbm, w_in, load_sem.at[0]),
             pltpu.make_async_copy(x_hbm, x, load_sem.at[1]),
             pltpu.make_async_copy(eta_hbm, eta_in, load_sem.at[2])]
    loads += [pltpu.make_async_copy(y_hbm.at[mine, columns(p)], r.at[p], load_sem.at[3 + p]) for p in range(PARTS)]
    for load in loads:
        load.start()
    barrier = pltpu.get_barrier_semaphore()
    for d in range(1, ring):
        for axis in (0, 1):
            pl.semaphore_signal(barrier, inc=1, device_id=along(axis, d), device_id_type=MESH)
    for i in range(len(peers)):
        pl.semaphore_signal(barrier, inc=1, device_id={"feat": feats[i]}, device_id_type=MESH)
    loads[0].wait()
    for p in range(PARTS):
        dw[p] = w_in[:, p * LANES:(p + 1) * LANES].astype(BF16)
        for h in everything:
            w[p, h] = w_in[chunk_at(h, 0), p * LANES:(p + 1) * LANES]
    loads[1].wait()
    take_u(0)
    pl.semaphore_wait(barrier, 2 * (ring - 1) + len(peers))
    send_u(0)
    for p in range(1, PARTS):
        take_u(p)
        send_u(p)
    tile = min(width, 256)
    for k in range(width // tile):
        xt[k * tile:(k + 1) * tile] = x[:, k * tile:(k + 1) * tile].T
    loads[2].wait()
    for h in everything:
        pos = own_chunks[h][0]
        line = eta_in[pl.ds(lax.div(pos, LANES), 1), :]
        eta_t[...] = jnp.broadcast_to(line, (LANES, LANES)).T
        eta[h] = eta_t[pl.ds(lax.rem(pos, LANES), chunk), :]
    for p in range(PARTS):
        loads[3 + p].wait()
        r[p] = r[p] - sum_u(p)
        send_r(p)

    def sweep(last):
        both = [(p, hs) for p in range(PARTS) for hs in UNITS]
        for p, hs in both:
            start_g(p, hs)
        for p in range(PARTS):
            drain(ur.at[p], rg_s.at[p])
        for p, hs in both:
            pass_g(p, hs)
            if p == 0:
                for q in range(1, PARTS):
                    send_g(q, hs, 1)
        for p, hs in both:
            mid_g(p, hs)
        for p, hs in both:
            end_g(p, hs, last)
        for p, hs in both:
            for h in hs:
                ag.second(p, h)
        if last:
            for p in range(PARTS):
                for h in everything:
                    wg.first(p, h)
        for p in range(PARTS):
            drain(g.at[p, pl.ds(0, QUARTERS * (3 * group + (ring - 1) * chunk))], gs_s.at[p])
            for h in everything:
                ag.last(p, h)
            ag.sent(p)
            take_u(p)
            send_u(p)
        if last:
            for p in range(PARTS):
                for h in everything:
                    wg.second(p, h)
        for p in range(PARTS):
            r[p] = r[p] - COMBINE_WEIGHT * sum_u(p)
            if last:
                ro[mine, p * LANES:(p + 1) * LANES] = r[p]
                for i in range(len(peers)):
                    r_copy(ro.at[mine, columns(p)], rf_s, rf_r, p, i).start()
            else:
                send_r(p)
        if last:
            for p in range(PARTS):
                for h in everything:
                    wg.third(p, h)

    def body(i, carry):
        sweep(False)
        return carry

    lax.fori_loop(0, SWEEPS - 1, body, 0)
    sweep(True)
    for p in range(PARTS):
        final = ro.at[pl.ds(0, len(peers) * piece), columns(p)]
        drain(final, rf_r.at[p])
        drain(final, rf_s.at[p])
    for p in range(PARTS):
        for h in everything:
            wg.last(p, h)
        wg.sent(p)


def store_kernel(w_in, r_in, w_out, r_out, sem):
    rows = w_in.shape[0] // STORES
    stores = [pltpu.make_async_copy(w_in.at[pl.ds(k * rows, rows)], w_out.at[pl.ds(k * rows, rows)], sem.at[k]) for k in range(STORES)]
    stores.append(pltpu.make_async_copy(r_in, r_out, sem.at[STORES]))
    for store in stores:
        store.start()
    for store in stores:
        store.wait()


def solution(mesh):
    samp_count = mesh.shape["samp"]
    feat_count = mesh.shape["feat"]
    ring = math.isqrt(samp_count)
    chips = feat_count // 2

    def local_solve(x_loc, w_loc, y_loc, eta_loc):
        rows, width = x_loc.shape
        samples = rows * samp_count
        ridge = RIDGE_SCALE * (width * feat_count) / samples
        group = width // QUARTERS // ring
        chunk = group // ring
        piece = rows // feat_count
        npeer = feat_count - 1
        dma = pltpu.SemaphoreType.DMA
        v = pltpu.VMEM
        each = (PARTS, QUARTERS)
        scratch = [
            v((rows, width), BF16),
            v((width, rows), BF16),
            v((width, PARTS * LANES), F32),
            v(each + (chunk, LANES), F32),
            v((PARTS, piece, LANES), F32),
            v((width // LANES, LANES), F32),
            v((LANES, LANES), F32),
            v((QUARTERS, chunk, LANES), F32),
            v((PARTS, width, LANES), F32),
            v(each + (2, group // 2, LANES), F32),
            v(each + (group, LANES), F32),
            v(each + (group, LANES), F32),
            v(each + (group, LANES), F32),
            v(each + (ring - 1, chunk, LANES), F32),
            v((PARTS, width, LANES), BF16),
            v((PARTS, rows, LANES), BF16),
            v((PARTS, npeer, piece, LANES), BF16),
            v((PARTS, rows, LANES), BF16),
            dma((3 + PARTS,)),
            dma(each + (2,)), dma(each), dma(each), dma((PARTS,)),
            dma(each), dma(each), dma((PARTS,)),
            dma((PARTS,)), dma((PARTS,)), dma((PARTS,)), dma((PARTS,)),
            dma(each), dma(each + (2,)), dma(each), dma((PARTS,)),
            dma((PARTS,)), dma((PARTS,)),
        ]
        solved = pl.pallas_call(
            functools.partial(ridge_kernel, ring, chips, samples, ridge),
            out_shape=[pltpu.VMEM(w_loc.shape, F32), pltpu.VMEM(y_loc.shape, F32)],
            in_specs=[pl.BlockSpec(memory_space=pltpu.HBM)] * 4,
            out_specs=[pl.BlockSpec(memory_space=pltpu.VMEM)] * 2,
            scratch_shapes=scratch,
            compiler_params=pltpu.CompilerParams(
                collective_id=0, has_side_effects=True, vmem_limit_bytes=56 * 1024 * 1024),
        )(x_loc, w_loc, y_loc, eta_loc.reshape(width // LANES, LANES))
        return pl.pallas_call(
            store_kernel,
            out_shape=[jax.ShapeDtypeStruct(w_loc.shape, F32), jax.ShapeDtypeStruct(y_loc.shape, F32)],
            in_specs=[pl.BlockSpec(memory_space=pltpu.VMEM)] * 2,
            out_specs=[pl.BlockSpec(memory_space=pltpu.HBM)] * 2,
            scratch_shapes=[dma((STORES + 1,))],
            compiler_params=pltpu.CompilerParams(vmem_limit_bytes=4 * 1024 * 1024),
        )(*solved)

    return jax.shard_map(
        local_solve,
        mesh=mesh,
        in_specs=(P(("prob", "samp"), "feat"), P(("prob", "feat"), None), P(("prob", "samp"), None), P(("prob", "feat"))),
        out_specs=(P(("prob", "feat"), None), P(("prob", "samp"), None)),
        check_vma=False,
    )
```

```python
import functools
import math

import jax
import jax.numpy as jnp
from jax import lax
from jax.experimental import pallas as pl
from jax.experimental.pallas import tpu as pltpu
from jax.sharding import PartitionSpec as P

SWEEPS = 4
COMBINE_WEIGHT = 0.8
RIDGE_SCALE = 0.1
PARTS = 2
LANES = 128
STORES = 4
QUARTERS = 8
UNITS = ((0, 1), (2, 3), (4, 5), (6, 7))
MESH = pl.DeviceIdType.MESH
F32 = jnp.float32
BF16 = jnp.bfloat16


def ridge_kernel(ring, chips, samples, ridge, x_hbm, w_hbm, y_hbm, eta_hbm, wo, ro,
                 x, xt, w_in, w, r, eta_in, eta_t, eta, g, rs1, near, far, s1, rs2, dw, u, ur, rb,
                 load_sem, rl_r, nf_r, rs2_r, gs_s, ag1_r, ag3_r, ag_s,
                 u_s, u_r, rg_s, rg_r, wg1_r, wg2_r, wg3_r, wg_s, rf_s, rf_r):
    samp = lax.axis_index("samp")
    feat = lax.axis_index("feat")
    rows, width = x.shape
    quarter = width // QUARTERS
    group = quarter // ring
    chunk = group // ring
    hg = group // 2
    piece = rows // (2 * chips)
    cy, cz = lax.rem(samp, ring), lax.div(samp, ring)
    cx, core = lax.div(feat, 2), lax.rem(feat, 2)
    ys = [cy] + [lax.rem(cy + d, ring) for d in range(1, ring)]
    zs = [cz] + [lax.rem(cz + d, ring) for d in range(1, ring)]
    neighbour = [[cz * ring + c for c in ys], [c * ring + cy for c in zs]]
    far_first = sorted(range(1, ring), key=lambda d: -min(d, ring - d))
    sides = (1, ring - 1)
    across = sorted(range(1, chips), key=lambda d: -min(d, chips - d))
    peers = [(dx, dc) for dx in across + [0] for dc in (0, 1) if dx or dc]
    xs = [cx] + [lax.rem(cx + d, chips) for d in range(1, chips)]
    cores = [core, 1 - core]
    feats = [xs[dx] * 2 + cores[dc] for dx, dc in peers]
    firsts = [(ys, zs)[h % 2] for h in range(QUARTERS)]
    seconds = [(zs, ys)[h % 2] for h in range(QUARTERS)]
    group_rows = [[h * quarter + c * group for c in firsts[h]] for h in range(QUARTERS)]
    chunk_rows = [[c * chunk for c in seconds[h]] for h in range(QUARTERS)]
    own_chunks = [[group_rows[h][0] + c for c in chunk_rows[h]] for h in range(QUARTERS)]
    piece_rows = [f * piece for f in feats]
    mine = pl.ds(feat * piece, piece)
    everything = tuple(range(QUARTERS))

    def along(axis, d):
        return {"samp": neighbour[axis % 2][d]}

    def remote(src, dst, send, recv, device):
        return pltpu.make_async_remote_copy(
            src_ref=src, dst_ref=dst, send_sem=send, recv_sem=recv, device_id=device, device_id_type=MESH)

    def drain(ref, sem):
        pltpu.make_async_copy(ref, ref, sem).wait()

    def group_at(h, d):
        return pl.ds(group_rows[h][d], group)

    def part_at(h, e):
        return pl.ds(chunk_rows[h][e], chunk)

    def chunk_at(h, e):
        return pl.ds(own_chunks[h][e], chunk)

    def columns(p):
        return pl.ds(p * LANES, LANES)

    def rs1_copy(p, h, kind, k):
        if kind == 0:
            row, dst, sem = group_rows[h][2] + k * hg, rs1.at[p, h, k], rl_r.at[p, h, k]
        elif kind == 1:
            row, dst, sem = group_rows[h][sides[k]] + (1 - k) * hg, near.at[p, h, pl.ds((1 - k) * hg, hg)], nf_r.at[p, h]
        else:
            row, dst, sem = group_rows[h][sides[k]] + k * hg, far.at[p, h, pl.ds(k * hg, hg)], nf_r.at[p, h]
        return remote(g.at[p, pl.ds(row, hg)], dst, gs_s.at[p], sem, along(h, sides[k]))

    def rs2_copy(p, h, d):
        return remote(s1.at[p, h, part_at(h, d)], rs2.at[p, h, d - 1], gs_s.at[p], rs2_r.at[p, h], along(h + 1, d))

    def u_copy(p, i):
        return remote(u.at[p, pl.ds(piece_rows[i], piece)], ur.at[p, i], u_s.at[p], u_r.at[p], {"feat": feats[i]})

    def r_copy(ref, ss, rr, p, i):
        return remote(ref, ref, ss.at[p], rr.at[p], {"feat": feats[i]})

    class Gather:
        def __init__(self, view, r1, r2, r3, s):
            self.view, self.r1, self.r2, self.r3, self.s = view, r1, r2, r3, s

        def first(self, p, h):
            ref = self.view(p, chunk_at(h, 0))
            for d in far_first:
                remote(ref, ref, self.s.at[p], self.r1.at[p, h], along(h + 1, d)).start()

        def second(self, p, h):
            drain(self.view(p, pl.ds(0, (ring - 1) * chunk)), self.r1.at[p, h])
            ref = self.view(p, group_at(h, 0))
            if self.r2 is None:
                for d in far_first:
                    remote(ref, ref, self.s.at[p], self.r3.at[p, h], along(h, d)).start()
            else:
                for k in (0, 1):
                    remote(ref, ref, self.s.at[p], self.r2.at[p, h, k], along(h, sides[k])).start()

        def third(self, p, h):
            for k in (0, 1):
                drain(self.view(p, pl.ds(0, group)), self.r2.at[p, h, k])
                ref = self.view(p, pl.ds(group_rows[h][ring - sides[k]] + k * hg, hg))
                remote(ref, ref, self.s.at[p], self.r3.at[p, h], along(h, sides[k])).start()

        def last(self, p, h):
            drain(self.view(p, pl.ds(0, group if self.r2 is not None else (ring - 1) * group)), self.r3.at[p, h])

        def sent(self, p):
            drain(self.view(p, pl.ds(0, QUARTERS * ((ring - 1) * chunk + 3 * group))), self.s.at[p])

    ag = Gather(lambda p, at: dw.at[p, at], ag1_r, None, ag3_r, ag_s)
    wg = Gather(lambda p, at: wo.at[at, columns(p)], wg1_r, wg2_r, wg3_r, wg_s)

    def take_u(p, k):
        step = rows // 2
        side = lax.div(cx, chips // 2)
        at = pl.ds((1 - side if k == 0 else side) * step, step)
        u[p, at] = jnp.dot(x[at], dw[p], preferred_element_type=F32).astype(BF16)

    def send_u(p, k):
        for i, (dx, dc) in enumerate(peers):
            if (dx == chips // 2) == (k == 0):
                u_copy(p, i).start()

    def sum_u(p):
        total = u[p, mine].astype(F32)
        drain(ur.at[p], u_r.at[p])
        for i in range(len(peers)):
            total = total + ur[p, i].astype(F32)
        drain(ur.at[p], u_s.at[p])
        return total

    def send_r(p):
        rb[p, mine] = r[p].astype(BF16)
        for i in range(len(peers)):
            r_copy(rb.at[p, mine], rg_s, rg_r, p, i).start()

    def start_g(p, hs):
        if hs == UNITS[0]:
            drain(ur.at[p], rg_r.at[p])
        at = slice(hs[0] * quarter, (hs[-1] + 1) * quarter)
        g[p, at] = jnp.dot(xt[at], rb[p], preferred_element_type=F32)
        send_g(p, hs, 0)
        if p == 0:
            send_g(p, hs, 1)

    def send_g(p, hs, kind):
        for h in hs:
            for k in (0, 1):
                rs1_copy(p, h, kind, k).start()

    def pass_g(p, hs):
        for h in hs:
            for k in (0, 1):
                rs1_copy(p, h, 0, k).wait_recv()
                at = pl.ds(group_rows[h][sides[k]] + k * hg, hg)
                g[p, at] = g[p, at] + rs1[p, h, k]
                rs1_copy(p, h, 2, k).start()

    def mid_g(p, hs):
        for h in hs:
            drain(g.at[p, pl.ds(0, 2 * group)], nf_r.at[p, h])
            for e in far_first + [0]:
                at = part_at(h, e)
                s1[p, h, at] = g[p, chunk_at(h, e)] + near[p, h, at] + far[p, h, at]
                if e:
                    rs2_copy(p, h, e).start()

    def end_g(p, hs, last):
        for h in hs:
            drain(g.at[p, pl.ds(0, (ring - 1) * chunk)], rs2_r.at[p, h])
            total = s1[p, h, part_at(h, 0)]
            for d in range(1, ring):
                total = total + rs2[p, h, d - 1]
            delta = eta[h] * (total / samples - ridge * w[p, h])
            at = chunk_at(h, 0)
            dw[p, at] = delta.astype(BF16)
            ag.first(p, h)
            new = w[p, h] + COMBINE_WEIGHT * delta
            w[p, h] = new
            if last:
                wo[at, p * LANES:(p + 1) * LANES] = new

    loads = [pltpu.make_async_copy(w_hbm, w_in, load_sem.at[0]),
             pltpu.make_async_copy(x_hbm, x, load_sem.at[1]),
             pltpu.make_async_copy(eta_hbm, eta_in, load_sem.at[2])]
    loads += [pltpu.make_async_copy(y_hbm.at[mine, columns(p)], r.at[p], load_sem.at[3 + p]) for p in range(PARTS)]
    for load in loads:
        load.start()
    barrier = pltpu.get_barrier_semaphore()
    for d in range(1, ring):
        for axis in (0, 1):
            pl.semaphore_signal(barrier, inc=1, device_id=along(axis, d), device_id_type=MESH)
    for i in range(len(peers)):
        pl.semaphore_signal(barrier, inc=1, device_id={"feat": feats[i]}, device_id_type=MESH)
    loads[0].wait()
    for p in range(PARTS):
        dw[p] = w_in[:, p * LANES:(p + 1) * LANES].astype(BF16)
        for h in everything:
            w[p, h] = w_in[chunk_at(h, 0), p * LANES:(p + 1) * LANES]
    loads[1].wait()
    for k in (0, 1):
        take_u(0, k)
    pl.semaphore_wait(barrier, 2 * (ring - 1) + len(peers))
    for k in (0, 1):
        send_u(0, k)
    for p in range(1, PARTS):
        for k in (0, 1):
            take_u(p, k)
            send_u(p, k)
    tile = min(width, 256)
    for k in range(width // tile):
        xt[k * tile:(k + 1) * tile] = x[:, k * tile:(k + 1) * tile].T
    loads[2].wait()
    for h in everything:
        pos = own_chunks[h][0]
        line = eta_in[pl.ds(lax.div(pos, LANES), 1), :]
        eta_t[...] = jnp.broadcast_to(line, (LANES, LANES)).T
        eta[h] = eta_t[pl.ds(lax.rem(pos, LANES), chunk), :]
    for p in range(PARTS):
        loads[3 + p].wait()
        r[p] = r[p] - sum_u(p)
        send_r(p)

    def sweep(last):
        both = [(p, hs) for p in range(PARTS) for hs in UNITS]
        for p, hs in both:
            start_g(p, hs)
        for p in range(PARTS):
            drain(ur.at[p], rg_s.at[p])
        for p, hs in both:
            pass_g(p, hs)
            if p == 0:
                for q in range(1, PARTS):
                    send_g(q, hs, 1)
        for p, hs in both:
            mid_g(p, hs)
        for p, hs in both:
            end_g(p, hs, last)
        for p, hs in both:
            for h in hs:
                ag.second(p, h)
        if last:
            for p in range(PARTS):
                for h in everything:
                    wg.first(p, h)
        for p in range(PARTS):
            drain(g.at[p, pl.ds(0, QUARTERS * (3 * group + (ring - 1) * chunk))], gs_s.at[p])
            for h in everything:
                ag.last(p, h)
            for k in (0, 1):
                take_u(p, k)
                send_u(p, k)
            ag.sent(p)
        if last:
            for p in range(PARTS):
                for h in everything:
                    wg.second(p, h)
        for p in range(PARTS):
            r[p] = r[p] - COMBINE_WEIGHT * sum_u(p)
            if last:
                ro[mine, p * LANES:(p + 1) * LANES] = r[p]
                for i in range(len(peers)):
                    r_copy(ro.at[mine, columns(p)], rf_s, rf_r, p, i).start()
            else:
                send_r(p)
        if last:
            for p in range(PARTS):
                for h in everything:
                    wg.third(p, h)

    def body(i, carry):
        sweep(False)
        return carry

    lax.fori_loop(0, SWEEPS - 1, body, 0)
    sweep(True)
    for p in range(PARTS):
        final = ro.at[pl.ds(0, len(peers) * piece), columns(p)]
        drain(final, rf_r.at[p])
        drain(final, rf_s.at[p])
    for p in range(PARTS):
        for h in everything:
            wg.last(p, h)
        wg.sent(p)


def store_kernel(w_in, r_in, w_out, r_out, sem):
    rows = w_in.shape[0] // STORES
    stores = [pltpu.make_async_copy(w_in.at[pl.ds(k * rows, rows)], w_out.at[pl.ds(k * rows, rows)], sem.at[k]) for k in range(STORES)]
    stores.append(pltpu.make_async_copy(r_in, r_out, sem.at[STORES]))
    for store in stores:
        store.start()
    for store in stores:
        store.wait()


def solution(mesh):
    samp_count = mesh.shape["samp"]
    feat_count = mesh.shape["feat"]
    ring = math.isqrt(samp_count)
    chips = feat_count // 2

    def local_solve(x_loc, w_loc, y_loc, eta_loc):
        rows, width = x_loc.shape
        samples = rows * samp_count
        ridge = RIDGE_SCALE * (width * feat_count) / samples
        group = width // QUARTERS // ring
        chunk = group // ring
        piece = rows // feat_count
        npeer = feat_count - 1
        dma = pltpu.SemaphoreType.DMA
        v = pltpu.VMEM
        each = (PARTS, QUARTERS)
        scratch = [
            v((rows, width), BF16),
            v((width, rows), BF16),
            v((width, PARTS * LANES), F32),
            v(each + (chunk, LANES), F32),
            v((PARTS, piece, LANES), F32),
            v((width // LANES, LANES), F32),
            v((LANES, LANES), F32),
            v((QUARTERS, chunk, LANES), F32),
            v((PARTS, width, LANES), F32),
            v(each + (2, group // 2, LANES), F32),
            v(each + (group, LANES), F32),
            v(each + (group, LANES), F32),
            v(each + (group, LANES), F32),
            v(each + (ring - 1, chunk, LANES), F32),
            v((PARTS, width, LANES), BF16),
            v((PARTS, rows, LANES), BF16),
            v((PARTS, npeer, piece, LANES), BF16),
            v((PARTS, rows, LANES), BF16),
            dma((3 + PARTS,)),
            dma(each + (2,)), dma(each), dma(each), dma((PARTS,)),
            dma(each), dma(each), dma((PARTS,)),
            dma((PARTS,)), dma((PARTS,)), dma((PARTS,)), dma((PARTS,)),
            dma(each), dma(each + (2,)), dma(each), dma((PARTS,)),
            dma((PARTS,)), dma((PARTS,)),
        ]
        solved = pl.pallas_call(
            functools.partial(ridge_kernel, ring, chips, samples, ridge),
            out_shape=[pltpu.VMEM(w_loc.shape, F32), pltpu.VMEM(y_loc.shape, F32)],
            in_specs=[pl.BlockSpec(memory_space=pltpu.HBM)] * 4,
            out_specs=[pl.BlockSpec(memory_space=pltpu.VMEM)] * 2,
            scratch_shapes=scratch,
            compiler_params=pltpu.CompilerParams(
                collective_id=0, has_side_effects=True, vmem_limit_bytes=56 * 1024 * 1024),
        )(x_loc, w_loc, y_loc, eta_loc.reshape(width // LANES, LANES))
        return pl.pallas_call(
            store_kernel,
            out_shape=[jax.ShapeDtypeStruct(w_loc.shape, F32), jax.ShapeDtypeStruct(y_loc.shape, F32)],
            in_specs=[pl.BlockSpec(memory_space=pltpu.VMEM)] * 2,
            out_specs=[pl.BlockSpec(memory_space=pltpu.HBM)] * 2,
            scratch_shapes=[dma((STORES + 1,))],
            compiler_params=pltpu.CompilerParams(vmem_limit_bytes=4 * 1024 * 1024),
        )(*solved)

    return jax.shard_map(
        local_solve,
        mesh=mesh,
        in_specs=(P(("prob", "samp"), "feat"), P(("prob", "feat"), None), P(("prob", "samp"), None), P(("prob", "feat"))),
        out_specs=(P(("prob", "feat"), None), P(("prob", "samp"), None)),
        check_vma=False,
    )
```

```python
import functools
import math

import jax
import jax.numpy as jnp
from jax import lax
from jax.experimental import pallas as pl
from jax.experimental.pallas import tpu as pltpu
from jax.sharding import PartitionSpec as P

SWEEPS = 4
COMBINE_WEIGHT = 0.8
RIDGE_SCALE = 0.1
PARTS = 2
LANES = 128
STORES = 4
QUARTERS = 8
UNITS = tuple((h,) for h in range(QUARTERS))
MESH = pl.DeviceIdType.MESH
F32 = jnp.float32
BF16 = jnp.bfloat16


def ridge_kernel(ring, chips, samples, ridge, x_hbm, w_hbm, y_hbm, eta_hbm, wo, ro,
                 x, xt, w_in, w, r, eta_in, eta_t, eta, g, rs1, near, far, s1, rs2, dw, u, ur, rb,
                 load_sem, rl_r, nf_r, rs2_r, gs_s, ag1_r, ag3_r, ag_s,
                 u_s, u_r, rg_s, rg_r, wg1_r, wg2_r, wg3_r, wg_s, rf_s, rf_r):
    samp = lax.axis_index("samp")
    feat = lax.axis_index("feat")
    rows, width = x.shape
    quarter = width // QUARTERS
    group = quarter // ring
    chunk = group // ring
    hg = group // 2
    piece = rows // (2 * chips)
    cy, cz = lax.rem(samp, ring), lax.div(samp, ring)
    cx, core = lax.div(feat, 2), lax.rem(feat, 2)
    ys = [cy] + [lax.rem(cy + d, ring) for d in range(1, ring)]
    zs = [cz] + [lax.rem(cz + d, ring) for d in range(1, ring)]
    neighbour = [[cz * ring + c for c in ys], [c * ring + cy for c in zs]]
    far_first = sorted(range(1, ring), key=lambda d: -min(d, ring - d))
    sides = (1, ring - 1)
    across = sorted(range(1, chips), key=lambda d: -min(d, chips - d))
    peers = [(dx, dc) for dx in across + [0] for dc in (0, 1) if dx or dc]
    xs = [cx] + [lax.rem(cx + d, chips) for d in range(1, chips)]
    cores = [core, 1 - core]
    feats = [xs[dx] * 2 + cores[dc] for dx, dc in peers]
    firsts = [(ys, zs)[h % 2] for h in range(QUARTERS)]
    seconds = [(zs, ys)[h % 2] for h in range(QUARTERS)]
    group_rows = [[h * quarter + c * group for c in firsts[h]] for h in range(QUARTERS)]
    chunk_rows = [[c * chunk for c in seconds[h]] for h in range(QUARTERS)]
    own_chunks = [[group_rows[h][0] + c for c in chunk_rows[h]] for h in range(QUARTERS)]
    piece_rows = [f * piece for f in feats]
    mine = pl.ds(feat * piece, piece)
    everything = tuple(range(QUARTERS))

    def along(axis, d):
        return {"samp": neighbour[axis % 2][d]}

    def remote(src, dst, send, recv, device):
        return pltpu.make_async_remote_copy(
            src_ref=src, dst_ref=dst, send_sem=send, recv_sem=recv, device_id=device, device_id_type=MESH)

    def drain(ref, sem):
        pltpu.make_async_copy(ref, ref, sem).wait()

    def group_at(h, d):
        return pl.ds(group_rows[h][d], group)

    def part_at(h, e):
        return pl.ds(chunk_rows[h][e], chunk)

    def chunk_at(h, e):
        return pl.ds(own_chunks[h][e], chunk)

    def columns(p):
        return pl.ds(p * LANES, LANES)

    def rs1_copy(p, h, kind, k):
        if kind == 0:
            row, dst, sem = group_rows[h][2] + k * hg, rs1.at[p, h, k], rl_r.at[p, h, k]
        elif kind == 1:
            row, dst, sem = group_rows[h][sides[k]] + (1 - k) * hg, near.at[p, h, pl.ds((1 - k) * hg, hg)], nf_r.at[p, h]
        else:
            row, dst, sem = group_rows[h][sides[k]] + k * hg, far.at[p, h, pl.ds(k * hg, hg)], nf_r.at[p, h]
        return remote(g.at[p, pl.ds(row, hg)], dst, gs_s.at[p], sem, along(h, sides[k]))

    def rs2_copy(p, h, d):
        return remote(s1.at[p, h, part_at(h, d)], rs2.at[p, h, d - 1], gs_s.at[p], rs2_r.at[p, h], along(h + 1, d))

    def u_copy(p, i):
        return remote(u.at[p, pl.ds(piece_rows[i], piece)], ur.at[p, i], u_s.at[p], u_r.at[p], {"feat": feats[i]})

    def r_copy(ref, ss, rr, p, i):
        return remote(ref, ref, ss.at[p], rr.at[p], {"feat": feats[i]})

    class Gather:
        def __init__(self, view, r1, r2, r3, s):
            self.view, self.r1, self.r2, self.r3, self.s = view, r1, r2, r3, s

        def first(self, p, h):
            ref = self.view(p, chunk_at(h, 0))
            for d in far_first:
                remote(ref, ref, self.s.at[p], self.r1.at[p, h], along(h + 1, d)).start()

        def second(self, p, h):
            drain(self.view(p, pl.ds(0, (ring - 1) * chunk)), self.r1.at[p, h])
            ref = self.view(p, group_at(h, 0))
            if self.r2 is None:
                for d in far_first:
                    remote(ref, ref, self.s.at[p], self.r3.at[p, h], along(h, d)).start()
            else:
                for k in (0, 1):
                    remote(ref, ref, self.s.at[p], self.r2.at[p, h, k], along(h, sides[k])).start()

        def third(self, p, h):
            for k in (0, 1):
                drain(self.view(p, pl.ds(0, group)), self.r2.at[p, h, k])
                ref = self.view(p, pl.ds(group_rows[h][ring - sides[k]] + k * hg, hg))
                remote(ref, ref, self.s.at[p], self.r3.at[p, h], along(h, sides[k])).start()

        def last(self, p, h):
            drain(self.view(p, pl.ds(0, group if self.r2 is not None else (ring - 1) * group)), self.r3.at[p, h])

        def sent(self, p):
            drain(self.view(p, pl.ds(0, QUARTERS * ((ring - 1) * chunk + 3 * group))), self.s.at[p])

    ag = Gather(lambda p, at: dw.at[p, at], ag1_r, None, ag3_r, ag_s)
    wg = Gather(lambda p, at: wo.at[at, columns(p)], wg1_r, wg2_r, wg3_r, wg_s)

    def take_u(p, k):
        step = rows // 2
        side = lax.div(cx, chips // 2)
        at = pl.ds((1 - side if k == 0 else side) * step, step)
        u[p, at] = jnp.dot(x[at], dw[p], preferred_element_type=F32).astype(BF16)

    def send_u(p, k):
        for i, (dx, dc) in enumerate(peers):
            if (dx == chips // 2) == (k == 0):
                u_copy(p, i).start()

    def sum_u(p):
        total = u[p, mine].astype(F32)
        drain(ur.at[p], u_r.at[p])
        for i in range(len(peers)):
            total = total + ur[p, i].astype(F32)
        drain(ur.at[p], u_s.at[p])
        return total

    def send_r(p):
        rb[p, mine] = r[p].astype(BF16)
        for i in range(len(peers)):
            r_copy(rb.at[p, mine], rg_s, rg_r, p, i).start()

    def start_g(p, hs):
        if hs == UNITS[0]:
            drain(ur.at[p], rg_r.at[p])
        at = slice(hs[0] * quarter, (hs[-1] + 1) * quarter)
        g[p, at] = jnp.dot(xt[at], rb[p], preferred_element_type=F32)
        send_g(p, hs, 0)
        if p == 0:
            send_g(p, hs, 1)

    def send_g(p, hs, kind):
        for h in hs:
            for k in (0, 1):
                rs1_copy(p, h, kind, k).start()

    def pass_g(p, hs):
        for h in hs:
            for k in (0, 1):
                rs1_copy(p, h, 0, k).wait_recv()
                at = pl.ds(group_rows[h][sides[k]] + k * hg, hg)
                g[p, at] = g[p, at] + rs1[p, h, k]
                rs1_copy(p, h, 2, k).start()

    def mid_g(p, hs):
        for h in hs:
            drain(g.at[p, pl.ds(0, 2 * group)], nf_r.at[p, h])
            for e in far_first + [0]:
                at = part_at(h, e)
                s1[p, h, at] = g[p, chunk_at(h, e)] + near[p, h, at] + far[p, h, at]
                if e:
                    rs2_copy(p, h, e).start()

    def end_g(p, hs, last):
        for h in hs:
            drain(g.at[p, pl.ds(0, (ring - 1) * chunk)], rs2_r.at[p, h])
            total = s1[p, h, part_at(h, 0)]
            for d in range(1, ring):
                total = total + rs2[p, h, d - 1]
            delta = eta[h] * (total / samples - ridge * w[p, h])
            at = chunk_at(h, 0)
            dw[p, at] = delta.astype(BF16)
            ag.first(p, h)
            new = w[p, h] + COMBINE_WEIGHT * delta
            w[p, h] = new
            if last:
                wo[at, p * LANES:(p + 1) * LANES] = new

    loads = [pltpu.make_async_copy(w_hbm, w_in, load_sem.at[0]),
             pltpu.make_async_copy(x_hbm, x, load_sem.at[1]),
             pltpu.make_async_copy(eta_hbm, eta_in, load_sem.at[2])]
    loads += [pltpu.make_async_copy(y_hbm.at[mine, columns(p)], r.at[p], load_sem.at[3 + p]) for p in range(PARTS)]
    for load in loads:
        load.start()
    barrier = pltpu.get_barrier_semaphore()
    for d in range(1, ring):
        for axis in (0, 1):
            pl.semaphore_signal(barrier, inc=1, device_id=along(axis, d), device_id_type=MESH)
    for i in range(len(peers)):
        pl.semaphore_signal(barrier, inc=1, device_id={"feat": feats[i]}, device_id_type=MESH)
    loads[0].wait()
    for p in range(PARTS):
        dw[p] = w_in[:, p * LANES:(p + 1) * LANES].astype(BF16)
        for h in everything:
            w[p, h] = w_in[chunk_at(h, 0), p * LANES:(p + 1) * LANES]
    loads[1].wait()
    for k in (0, 1):
        take_u(0, k)
    pl.semaphore_wait(barrier, 2 * (ring - 1) + len(peers))
    for k in (0, 1):
        send_u(0, k)
    for p in range(1, PARTS):
        for k in (0, 1):
            take_u(p, k)
            send_u(p, k)
    tile = min(width, 256)
    for k in range(width // tile):
        xt[k * tile:(k + 1) * tile] = x[:, k * tile:(k + 1) * tile].T
    loads[2].wait()
    for h in everything:
        pos = own_chunks[h][0]
        line = eta_in[pl.ds(lax.div(pos, LANES), 1), :]
        eta_t[...] = jnp.broadcast_to(line, (LANES, LANES)).T
        eta[h] = eta_t[pl.ds(lax.rem(pos, LANES), chunk), :]
    for p in range(PARTS):
        loads[3 + p].wait()
        r[p] = r[p] - sum_u(p)
        send_r(p)

    def sweep(last):
        both = [(p, hs) for p in range(PARTS) for hs in UNITS]
        for p, hs in both:
            start_g(p, hs)
        for p in range(PARTS):
            drain(ur.at[p], rg_s.at[p])
        for p, hs in both:
            pass_g(p, hs)
            if p == 0:
                for q in range(1, PARTS):
                    send_g(q, hs, 1)
        for p, hs in both:
            mid_g(p, hs)
        for p, hs in both:
            end_g(p, hs, last)
        for p, hs in both:
            for h in hs:
                ag.second(p, h)
        if last:
            for p in range(PARTS):
                for h in everything:
                    wg.first(p, h)
        for p in range(PARTS):
            drain(g.at[p, pl.ds(0, QUARTERS * (3 * group + (ring - 1) * chunk))], gs_s.at[p])
            for h in everything:
                ag.last(p, h)
            for k in (0, 1):
                take_u(p, k)
                send_u(p, k)
            ag.sent(p)
        if last:
            for p in range(PARTS):
                for h in everything:
                    wg.second(p, h)
        for p in range(PARTS):
            r[p] = r[p] - COMBINE_WEIGHT * sum_u(p)
            if last:
                ro[mine, p * LANES:(p + 1) * LANES] = r[p]
                for i in range(len(peers)):
                    r_copy(ro.at[mine, columns(p)], rf_s, rf_r, p, i).start()
            else:
                send_r(p)
        if last:
            for p in range(PARTS):
                for h in everything:
                    wg.third(p, h)

    def body(i, carry):
        sweep(False)
        return carry

    lax.fori_loop(0, SWEEPS - 1, body, 0)
    sweep(True)
    for p in range(PARTS):
        final = ro.at[pl.ds(0, len(peers) * piece), columns(p)]
        drain(final, rf_r.at[p])
        drain(final, rf_s.at[p])
    for p in range(PARTS):
        for h in everything:
            wg.last(p, h)
        wg.sent(p)


def store_kernel(w_in, r_in, w_out, r_out, sem):
    rows = w_in.shape[0] // STORES
    stores = [pltpu.make_async_copy(w_in.at[pl.ds(k * rows, rows)], w_out.at[pl.ds(k * rows, rows)], sem.at[k]) for k in range(STORES)]
    stores.append(pltpu.make_async_copy(r_in, r_out, sem.at[STORES]))
    for store in stores:
        store.start()
    for store in stores:
        store.wait()


def solution(mesh):
    samp_count = mesh.shape["samp"]
    feat_count = mesh.shape["feat"]
    ring = math.isqrt(samp_count)
    chips = feat_count // 2

    def local_solve(x_loc, w_loc, y_loc, eta_loc):
        rows, width = x_loc.shape
        samples = rows * samp_count
        ridge = RIDGE_SCALE * (width * feat_count) / samples
        group = width // QUARTERS // ring
        chunk = group // ring
        piece = rows // feat_count
        npeer = feat_count - 1
        dma = pltpu.SemaphoreType.DMA
        v = pltpu.VMEM
        each = (PARTS, QUARTERS)
        scratch = [
            v((rows, width), BF16),
            v((width, rows), BF16),
            v((width, PARTS * LANES), F32),
            v(each + (chunk, LANES), F32),
            v((PARTS, piece, LANES), F32),
            v((width // LANES, LANES), F32),
            v((LANES, LANES), F32),
            v((QUARTERS, chunk, LANES), F32),
            v((PARTS, width, LANES), F32),
            v(each + (2, group // 2, LANES), F32),
            v(each + (group, LANES), F32),
            v(each + (group, LANES), F32),
            v(each + (group, LANES), F32),
            v(each + (ring - 1, chunk, LANES), F32),
            v((PARTS, width, LANES), BF16),
            v((PARTS, rows, LANES), BF16),
            v((PARTS, npeer, piece, LANES), BF16),
            v((PARTS, rows, LANES), BF16),
            dma((3 + PARTS,)),
            dma(each + (2,)), dma(each), dma(each), dma((PARTS,)),
            dma(each), dma(each), dma((PARTS,)),
            dma((PARTS,)), dma((PARTS,)), dma((PARTS,)), dma((PARTS,)),
            dma(each), dma(each + (2,)), dma(each), dma((PARTS,)),
            dma((PARTS,)), dma((PARTS,)),
        ]
        solved = pl.pallas_call(
            functools.partial(ridge_kernel, ring, chips, samples, ridge),
            out_shape=[pltpu.VMEM(w_loc.shape, F32), pltpu.VMEM(y_loc.shape, F32)],
            in_specs=[pl.BlockSpec(memory_space=pltpu.HBM)] * 4,
            out_specs=[pl.BlockSpec(memory_space=pltpu.VMEM)] * 2,
            scratch_shapes=scratch,
            compiler_params=pltpu.CompilerParams(
                collective_id=0, has_side_effects=True, vmem_limit_bytes=56 * 1024 * 1024),
        )(x_loc, w_loc, y_loc, eta_loc.reshape(width // LANES, LANES))
        return pl.pallas_call(
            store_kernel,
            out_shape=[jax.ShapeDtypeStruct(w_loc.shape, F32), jax.ShapeDtypeStruct(y_loc.shape, F32)],
            in_specs=[pl.BlockSpec(memory_space=pltpu.VMEM)] * 2,
            out_specs=[pl.BlockSpec(memory_space=pltpu.HBM)] * 2,
            scratch_shapes=[dma((STORES + 1,))],
            compiler_params=pltpu.CompilerParams(vmem_limit_bytes=4 * 1024 * 1024),
        )(*solved)

    return jax.shard_map(
        local_solve,
        mesh=mesh,
        in_specs=(P(("prob", "samp"), "feat"), P(("prob", "feat"), None), P(("prob", "samp"), None), P(("prob", "feat"))),
        out_specs=(P(("prob", "feat"), None), P(("prob", "samp"), None)),
        check_vma=False,
    )
```

```python
import functools
import math

import jax
import jax.numpy as jnp
from jax import lax
from jax.experimental import pallas as pl
from jax.experimental.pallas import tpu as pltpu
from jax.sharding import PartitionSpec as P

SWEEPS = 4
COMBINE_WEIGHT = 0.8
RIDGE_SCALE = 0.1
PARTS = 2
LANES = 128
STORES = 4
QUARTERS = 8
UNITS = tuple((h,) for h in range(QUARTERS))
MESH = pl.DeviceIdType.MESH
F32 = jnp.float32
BF16 = jnp.bfloat16


def ridge_kernel(ring, chips, samples, ridge, x_hbm, w_hbm, y_hbm, eta_hbm, wo, ro,
                 x, xt, w_in, w, r, eta_in, eta_t, eta, g, rs1, near, far, s1, rs2, dw, u, ur, rb,
                 load_sem, rl_r, nf_r, rs2_r, gs_s, ag1_r, ag3_r, ag_s,
                 u_s, u_r, rg_s, rg_r, wg1_r, wg2_r, wg3_r, wg_s, rf_s, rf_r):
    samp = lax.axis_index("samp")
    feat = lax.axis_index("feat")
    rows, width = x.shape
    quarter = width // QUARTERS
    group = quarter // ring
    chunk = group // ring
    hg = group // 2
    piece = rows // (2 * chips)
    cy, cz = lax.rem(samp, ring), lax.div(samp, ring)
    cx, core = lax.div(feat, 2), lax.rem(feat, 2)
    ys = [cy] + [lax.rem(cy + d, ring) for d in range(1, ring)]
    zs = [cz] + [lax.rem(cz + d, ring) for d in range(1, ring)]
    neighbour = [[cz * ring + c for c in ys], [c * ring + cy for c in zs]]
    far_first = sorted(range(1, ring), key=lambda d: -min(d, ring - d))
    sides = (1, ring - 1)
    across = sorted(range(1, chips), key=lambda d: -min(d, chips - d))
    peers = [(dx, dc) for dx in across + [0] for dc in (0, 1) if dx or dc]
    xs = [cx] + [lax.rem(cx + d, chips) for d in range(1, chips)]
    cores = [core, 1 - core]
    feats = [xs[dx] * 2 + cores[dc] for dx, dc in peers]
    firsts = [(ys, zs)[h % 2] for h in range(QUARTERS)]
    seconds = [(zs, ys)[h % 2] for h in range(QUARTERS)]
    group_rows = [[h * quarter + c * group for c in firsts[h]] for h in range(QUARTERS)]
    chunk_rows = [[c * chunk for c in seconds[h]] for h in range(QUARTERS)]
    own_chunks = [[group_rows[h][0] + c for c in chunk_rows[h]] for h in range(QUARTERS)]
    piece_rows = [f * piece for f in feats]
    mine = pl.ds(feat * piece, piece)
    everything = tuple(range(QUARTERS))

    def along(axis, d):
        return {"samp": neighbour[axis % 2][d]}

    def remote(src, dst, send, recv, device):
        return pltpu.make_async_remote_copy(
            src_ref=src, dst_ref=dst, send_sem=send, recv_sem=recv, device_id=device, device_id_type=MESH)

    def drain(ref, sem):
        pltpu.make_async_copy(ref, ref, sem).wait()

    def group_at(h, d):
        return pl.ds(group_rows[h][d], group)

    def part_at(h, e):
        return pl.ds(chunk_rows[h][e], chunk)

    def chunk_at(h, e):
        return pl.ds(own_chunks[h][e], chunk)

    def columns(p):
        return pl.ds(p * LANES, LANES)

    def rs1_copy(p, h, kind, k):
        if kind == 0:
            row, dst, sem = group_rows[h][2] + k * hg, rs1.at[p, h, k], rl_r.at[p, h, k]
        elif kind == 1:
            row, dst, sem = group_rows[h][sides[k]] + (1 - k) * hg, near.at[p, h, pl.ds((1 - k) * hg, hg)], nf_r.at[p, h]
        else:
            row, dst, sem = group_rows[h][sides[k]] + k * hg, far.at[p, h, pl.ds(k * hg, hg)], nf_r.at[p, h]
        return remote(g.at[p, pl.ds(row, hg)], dst, gs_s.at[p], sem, along(h, sides[k]))

    def rs2_copy(p, h, d):
        return remote(s1.at[p, h, part_at(h, d)], rs2.at[p, h, d - 1], gs_s.at[p], rs2_r.at[p, h], along(h + 1, d))

    def u_copy(p, i):
        return remote(u.at[p, pl.ds(piece_rows[i], piece)], ur.at[p, i], u_s.at[p], u_r.at[p], {"feat": feats[i]})

    def r_copy(ref, ss, rr, p, i):
        return remote(ref, ref, ss.at[p], rr.at[p], {"feat": feats[i]})

    class Gather:
        def __init__(self, view, r1, r2, r3, s):
            self.view, self.r1, self.r2, self.r3, self.s = view, r1, r2, r3, s

        def first(self, p, h):
            ref = self.view(p, chunk_at(h, 0))
            for d in far_first:
                remote(ref, ref, self.s.at[p], self.r1.at[p, h], along(h + 1, d)).start()

        def second(self, p, h):
            drain(self.view(p, pl.ds(0, (ring - 1) * chunk)), self.r1.at[p, h])
            ref = self.view(p, group_at(h, 0))
            if self.r2 is None:
                for d in far_first:
                    remote(ref, ref, self.s.at[p], self.r3.at[p, h], along(h, d)).start()
            else:
                for k in (0, 1):
                    remote(ref, ref, self.s.at[p], self.r2.at[p, h, k], along(h, sides[k])).start()

        def third(self, p, h):
            for k in (0, 1):
                drain(self.view(p, pl.ds(0, group)), self.r2.at[p, h, k])
                ref = self.view(p, pl.ds(group_rows[h][ring - sides[k]] + k * hg, hg))
                remote(ref, ref, self.s.at[p], self.r3.at[p, h], along(h, sides[k])).start()

        def last(self, p, h):
            drain(self.view(p, pl.ds(0, group if self.r2 is not None else (ring - 1) * group)), self.r3.at[p, h])

        def sent(self, p):
            drain(self.view(p, pl.ds(0, QUARTERS * ((ring - 1) * chunk + 3 * group))), self.s.at[p])

    ag = Gather(lambda p, at: dw.at[p, at], ag1_r, None, ag3_r, ag_s)
    wg = Gather(lambda p, at: wo.at[at, columns(p)], wg1_r, wg2_r, wg3_r, wg_s)

    def take_u(p, k):
        step = rows // 2
        side = lax.div(cx, chips // 2)
        at = pl.ds((1 - side if k == 0 else side) * step, step)
        u[p, at] = jnp.dot(x[at], dw[p], preferred_element_type=F32).astype(BF16)

    def send_u(p, k):
        for i, (dx, dc) in enumerate(peers):
            if (dx == chips // 2) == (k == 0):
                u_copy(p, i).start()

    def sum_u(p):
        total = u[p, mine].astype(F32)
        drain(ur.at[p], u_r.at[p])
        for i in range(len(peers)):
            total = total + ur[p, i].astype(F32)
        drain(ur.at[p], u_s.at[p])
        return total

    def send_r(p):
        rb[p, mine] = r[p].astype(BF16)
        for i in range(len(peers)):
            r_copy(rb.at[p, mine], rg_s, rg_r, p, i).start()

    def start_g(p, hs):
        if hs == UNITS[0]:
            drain(ur.at[p], rg_r.at[p])
        at = slice(hs[0] * quarter, (hs[-1] + 1) * quarter)
        g[p, at] = jnp.dot(xt[at], rb[p], preferred_element_type=F32)
        send_g(p, hs, 0)
        if p == 0 and hs == UNITS[-1]:
            for each in UNITS:
                send_g(p, each, 1)

    def send_g(p, hs, kind):
        for h in hs:
            for k in (0, 1):
                rs1_copy(p, h, kind, k).start()

    def pass_g(p, hs):
        for h in hs:
            for k in (0, 1):
                rs1_copy(p, h, 0, k).wait_recv()
                at = pl.ds(group_rows[h][sides[k]] + k * hg, hg)
                g[p, at] = g[p, at] + rs1[p, h, k]
                rs1_copy(p, h, 2, k).start()

    def mid_g(p, hs):
        for h in hs:
            drain(g.at[p, pl.ds(0, 2 * group)], nf_r.at[p, h])
            for e in far_first + [0]:
                at = part_at(h, e)
                s1[p, h, at] = g[p, chunk_at(h, e)] + near[p, h, at] + far[p, h, at]
                if e:
                    rs2_copy(p, h, e).start()

    def end_g(p, hs, last):
        for h in hs:
            drain(g.at[p, pl.ds(0, (ring - 1) * chunk)], rs2_r.at[p, h])
            total = s1[p, h, part_at(h, 0)]
            for d in range(1, ring):
                total = total + rs2[p, h, d - 1]
            delta = eta[h] * (total / samples - ridge * w[p, h])
            at = chunk_at(h, 0)
            dw[p, at] = delta.astype(BF16)
            ag.first(p, h)
            new = w[p, h] + COMBINE_WEIGHT * delta
            w[p, h] = new
            if last:
                wo[at, p * LANES:(p + 1) * LANES] = new

    loads = [pltpu.make_async_copy(w_hbm, w_in, load_sem.at[0]),
             pltpu.make_async_copy(x_hbm, x, load_sem.at[1]),
             pltpu.make_async_copy(eta_hbm, eta_in, load_sem.at[2])]
    loads += [pltpu.make_async_copy(y_hbm.at[mine, columns(p)], r.at[p], load_sem.at[3 + p]) for p in range(PARTS)]
    for load in loads:
        load.start()
    barrier = pltpu.get_barrier_semaphore()
    for d in range(1, ring):
        for axis in (0, 1):
            pl.semaphore_signal(barrier, inc=1, device_id=along(axis, d), device_id_type=MESH)
    for i in range(len(peers)):
        pl.semaphore_signal(barrier, inc=1, device_id={"feat": feats[i]}, device_id_type=MESH)
    loads[0].wait()
    for p in range(PARTS):
        dw[p] = w_in[:, p * LANES:(p + 1) * LANES].astype(BF16)
        for h in everything:
            w[p, h] = w_in[chunk_at(h, 0), p * LANES:(p + 1) * LANES]
    loads[1].wait()
    for k in (0, 1):
        take_u(0, k)
    pl.semaphore_wait(barrier, 2 * (ring - 1) + len(peers))
    for k in (0, 1):
        send_u(0, k)
    for p in range(1, PARTS):
        for k in (0, 1):
            take_u(p, k)
            send_u(p, k)
    tile = min(width, 256)
    for k in range(width // tile):
        xt[k * tile:(k + 1) * tile] = x[:, k * tile:(k + 1) * tile].T
    loads[2].wait()
    for h in everything:
        pos = own_chunks[h][0]
        line = eta_in[pl.ds(lax.div(pos, LANES), 1), :]
        eta_t[...] = jnp.broadcast_to(line, (LANES, LANES)).T
        eta[h] = eta_t[pl.ds(lax.rem(pos, LANES), chunk), :]
    for p in range(PARTS):
        loads[3 + p].wait()
        r[p] = r[p] - sum_u(p)
        send_r(p)

    def sweep(last):
        both = [(p, hs) for p in range(PARTS) for hs in UNITS]
        for p, hs in both:
            start_g(p, hs)
        for p in range(PARTS):
            drain(ur.at[p], rg_s.at[p])
        for p, hs in both:
            pass_g(p, hs)
            if p == 0:
                for q in range(1, PARTS):
                    send_g(q, hs, 1)
        for p, hs in both:
            mid_g(p, hs)
        for p, hs in both:
            end_g(p, hs, last)
        for p, hs in both:
            for h in hs:
                ag.second(p, h)
        if last:
            for p in range(PARTS):
                for h in everything:
                    wg.first(p, h)
        for p in range(PARTS):
            drain(g.at[p, pl.ds(0, QUARTERS * (3 * group + (ring - 1) * chunk))], gs_s.at[p])
            for h in everything:
                ag.last(p, h)
            for k in (0, 1):
                take_u(p, k)
                send_u(p, k)
            ag.sent(p)
        if last:
            for p in range(PARTS):
                for h in everything:
                    wg.second(p, h)
        for p in range(PARTS):
            r[p] = r[p] - COMBINE_WEIGHT * sum_u(p)
            if last:
                ro[mine, p * LANES:(p + 1) * LANES] = r[p]
                for i in range(len(peers)):
                    r_copy(ro.at[mine, columns(p)], rf_s, rf_r, p, i).start()
            else:
                send_r(p)
        if last:
            for p in range(PARTS):
                for h in everything:
                    wg.third(p, h)

    def body(i, carry):
        sweep(False)
        return carry

    lax.fori_loop(0, SWEEPS - 1, body, 0)
    sweep(True)
    for p in range(PARTS):
        final = ro.at[pl.ds(0, len(peers) * piece), columns(p)]
        drain(final, rf_r.at[p])
        drain(final, rf_s.at[p])
    for p in range(PARTS):
        for h in everything:
            wg.last(p, h)
        wg.sent(p)


def store_kernel(w_in, r_in, w_out, r_out, sem):
    rows = w_in.shape[0] // STORES
    stores = [pltpu.make_async_copy(w_in.at[pl.ds(k * rows, rows)], w_out.at[pl.ds(k * rows, rows)], sem.at[k]) for k in range(STORES)]
    stores.append(pltpu.make_async_copy(r_in, r_out, sem.at[STORES]))
    for store in stores:
        store.start()
    for store in stores:
        store.wait()


def solution(mesh):
    samp_count = mesh.shape["samp"]
    feat_count = mesh.shape["feat"]
    ring = math.isqrt(samp_count)
    chips = feat_count // 2

    def local_solve(x_loc, w_loc, y_loc, eta_loc):
        rows, width = x_loc.shape
        samples = rows * samp_count
        ridge = RIDGE_SCALE * (width * feat_count) / samples
        group = width // QUARTERS // ring
        chunk = group // ring
        piece = rows // feat_count
        npeer = feat_count - 1
        dma = pltpu.SemaphoreType.DMA
        v = pltpu.VMEM
        each = (PARTS, QUARTERS)
        scratch = [
            v((rows, width), BF16),
            v((width, rows), BF16),
            v((width, PARTS * LANES), F32),
            v(each + (chunk, LANES), F32),
            v((PARTS, piece, LANES), F32),
            v((width // LANES, LANES), F32),
            v((LANES, LANES), F32),
            v((QUARTERS, chunk, LANES), F32),
            v((PARTS, width, LANES), F32),
            v(each + (2, group // 2, LANES), F32),
            v(each + (group, LANES), F32),
            v(each + (group, LANES), F32),
            v(each + (group, LANES), F32),
            v(each + (ring - 1, chunk, LANES), F32),
            v((PARTS, width, LANES), BF16),
            v((PARTS, rows, LANES), BF16),
            v((PARTS, npeer, piece, LANES), BF16),
            v((PARTS, rows, LANES), BF16),
            dma((3 + PARTS,)),
            dma(each + (2,)), dma(each), dma(each), dma((PARTS,)),
            dma(each), dma(each), dma((PARTS,)),
            dma((PARTS,)), dma((PARTS,)), dma((PARTS,)), dma((PARTS,)),
            dma(each), dma(each + (2,)), dma(each), dma((PARTS,)),
            dma((PARTS,)), dma((PARTS,)),
        ]
        solved = pl.pallas_call(
            functools.partial(ridge_kernel, ring, chips, samples, ridge),
            out_shape=[pltpu.VMEM(w_loc.shape, F32), pltpu.VMEM(y_loc.shape, F32)],
            in_specs=[pl.BlockSpec(memory_space=pltpu.HBM)] * 4,
            out_specs=[pl.BlockSpec(memory_space=pltpu.VMEM)] * 2,
            scratch_shapes=scratch,
            compiler_params=pltpu.CompilerParams(
                collective_id=0, has_side_effects=True, vmem_limit_bytes=56 * 1024 * 1024),
        )(x_loc, w_loc, y_loc, eta_loc.reshape(width // LANES, LANES))
        return pl.pallas_call(
            store_kernel,
            out_shape=[jax.ShapeDtypeStruct(w_loc.shape, F32), jax.ShapeDtypeStruct(y_loc.shape, F32)],
            in_specs=[pl.BlockSpec(memory_space=pltpu.VMEM)] * 2,
            out_specs=[pl.BlockSpec(memory_space=pltpu.HBM)] * 2,
            scratch_shapes=[dma((STORES + 1,))],
            compiler_params=pltpu.CompilerParams(vmem_limit_bytes=4 * 1024 * 1024),
        )(*solved)

    return jax.shard_map(
        local_solve,
        mesh=mesh,
        in_specs=(P(("prob", "samp"), "feat"), P(("prob", "feat"), None), P(("prob", "samp"), None), P(("prob", "feat"))),
        out_specs=(P(("prob", "feat"), None), P(("prob", "samp"), None)),
        check_vma=False,
    )
```

```python
import functools
import math

import jax
import jax.numpy as jnp
from jax import lax
from jax.experimental import pallas as pl
from jax.experimental.pallas import tpu as pltpu
from jax.sharding import PartitionSpec as P

SWEEPS = 4
COMBINE_WEIGHT = 0.8
RIDGE_SCALE = 0.1
PARTS = 2
LANES = 128
STORES = 4
QUARTERS = 8
UNITS = tuple((h,) for h in range(QUARTERS))
MESH = pl.DeviceIdType.MESH
F32 = jnp.float32
BF16 = jnp.bfloat16


def ridge_kernel(ring, chips, samples, ridge, x_hbm, w_hbm, y_hbm, eta_hbm, wo, ro,
                 x, xt, w_in, w, r, eta_in, eta_t, eta, g, rs1, near, far, s1, rs2, dw, u, ur, rb,
                 load_sem, rl_r, nf_r, rs2_r, gs_s, ag1_r, ag3_r, ag_s,
                 u_s, u_r, rg_s, rg_r, wg1_r, wg2_r, wg3_r, wg_s, rf_s, rf_r):
    samp = lax.axis_index("samp")
    feat = lax.axis_index("feat")
    rows, width = x.shape
    quarter = width // QUARTERS
    group = quarter // ring
    chunk = group // ring
    hg = group // 2
    piece = rows // (2 * chips)
    cy, cz = lax.rem(samp, ring), lax.div(samp, ring)
    cx, core = lax.div(feat, 2), lax.rem(feat, 2)
    ys = [cy] + [lax.rem(cy + d, ring) for d in range(1, ring)]
    zs = [cz] + [lax.rem(cz + d, ring) for d in range(1, ring)]
    neighbour = [[cz * ring + c for c in ys], [c * ring + cy for c in zs]]
    far_first = sorted(range(1, ring), key=lambda d: -min(d, ring - d))
    sides = (1, ring - 1)
    across = sorted(range(1, chips), key=lambda d: -min(d, chips - d))
    peers = [(dx, dc) for dx in across + [0] for dc in (0, 1) if dx or dc]
    xs = [cx] + [lax.rem(cx + d, chips) for d in range(1, chips)]
    cores = [core, 1 - core]
    feats = [xs[dx] * 2 + cores[dc] for dx, dc in peers]
    firsts = [(ys, zs)[h % 2] for h in range(QUARTERS)]
    seconds = [(zs, ys)[h % 2] for h in range(QUARTERS)]
    group_rows = [[h * quarter + c * group for c in firsts[h]] for h in range(QUARTERS)]
    chunk_rows = [[c * chunk for c in seconds[h]] for h in range(QUARTERS)]
    own_chunks = [[group_rows[h][0] + c for c in chunk_rows[h]] for h in range(QUARTERS)]
    piece_rows = [f * piece for f in feats]
    mine = pl.ds(feat * piece, piece)
    everything = tuple(range(QUARTERS))

    def along(axis, d):
        return {"samp": neighbour[axis % 2][d]}

    def remote(src, dst, send, recv, device):
        return pltpu.make_async_remote_copy(
            src_ref=src, dst_ref=dst, send_sem=send, recv_sem=recv, device_id=device, device_id_type=MESH)

    def drain(ref, sem):
        pltpu.make_async_copy(ref, ref, sem).wait()

    def group_at(h, d):
        return pl.ds(group_rows[h][d], group)

    def part_at(h, e):
        return pl.ds(chunk_rows[h][e], chunk)

    def chunk_at(h, e):
        return pl.ds(own_chunks[h][e], chunk)

    def columns(p):
        return pl.ds(p * LANES, LANES)

    def rs1_copy(p, h, kind, k):
        if kind == 0:
            row, dst, sem = group_rows[h][2] + k * hg, rs1.at[p, h, k], rl_r.at[p, h, k]
        elif kind == 1:
            row, dst, sem = group_rows[h][sides[k]] + (1 - k) * hg, near.at[p, h, pl.ds((1 - k) * hg, hg)], nf_r.at[p, h]
        else:
            row, dst, sem = group_rows[h][sides[k]] + k * hg, far.at[p, h, pl.ds(k * hg, hg)], nf_r.at[p, h]
        return remote(g.at[p, pl.ds(row, hg)], dst, gs_s.at[p], sem, along(h, sides[k]))

    def rs2_copy(p, h, d):
        return remote(s1.at[p, h, part_at(h, d)], rs2.at[p, h, d - 1], gs_s.at[p], rs2_r.at[p, h], along(h + 1, d))

    def u_copy(p, i):
        return remote(u.at[p, pl.ds(piece_rows[i], piece)], ur.at[p, i], u_s.at[p], u_r.at[p], {"feat": feats[i]})

    def r_copy(ref, ss, rr, p, i):
        return remote(ref, ref, ss.at[p], rr.at[p], {"feat": feats[i]})

    class Gather:
        def __init__(self, view, r1, r2, r3, s):
            self.view, self.r1, self.r2, self.r3, self.s = view, r1, r2, r3, s

        def first(self, p, h):
            ref = self.view(p, chunk_at(h, 0))
            for d in far_first:
                remote(ref, ref, self.s.at[p], self.r1.at[p, h], along(h + 1, d)).start()

        def second(self, p, h):
            drain(self.view(p, pl.ds(0, (ring - 1) * chunk)), self.r1.at[p, h])
            ref = self.view(p, group_at(h, 0))
            if self.r2 is None:
                for d in far_first:
                    remote(ref, ref, self.s.at[p], self.r3.at[p, h], along(h, d)).start()
            else:
                for k in (0, 1):
                    remote(ref, ref, self.s.at[p], self.r2.at[p, h, k], along(h, sides[k])).start()

        def third(self, p, h):
            for k in (0, 1):
                drain(self.view(p, pl.ds(0, group)), self.r2.at[p, h, k])
                ref = self.view(p, pl.ds(group_rows[h][ring - sides[k]] + k * hg, hg))
                remote(ref, ref, self.s.at[p], self.r3.at[p, h], along(h, sides[k])).start()

        def last(self, p, h):
            drain(self.view(p, pl.ds(0, group if self.r2 is not None else (ring - 1) * group)), self.r3.at[p, h])

        def sent(self, p):
            drain(self.view(p, pl.ds(0, QUARTERS * ((ring - 1) * chunk + 3 * group))), self.s.at[p])

    ag = Gather(lambda p, at: dw.at[p, at], ag1_r, None, ag3_r, ag_s)
    wg = Gather(lambda p, at: wo.at[at, columns(p)], wg1_r, wg2_r, wg3_r, wg_s)

    def take_u(p, k):
        step = rows // 2
        side = lax.div(cx, chips // 2)
        at = pl.ds((1 - side if k == 0 else side) * step, step)
        u[p, at] = jnp.dot(x[at], dw[p], preferred_element_type=F32).astype(BF16)

    def send_u(p, k):
        for i, (dx, dc) in enumerate(peers):
            if (dx == chips // 2) == (k == 0):
                u_copy(p, i).start()

    def sum_u(p):
        total = u[p, mine].astype(F32)
        drain(ur.at[p], u_r.at[p])
        for i in range(len(peers)):
            total = total + ur[p, i].astype(F32)
        drain(ur.at[p], u_s.at[p])
        return total

    def send_r(p):
        rb[p, mine] = r[p].astype(BF16)
        for i in range(len(peers)):
            r_copy(rb.at[p, mine], rg_s, rg_r, p, i).start()

    def start_g(p, hs):
        if hs == UNITS[0]:
            drain(ur.at[p], rg_r.at[p])
        at = slice(hs[0] * quarter, (hs[-1] + 1) * quarter)
        g[p, at] = jnp.dot(xt[at], rb[p], preferred_element_type=F32)
        send_g(p, hs, 0)
        send_g(p, hs, 1)

    def send_g(p, hs, kind):
        for h in hs:
            for k in (0, 1):
                rs1_copy(p, h, kind, k).start()

    def pass_g(p, hs):
        for h in hs:
            for k in (0, 1):
                rs1_copy(p, h, 0, k).wait_recv()
                at = pl.ds(group_rows[h][sides[k]] + k * hg, hg)
                g[p, at] = g[p, at] + rs1[p, h, k]
                rs1_copy(p, h, 2, k).start()

    def mid_g(p, hs):
        for h in hs:
            drain(g.at[p, pl.ds(0, 2 * group)], nf_r.at[p, h])
            for e in far_first + [0]:
                at = part_at(h, e)
                s1[p, h, at] = g[p, chunk_at(h, e)] + near[p, h, at] + far[p, h, at]
                if e:
                    rs2_copy(p, h, e).start()

    def end_g(p, hs, last):
        for h in hs:
            drain(g.at[p, pl.ds(0, (ring - 1) * chunk)], rs2_r.at[p, h])
            total = s1[p, h, part_at(h, 0)]
            for d in range(1, ring):
                total = total + rs2[p, h, d - 1]
            delta = eta[h] * (total / samples - ridge * w[p, h])
            at = chunk_at(h, 0)
            dw[p, at] = delta.astype(BF16)
            ag.first(p, h)
            new = w[p, h] + COMBINE_WEIGHT * delta
            w[p, h] = new
            if last:
                wo[at, p * LANES:(p + 1) * LANES] = new

    loads = [pltpu.make_async_copy(w_hbm, w_in, load_sem.at[0]),
             pltpu.make_async_copy(x_hbm, x, load_sem.at[1]),
             pltpu.make_async_copy(eta_hbm, eta_in, load_sem.at[2])]
    loads += [pltpu.make_async_copy(y_hbm.at[mine, columns(p)], r.at[p], load_sem.at[3 + p]) for p in range(PARTS)]
    for load in loads:
        load.start()
    barrier = pltpu.get_barrier_semaphore()
    for d in range(1, ring):
        for axis in (0, 1):
            pl.semaphore_signal(barrier, inc=1, device_id=along(axis, d), device_id_type=MESH)
    for i in range(len(peers)):
        pl.semaphore_signal(barrier, inc=1, device_id={"feat": feats[i]}, device_id_type=MESH)
    loads[0].wait()
    for p in range(PARTS):
        dw[p] = w_in[:, p * LANES:(p + 1) * LANES].astype(BF16)
        for h in everything:
            w[p, h] = w_in[chunk_at(h, 0), p * LANES:(p + 1) * LANES]
    loads[1].wait()
    for k in (0, 1):
        take_u(0, k)
    pl.semaphore_wait(barrier, 2 * (ring - 1) + len(peers))
    for k in (0, 1):
        send_u(0, k)
    for p in range(1, PARTS):
        for k in (0, 1):
            take_u(p, k)
            send_u(p, k)
    tile = min(width, 256)
    for k in range(width // tile):
        xt[k * tile:(k + 1) * tile] = x[:, k * tile:(k + 1) * tile].T
    loads[2].wait()
    for h in everything:
        pos = own_chunks[h][0]
        line = eta_in[pl.ds(lax.div(pos, LANES), 1), :]
        eta_t[...] = jnp.broadcast_to(line, (LANES, LANES)).T
        eta[h] = eta_t[pl.ds(lax.rem(pos, LANES), chunk), :]
    for p in range(PARTS):
        loads[3 + p].wait()
        r[p] = r[p] - sum_u(p)
        send_r(p)

    def sweep(last):
        both = [(p, hs) for p in range(PARTS) for hs in UNITS]
        for p, hs in both:
            start_g(p, hs)
        for p in range(PARTS):
            drain(ur.at[p], rg_s.at[p])
        for p, hs in both:
            pass_g(p, hs)
        for p, hs in both:
            mid_g(p, hs)
        for p, hs in both:
            end_g(p, hs, last)
        for p, hs in both:
            for h in hs:
                ag.second(p, h)
        if last:
            for p in range(PARTS):
                for h in everything:
                    wg.first(p, h)
        for p in range(PARTS):
            drain(g.at[p, pl.ds(0, QUARTERS * (3 * group + (ring - 1) * chunk))], gs_s.at[p])
            for h in everything:
                ag.last(p, h)
            for k in (0, 1):
                take_u(p, k)
                send_u(p, k)
            ag.sent(p)
        if last:
            for p in range(PARTS):
                for h in everything:
                    wg.second(p, h)
        for p in range(PARTS):
            r[p] = r[p] - COMBINE_WEIGHT * sum_u(p)
            if last:
                ro[mine, p * LANES:(p + 1) * LANES] = r[p]
                for i in range(len(peers)):
                    r_copy(ro.at[mine, columns(p)], rf_s, rf_r, p, i).start()
            else:
                send_r(p)
        if last:
            for p in range(PARTS):
                for h in everything:
                    wg.third(p, h)

    def body(i, carry):
        sweep(False)
        return carry

    lax.fori_loop(0, SWEEPS - 1, body, 0)
    sweep(True)
    for p in range(PARTS):
        final = ro.at[pl.ds(0, len(peers) * piece), columns(p)]
        drain(final, rf_r.at[p])
        drain(final, rf_s.at[p])
    for p in range(PARTS):
        for h in everything:
            wg.last(p, h)
        wg.sent(p)


def store_kernel(w_in, r_in, w_out, r_out, sem):
    rows = w_in.shape[0] // STORES
    stores = [pltpu.make_async_copy(w_in.at[pl.ds(k * rows, rows)], w_out.at[pl.ds(k * rows, rows)], sem.at[k]) for k in range(STORES)]
    stores.append(pltpu.make_async_copy(r_in, r_out, sem.at[STORES]))
    for store in stores:
        store.start()
    for store in stores:
        store.wait()


def solution(mesh):
    samp_count = mesh.shape["samp"]
    feat_count = mesh.shape["feat"]
    ring = math.isqrt(samp_count)
    chips = feat_count // 2

    def local_solve(x_loc, w_loc, y_loc, eta_loc):
        rows, width = x_loc.shape
        samples = rows * samp_count
        ridge = RIDGE_SCALE * (width * feat_count) / samples
        group = width // QUARTERS // ring
        chunk = group // ring
        piece = rows // feat_count
        npeer = feat_count - 1
        dma = pltpu.SemaphoreType.DMA
        v = pltpu.VMEM
        each = (PARTS, QUARTERS)
        scratch = [
            v((rows, width), BF16),
            v((width, rows), BF16),
            v((width, PARTS * LANES), F32),
            v(each + (chunk, LANES), F32),
            v((PARTS, piece, LANES), F32),
            v((width // LANES, LANES), F32),
            v((LANES, LANES), F32),
            v((QUARTERS, chunk, LANES), F32),
            v((PARTS, width, LANES), F32),
            v(each + (2, group // 2, LANES), F32),
            v(each + (group, LANES), F32),
            v(each + (group, LANES), F32),
            v(each + (group, LANES), F32),
            v(each + (ring - 1, chunk, LANES), F32),
            v((PARTS, width, LANES), BF16),
            v((PARTS, rows, LANES), BF16),
            v((PARTS, npeer, piece, LANES), BF16),
            v((PARTS, rows, LANES), BF16),
            dma((3 + PARTS,)),
            dma(each + (2,)), dma(each), dma(each), dma((PARTS,)),
            dma(each), dma(each), dma((PARTS,)),
            dma((PARTS,)), dma((PARTS,)), dma((PARTS,)), dma((PARTS,)),
            dma(each), dma(each + (2,)), dma(each), dma((PARTS,)),
            dma((PARTS,)), dma((PARTS,)),
        ]
        solved = pl.pallas_call(
            functools.partial(ridge_kernel, ring, chips, samples, ridge),
            out_shape=[pltpu.VMEM(w_loc.shape, F32), pltpu.VMEM(y_loc.shape, F32)],
            in_specs=[pl.BlockSpec(memory_space=pltpu.HBM)] * 4,
            out_specs=[pl.BlockSpec(memory_space=pltpu.VMEM)] * 2,
            scratch_shapes=scratch,
            compiler_params=pltpu.CompilerParams(
                collective_id=0, has_side_effects=True, vmem_limit_bytes=56 * 1024 * 1024),
        )(x_loc, w_loc, y_loc, eta_loc.reshape(width // LANES, LANES))
        return pl.pallas_call(
            store_kernel,
            out_shape=[jax.ShapeDtypeStruct(w_loc.shape, F32), jax.ShapeDtypeStruct(y_loc.shape, F32)],
            in_specs=[pl.BlockSpec(memory_space=pltpu.VMEM)] * 2,
            out_specs=[pl.BlockSpec(memory_space=pltpu.HBM)] * 2,
            scratch_shapes=[dma((STORES + 1,))],
            compiler_params=pltpu.CompilerParams(vmem_limit_bytes=4 * 1024 * 1024),
        )(*solved)

    return jax.shard_map(
        local_solve,
        mesh=mesh,
        in_specs=(P(("prob", "samp"), "feat"), P(("prob", "feat"), None), P(("prob", "samp"), None), P(("prob", "feat"))),
        out_specs=(P(("prob", "feat"), None), P(("prob", "samp"), None)),
        check_vma=False,
    )
```
